32 devices in a mesh: comp: 8 (over z, x), gy: 2 (over y), gx: 2 (over core).
Axes of the slice: x: 2, y: 2, z: 4, core: 2. Of those that a mesh axis runs over, the one named last changes fastest.
Arguments:
- flow_fields: float32 [4, 6, 256, 384], P(None, None, ('comp', 'gy', 'gx')), may hold values from -6 to 6
- chlorophyll_lag: float32 [6, 256, 384], P(None, ('comp', 'gy', 'gx')), may hold values from 0.1 to 3
- tracers: float32 [16, 6, 256, 128], P(None, None, ('comp', 'gy', 'gx')), may hold values from -6 to 6
- forcing: float32 [4, 6, 256, 128], P(None, None, ('comp', 'gy', 'gx')), may hold values from -6 to 6
- ocean_mask: int32 [64, 384], replicated, may hold values 0 or 1
- bottom: int32 [64, 384], replicated, may hold values from 1 to 6
- reaction: float32 [16, 16], replicated, may hold values from -1.5 to 0.1
Outputs:
- flow_out: float32 [4, 6, 256, 384], P(None, None, ('comp', 'gy', 'gx'))
- light_out: float32 [6, 256, 384], P(None, ('comp', 'gy', 'gx'))
- tracers_out: float32 [16, 6, 256, 128], P(None, None, ('comp', 'gy', 'gx'))
- forcing_out: float32 [4, 6, 256, 128], P(None, None, ('comp', 'gy', 'gx'))
The draws below stay inside these ranges and needn't reach their ends.
All inputs are finite; a program needn't handle non-finite values.
Results may differ from the reference program's by a relative error of at most 0.0002.
Values sent between devices are 32-bit elements; how exact they have to be, the bound alone decides.
A program may use at most 64 MiB of HBM per device.

```python
import math
import jax
import jax.numpy as jnp
from jax import lax

DX = 8
YT = 128
Z = 6
NT = 16
SUB = 4
COUPLE = 2
NX = 64
NY = 384
ROWS = 256


def draw_reaction(key, part):
    first_key, second_key = jax.random.split(jax.random.fold_in(key, 7))
    spread = jnp.clip(0.05 * jax.random.normal(first_key, (NT, NT), jnp.float32), -0.1, 0.1)
    diagonal = -jax.random.uniform(second_key, (NT,), jnp.float32, 0.5, 1.5)
    eye_mask = jnp.eye(NT, dtype=jnp.float32)
    return spread * (1.0 - eye_mask) + eye_mask * diagonal[None, :]


def draw_flow_fields(key, part):
    sign_key, speed_key, scalar_key = jax.random.split(jax.random.fold_in(key, 11), 3)
    grid_shape = (2, Z, ROWS, NY)
    flow_signs = jnp.where(jax.random.uniform(sign_key, grid_shape, jnp.float32) < 0.5, -1.0, 1.0)
    flow_speed = jnp.clip(4.6 + 0.7 * jax.random.normal(speed_key, grid_shape, jnp.float32), 3.0, 6.0)
    scalars = jnp.clip(jax.random.normal(scalar_key, grid_shape, jnp.float32), -6.0, 6.0)
    return jnp.concatenate([flow_signs * flow_speed, scalars], axis=0).astype(jnp.float32)


def touch_ends(array, rng, smallest, top_value):
    spot = [jax.random.randint(jax.random.fold_in(rng, axis), (), 0, length) for axis, length in enumerate(array.shape)]
    widest = array.shape.index(max(array.shape))
    beside = spot[:widest] + [(spot[widest] + 1) % array.shape[widest]] + spot[widest + 1:]
    return array.at[tuple(spot)].set(smallest).at[tuple(beside)].set(top_value)


def block_levels(own_key, shape, cuts, least, largest):
    def one(dim, blocks):
        heights = jax.random.uniform(jax.random.fold_in(jax.random.fold_in(own_key, 6), dim), (blocks,), jnp.float32, least / len(cuts), largest / len(cuts))
        return jnp.repeat(jnp.exp(heights), shape[dim] // blocks).reshape((-1,) + (1,) * (len(shape) - dim - 1))

    level = one(*cuts[0])
    for cut in cuts[1:]:
        level = level * one(*cut)
    return level


def scatter_about(own_key, dims, scale, bound, pieces=(), kind=jnp.bfloat16):
    factor_of = block_levels(own_key, dims, pieces, -0.22, 0.18) if pieces else 1.0
    array = jax.random.normal(own_key, dims, jnp.float32) * scale * factor_of
    return jnp.minimum(jnp.maximum(array, -bound), bound).astype(kind)


def setup_inputs(seed: int = 0) -> dict:
    seeds = jax.random.split(jax.random.key(seed), 8)
    flow_fields = draw_flow_fields(jax.random.fold_in(seeds[7], 71), 0)
    chlorophyll_lag = jnp.clip(jnp.exp(math.log(3.0) - 3.4011974 * jax.random.uniform(seeds[1], (Z, ROWS, NY), jnp.float32) ** block_levels(seeds[1], (Z, ROWS, NY), ((1, 32),), -0.2, 0.2)), 0.1, 3.0)
    tracers = scatter_about(seeds[2], (NT, Z, ROWS, YT), 1.0, 6.0, ((2, 32),), jnp.float32)
    forcing = scatter_about(seeds[3], (4, Z, ROWS, YT), 1.0, 6.0, ((2, 32),), jnp.float32)
    ocean_mask = touch_ends((jax.random.randint(seeds[4], (NX, NY), 0, 5) < 4).astype(jnp.int32), jax.random.fold_in(seeds[4], 1), 0, 1)
    bottom = touch_ends(jax.random.randint(seeds[5], (NX, NY), 1, Z + 1), jax.random.fold_in(seeds[5], 1), 1, Z).astype(jnp.int32)
    reaction = draw_reaction(jax.random.fold_in(seeds[7], 71), 0)
    return dict(flow_fields=flow_fields, chlorophyll_lag=chlorophyll_lag, tracers=tracers, forcing=forcing, ocean_mask=ocean_mask, bottom=bottom, reaction=reaction)


step_time = 0.1
coriolis = 1.0
viscosity = 0.5
friction = 0.1
diffusion = 0.5
expansion = 0.2
contraction = 0.2
water_attenuation = 0.05
pigment_attenuation = 0.3
heating_rate = 5.0
tracer_time = 0.1
tracer_diffusion = 0.5
warm_rate = 0.1
salt_rate = 0.05


def interior(values):
    return values[..., 1:-1, 1:-1]


def laplace(values):
    return (values[..., 2:, 1:-1] + values[..., :-2, 1:-1] + values[..., 1:-1, 2:] + values[..., 1:-1, :-2]
            - 4.0 * interior(values))


def derive_rows(values):
    return 0.5 * (values[..., 2:, 1:-1] - values[..., :-2, 1:-1])


def derive_cols(values):
    return 0.5 * (values[..., 1:-1, 2:] - values[..., 1:-1, :-2])


def pad_plane(values):
    return jnp.pad(values, [(0, 0)] * (values.ndim - 2) + [(1, 1), (1, 1)])


def absorb(pigment):
    optical = jnp.cumsum(water_attenuation + pigment_attenuation * pigment, axis=0)
    lower_light = jnp.exp(-optical)
    upper_light = jnp.concatenate([jnp.ones_like(lower_light[:1]), lower_light[:-1]], axis=0)
    return heating_rate * (upper_light - lower_light)


def dynamics_update(padded, heating, wet_cells):
    flow_x, flow_y, warmth, saltness = padded[0], padded[1], padded[2], padded[3]
    pressure = jnp.cumsum(expansion * saltness - contraction * warmth, axis=0)
    centre_x = interior(flow_x)
    centre_y = interior(flow_y)
    centre_warm = interior(warmth)
    centre_salt = interior(saltness)
    new_x = wet_cells * (centre_x + step_time * (coriolis * centre_y - derive_rows(pressure)
                                                 + viscosity * laplace(flow_x) - friction * centre_x))
    new_y = wet_cells * (centre_y + step_time * (-coriolis * centre_x - derive_cols(pressure)
                                                 + viscosity * laplace(flow_y) - friction * centre_y))
    new_warm = wet_cells * (centre_warm + step_time * (-(derive_rows(flow_x * warmth) + derive_cols(flow_y * warmth))
                                                       + diffusion * laplace(warmth) + heating))
    new_salt = wet_cells * (centre_salt + step_time * (-(derive_rows(flow_x * saltness) + derive_cols(flow_y * saltness))
                                                       + diffusion * laplace(saltness)))
    return jnp.stack([new_x, new_y, new_warm, new_salt], axis=0)


def tracer_update(padded, warmth, saltness, wet_cells, reaction):
    planes = padded.shape[0] - 2
    tracer_pad = padded[:planes]
    flow_x = padded[planes]
    flow_y = padded[planes + 1]
    advect = derive_rows(flow_x[None] * tracer_pad) + derive_cols(flow_y[None] * tracer_pad)
    centre = interior(tracer_pad)
    growth = jnp.exp(warm_rate * warmth - salt_rate * saltness)
    reacted = jnp.einsum("ab,bzxy->azxy", reaction, centre, precision=lax.Precision.HIGHEST) * growth[None]
    return wet_cells[None] * (centre + tracer_time * (tracer_diffusion * laplace(tracer_pad) - advect + reacted))


def pigment_of(tracer_state):
    return 0.25 * (tracer_state[0] * tracer_state[0] + tracer_state[1] * tracer_state[1])


def tracer_view(values):
    planes = values.shape[0]
    live_rows = jnp.roll(values, DX, axis=2)[:, :, :3 * NX]
    return live_rows.reshape(planes, Z, 3, NX, YT).transpose(0, 1, 3, 2, 4).reshape(planes, Z, NX, NY)


def tracer_store(values):
    planes = values.shape[0]
    arranged = values.reshape(planes, Z, NX, 3, YT).transpose(0, 1, 3, 2, 4).reshape(planes, Z, 3 * NX, YT)
    whole = jnp.concatenate([arranged, jnp.zeros((planes, Z, NX, YT), jnp.float32)], axis=2)
    return jnp.roll(whole, -DX, axis=2)


def reference(flow_fields, chlorophyll_lag, tracers, forcing, ocean_mask, bottom, reaction):
    level_index = jnp.arange(Z, dtype=jnp.int32)[:, None, None]
    wet_cells = jnp.where((ocean_mask[None] == 1) & (level_index < bottom[None]), 1.0, 0.0).astype(jnp.float32)
    flow_state = jnp.roll(flow_fields, DX, axis=2)[:, :, 3 * NX:]
    pigment = jnp.roll(chlorophyll_lag, DX, axis=1)[:, 3 * NX:]
    tracer_state = tracer_view(tracers)
    driving = tracer_view(forcing)
    for coupling in range(COUPLE):
        heating = absorb(pigment)
        total_x = jnp.zeros_like(flow_state[0])
        total_y = jnp.zeros_like(flow_state[0])
        for substep in range(SUB):
            flow_state = dynamics_update(pad_plane(flow_state), heating, wet_cells)
            total_x = total_x + flow_state[0]
            total_y = total_y + flow_state[1]
        new_driving = jnp.stack([total_x / SUB, total_y / SUB, flow_state[2], flow_state[3]], axis=0)
        stacked = pad_plane(jnp.concatenate([tracer_state, driving[:2]], axis=0))
        tracer_state = tracer_update(stacked, driving[2], driving[3], wet_cells, reaction)
        pigment = pigment_of(tracer_state)
        driving = new_driving
    flow_out = jnp.roll(jnp.concatenate([jnp.zeros((4, Z, 3 * NX, NY), jnp.float32), flow_state], axis=2), -DX, axis=2)
    light_out = jnp.roll(jnp.concatenate([jnp.zeros((Z, 3 * NX, NY), jnp.float32), pigment], axis=1), -DX, axis=1)
    return flow_out, light_out, tracer_store(tracer_state), tracer_store(driving)
```

```python
import functools
import math

import jax
import jax.numpy as jnp
from jax import lax
from jax.experimental import pallas as pl
from jax.experimental.pallas import tpu as pltpu
from jax.sharding import PartitionSpec as P

SUB = 4
MESH = pl.DeviceIdType.MESH
AXES = ("comp", "gy", "gx")


def substep(state, above, heat, wet, first, last):
    u, v, t, s = state
    rows, cols = u.shape
    p = above + 0.2 * (s - t)

    def row_next(x):
        return pltpu.roll(x, rows - 1, 0)

    def row_prev(x):
        return pltpu.roll(x, 1, 0)

    def col_next(x):
        return jnp.where(last, 0.0, pltpu.roll(x, cols - 1, 1))

    def col_prev(x):
        return jnp.where(first, 0.0, pltpu.roll(x, 1, 1))

    um, up, vm, vp = 1.0 - u, 1.0 + u, 1.0 - v, 1.0 + v
    new_u = 0.79 * u + 0.1 * v + 0.05 * (row_next(u - p) + row_prev(u + p) + col_next(u) + col_prev(u))
    new_v = 0.79 * v - 0.1 * u + 0.05 * (row_next(v) + row_prev(v) + col_next(v - p) + col_prev(v + p))
    new_t = 0.8 * t + 0.05 * (row_next(t * um) + row_prev(t * up) + col_next(t * vm) + col_prev(t * vp)) + heat
    new_s = 0.8 * s + 0.05 * (row_next(s * um) + row_prev(s * up) + col_next(s * vm) + col_prev(s * vp))
    return tuple(jnp.where(wet, x, 0.0) for x in (new_u, new_v, new_t, new_s)), p


def kernel(sizes, flow_h, chl_h, tracers_h, forcing_h, ocean_h, bottom_h, reaction_h,
           flow_out, light_out, tracers_out, forcing_out,
           flow, chl, tracers, forcing, ocean, bottom, reaction, load_s,
           gflow, gchl, mid, gmid, depth, total, optical, light, total2, optical2, light2, pig,
           drive_send, drive_row_send, drive2_send,
           row_send, col_send, row_recv, col_recv, row_send2, col_send2, row_recv2, col_recv2,
           held, pig_s, drive, drive_row, light_s,
           flow_ss, flow_rs, chl_ss, chl_rs, mid_ss, mid_rs, row_ss, row_rs, col_ss, col_rs,
           row2_ss, row2_rs, col2_ss, col2_rs, pig_ss, pig_rs,
           drive_ss, drive_rs, drow_ss, drow_rs, drive2_ss, drive2_rs, light_ss, light_rs, ready):
    n_comp, n_gy, n_gx = sizes
    grid = n_gy * n_gx
    every = n_comp * grid
    group = every // 4
    levels, tile, cols = chl.shape
    half = tile // 2
    wide = 2 * tile
    nt = tracers.shape[0]
    yt = tracers.shape[3]
    position = (lax.axis_index("comp") * grid + lax.axis_index("gy") * n_gx + lax.axis_index("gx")).astype(jnp.int32)
    moved = lax.rem(position + 1, jnp.int32(every))
    strip = lax.rem(moved, jnp.int32(group))
    section = lax.div(moved, jnp.int32(group))
    is_dyn = section == 3
    has_lo = strip > 0
    has_hi = strip < group - 1
    has_left = section > 0
    has_right = section < 2

    def dev(sec, row):
        pos = lax.rem(sec * group + row + (every - 1), jnp.int32(every))
        return (lax.div(pos, jnp.int32(grid)), lax.rem(lax.div(pos, jnp.int32(n_gx)), jnp.int32(n_gy)),
                lax.rem(pos, jnp.int32(n_gx)))

    def remote(src, dst, send_sem, recv_sem, target):
        return pltpu.make_async_remote_copy(src_ref=src, dst_ref=dst, send_sem=send_sem, recv_sem=recv_sem,
                                            device_id=target, device_id_type=MESH)

    three = jnp.int32(3)
    scope = jax.named_scope
    barrier = pltpu.get_barrier_semaphore()

    def load(i, src, dst):
        return pltpu.make_async_copy(src, dst, load_s.at[i])

    def mask_loads(part, offset):
        begin = pl.multiple_of(jnp.clip(strip + offset, 0, group - 1) * tile, tile)
        return (load(2 + 2 * part, ocean_h.at[pl.ds(begin, tile), :], ocean.at[part]),
                load(3 + 2 * part, bottom_h.at[pl.ds(begin, tile), :], bottom.at[part]))

    def greet(sem, sec, row):
        pl.semaphore_signal(sem, inc=1, device_id=dev(sec, row), device_id_type=MESH)

    sides = ((0, -1, has_lo), (1, 1, has_hi))
    lo_n = has_lo.astype(jnp.int32)
    hi_n = has_hi.astype(jnp.int32)

    def pig_copy(k, sec, part, row):
        from_rows = (pl.ds(0, tile), pl.ds(0, half), pl.ds(half, half))[part]
        to_rows = (pl.ds(0, tile), pl.ds(tile, half), pl.ds(tile + half, half))[part]
        return remote(pig_s.at[k, from_rows], pig.at[sec, k, to_rows], pig_ss.at[part, k], pig_rs.at[sec, part, k],
                      dev(three, row))

    def light_copy(k, sec, begin, row):
        return remote(light_s.at[k], light_out.at[k, :, pl.ds(begin, yt)], light_ss.at[k], light_rs.at[sec, k],
                      dev(three, row))

    @pl.when(is_dyn)
    def _():
        loads = [load(0, flow_h, flow), load(1, chl_h, chl)]
        for part in range(3):
            loads.extend(mask_loads(part, part - 1))
        for copy in loads:
            copy.start()
        for _, offset, present in sides:
            @pl.when(present)
            def _():
                greet(barrier, three, strip + offset)
        for place, present in ((half, has_lo), (0, has_hi)):
            @pl.when(jnp.logical_not(present))
            def _():
                for f in range(4):
                    gflow[f, :, place:place + half, :] = jnp.zeros((levels, half, cols), jnp.float32)
                    gmid[f, :, place:place + half, :] = jnp.zeros((levels, half, cols), jnp.float32)
                gchl[:, place:place + half, :] = jnp.zeros((levels, half, cols), jnp.float32)
                for sec in range(3):
                    pig[sec, :, tile + place:tile + place + half, :] = jnp.zeros((levels, half, yt), jnp.float32)
        total[...] = jnp.zeros_like(total)
        total2[...] = jnp.zeros_like(total2)
        optical[...] = jnp.zeros_like(optical)
        optical2[...] = jnp.zeros_like(optical2)
        light[...] = jnp.ones_like(light)
        light2[...] = jnp.ones_like(light2)
        with scope("d_load"):
            for copy in loads:
                copy.wait()
        with scope("d_bar"):
            pl.semaphore_wait(barrier, 3 + 4 * lo_n + 4 * hi_n)

        def flow_copies(k, side, offset, arriving):
            at = side if arriving else 1 - side
            place = pl.ds(half * (1 - at), half)
            target = dev(three, strip + offset)
            return (remote(flow.at[:, k, place, :], gflow.at[:, k, place, :], flow_ss.at[side, k], flow_rs.at[at, k], target),
                    remote(chl.at[k, place, :], gchl.at[k, place, :], chl_ss.at[side, k], chl_rs.at[at, k], target))

        def mid_copy(k, side, offset, arriving):
            at = side if arriving else 1 - side
            place = pl.ds(half * (1 - at), half)
            return remote(mid.at[:, k, place, :], gmid.at[:, k, place, :], mid_ss.at[side, k], mid_rs.at[at, k],
                          dev(three, strip + offset))

        def drive_copies(k, sec):
            target = dev(jnp.int32(sec), strip)
            return (remote(drive_send.at[k, sec], drive.at[k], drive_ss.at[sec, k], drive_rs.at[k], target),
                    remote(drive_row_send.at[k, sec], drive_row.at[k], drow_ss.at[sec, k], drow_rs.at[k], target))

        def drive2_copy(k, sec):
            return remote(drive2_send.at[k, sec], forcing_out.at[:, k], drive2_ss.at[sec, k], drive2_rs.at[k],
                          dev(jnp.int32(sec), strip))

        @pl.loop(0, levels)
        def _(k):
            for side, offset, present in sides:
                @pl.when(present)
                def _():
                    for copy in flow_copies(k, side, offset, False):
                        copy.start()

        for sec in range(3):
            greet(ready, jnp.int32(sec), strip)
            for _, offset, present in sides:
                @pl.when(present)
                def _():
                    greet(ready, jnp.int32(sec), strip + offset)

        def deep_of(part):
            return jnp.where(ocean[part] == 1, bottom[part], 0)

        row_d = lax.broadcasted_iota(jnp.int32, (tile, cols), 0)
        depth[0:tile, :] = deep_of(1)
        depth[tile:wide, :] = jnp.where(row_d < half, deep_of(2) * hi_n, deep_of(0) * lo_n)
        tracers_out[...] = jnp.zeros_like(tracers_out)
        forcing_out[...] = jnp.zeros_like(forcing_out)

        lane_d = lax.broadcasted_iota(jnp.int32, (wide, cols), 1)
        lane_t = lax.broadcasted_iota(jnp.int32, (tile, yt), 1)

        def phase(k, now, pigment, sums, opt_s, light_ref):
            first, last = lane_d == 0, lane_d == cols - 1
            opt = opt_s[...] + (0.05 + 0.3 * pigment)
            lower = jnp.exp(-opt)
            heat = 0.5 * (light_ref[...] - lower)
            opt_s[...] = opt
            light_ref[...] = lower
            wet = k < depth[...]
            sum_u = None
            for n in range(SUB):
                now, p = substep(now, sums[n], heat, wet, first, last)
                sums[n] = p
                sum_u = now[0] if n == 0 else sum_u + now[0]
                sum_v = now[1] if n == 0 else sum_v + now[1]
            return now, sum_u * (1.0 / SUB), sum_v[0:tile] * (1.0 / SUB)

        @pl.loop(0, levels)
        def _(k):
            with scope("d_halo"):
                for side, offset, present in sides:
                    @pl.when(present)
                    def _():
                        for copy in flow_copies(k, side, offset, True):
                            copy.wait_recv()
            now = tuple(jnp.concatenate([flow[f, k], gflow[f, k]], axis=0) for f in range(4))
            now, mean_u, mean_v = phase(k, now, jnp.concatenate([chl[k], gchl[k]], axis=0), total, optical, light)
            for f in range(4):
                mid[f, k] = now[f][0:tile]
            for side, offset, present in sides:
                @pl.when(present)
                def _():
                    mid_copy(k, side, offset, False).start()
            mix = 0.1 * now[2][0:tile] - 0.05 * now[3][0:tile]
            zero = jnp.zeros((tile, yt), jnp.float32)
            for sec in range(3):
                here = slice(sec * yt, (sec + 1) * yt)
                before = mean_v[:, (sec - 1) * yt:sec * yt] if sec > 0 else zero
                after = mean_v[:, (sec + 1) * yt:(sec + 2) * yt] if sec < 2 else zero
                drive_send[k, sec, 0] = mean_u[0:tile, here]
                drive_send[k, sec, 1] = mean_v[:, here]
                drive_send[k, sec, 2] = mix[:, here]
                drive_send[k, sec, 3] = jnp.where(lane_t == yt - 1, before, after)
                drive_row_send[k, sec, 0] = mean_u[wide - 1:wide, here]
                drive_row_send[k, sec, 1] = mean_u[tile:tile + 1, here]
            for sec in range(3):
                for copy in drive_copies(k, sec):
                    copy.start()

        @pl.loop(0, levels)
        def _(k):
            with scope("d_mid"):
                for side, offset, present in sides:
                    @pl.when(present)
                    def _():
                        mid_copy(k, side, offset, True).wait_recv()
            with scope("d_pig"):
                for sec in range(3):
                    pig_copy(k, sec, 0, strip).wait_recv()
                    for part, offset, present in ((1, 1, has_hi), (2, -1, has_lo)):
                        @pl.when(present)
                        def _():
                            pig_copy(k, sec, part, strip + offset).wait_recv()
            now = tuple(jnp.concatenate([mid[f, k], gmid[f, k]], axis=0) for f in range(4))
            pigment = jnp.concatenate([pig[sec, k] for sec in range(3)], axis=1)
            now, mean_u, mean_v = phase(k, now, pigment, total2, optical2, light2)
            items = (mean_u[0:tile], mean_v, now[2][0:tile], now[3][0:tile])
            for sec in range(3):
                for f in range(4):
                    drive2_send[k, sec, f] = items[f][:, sec * yt:(sec + 1) * yt]
            drive2_copy(k, 0).start()
            for f in range(4):
                flow_out[f, k] = now[f][0:tile]

        for sec in (1, 2):
            @pl.loop(0, levels)
            def _(k):
                drive2_copy(k, sec).start()

        with scope("d_light"):
            @pl.loop(0, levels)
            def _(k):
                for sec in range(3):
                    light_copy(k, jnp.int32(sec), sec * yt, strip).wait_recv()

        with scope("d_sends"):
            @pl.loop(0, levels)
            def _(k):
                for side, offset, present in sides:
                    @pl.when(present)
                    def _():
                        for copy in flow_copies(k, side, offset, False):
                            copy.wait_send()
                        mid_copy(k, side, offset, False).wait_send()
                for sec in range(3):
                    for copy in drive_copies(k, sec):
                        copy.wait_send()
                    drive2_copy(k, sec).wait_send()


    @pl.when(jnp.logical_not(is_dyn))
    def _():
        loads = [load(0, tracers_h, tracers), load(1, forcing_h, forcing), load(4, reaction_h, reaction)]
        begin = pl.multiple_of(strip * tile, tile)
        loads.extend((load(2, ocean_h.at[pl.ds(begin, tile), :], ocean.at[1]), load(3, bottom_h.at[pl.ds(begin, tile), :], bottom.at[1])))
        for copy in loads:
            copy.start()
        for _, offset, present in sides:
            @pl.when(present)
            def _():
                greet(barrier, section, strip + offset)
                greet(barrier, three, strip + offset)
        greet(barrier, three, strip)
        beside = ((0, -1, has_left), (1, 1, has_right))
        for _, offset, present in beside:
            @pl.when(present)
            def _():
                greet(barrier, section + offset, strip)
        for side, present, bufs in ((0, has_lo, (row_recv, row_recv2)), (1, has_hi, (row_recv, row_recv2)),
                                    (0, has_left, (col_recv, col_recv2)), (1, has_right, (col_recv, col_recv2))):
            @pl.when(jnp.logical_not(present))
            def _():
                for buf in bufs:
                    buf[side] = jnp.zeros(buf.shape[1:], jnp.float32)

        lane = lax.broadcasted_iota(jnp.int32, (tile, yt), 1)
        row = lax.broadcasted_iota(jnp.int32, (tile, yt), 0)
        pair = lax.div(lane, jnp.int32(2))
        odd = lax.rem(lane, jnp.int32(2)) == 1

        flow_out[...] = jnp.zeros_like(flow_out)
        light_out[...] = jnp.zeros_like(light_out)
        with scope('t_load'):
            for copy in loads:
                copy.wait()

        def pack(items):
            packed = jnp.zeros((tile, yt), jnp.float32)
            for i, x in enumerate(items):
                packed = jnp.where(pair == i, pltpu.roll(x, 2 * i + 1, 1), packed)
            return packed

        @pl.loop(0, levels)
        def _(k):
            items = [tracers[i, k] for i in range(nt)]
            col_send[k] = pack(items + [forcing[1, k]])
            for i, x in enumerate(items + [forcing[0, k]]):
                row_send[0, k, i] = x[0:1]
                row_send[1, k, i] = x[tile - 1:tile]

        left = pl.multiple_of(section * yt, yt)
        deep = jnp.where(ocean[1, :, pl.ds(left, yt)] == 1, bottom[1, :, pl.ds(left, yt)], 0)
        with scope('t_bar'):
            pl.semaphore_wait(barrier, lo_n + hi_n + has_left.astype(jnp.int32) + has_right.astype(jnp.int32))

        def row_copy(side, offset, arriving, s_buf, r_buf, ss, rs):
            at = side if arriving else 1 - side
            return remote(s_buf.at[side], r_buf.at[at], ss.at[side], rs.at[at], dev(section, strip + offset))

        def col_copy(side, offset, arriving, s_buf, r_buf, ss, rs):
            at = side if arriving else 1 - side
            return remote(s_buf, r_buf.at[at], ss.at[side], rs.at[at], dev(section + offset, strip))

        exchange_a = ((sides, row_copy, (row_send, row_recv, row_ss, row_rs)),
                      (beside, col_copy, (col_send, col_recv, col_ss, col_rs)))
        exchange_b = ((sides, row_copy, (row_send2, row_recv2, row2_ss, row2_rs)),
                      (beside, col_copy, (col_send2, col_recv2, col2_ss, col2_rs)))

        def run(exchange, arriving, what):
            for places, make, bufs in exchange:
                for side, offset, present in places:
                    @pl.when(present)
                    def _():
                        copy = make(side, offset, arriving, *bufs)
                        if what == "start":
                            copy.start()
                        elif what == "recv":
                            copy.wait_recv()
                        else:
                            copy.wait_send()

        run(exchange_a, False, "start")
        with scope('t_xa'):
            run(exchange_a, True, "recv")
        with scope('t_ready'):
            pl.semaphore_wait(ready, 1 + lo_n + hi_n)

        def tracer_step(k, cs, u, v, growth, u_lo, u_hi, v_edge, rows_of, packed):
            um, up, vm, vp = 1.0 - u, 1.0 + u, 1.0 - v, 1.0 + v
            hi_m, lo_p = 1.0 - u_hi, 1.0 + u_lo
            edge_m, edge_p = 1.0 - v_edge, 1.0 + v_edge
            wet = k < deep
            out = []
            for i in range(nt):
                c = cs[i]
                react = reaction[i, 0] * cs[0]
                for b in range(1, nt):
                    react = react + reaction[i, b] * cs[b]
                nxt = jnp.where(row == tile - 1, rows_of[1, k, i] * hi_m, pltpu.roll(c * um, tile - 1, 0))
                prv = jnp.where(row == 0, rows_of[0, k, i] * lo_p, pltpu.roll(c * up, 1, 0))
                edge = pltpu.roll(packed, yt - (2 * i + 1), 1)
                rgt = pltpu.roll(jnp.where(lane == 0, edge * edge_m, c * vm), yt - 1, 1)
                lft = pltpu.roll(jnp.where(lane == yt - 1, edge * edge_p, c * vp), 1, 1)
                out.append(jnp.where(wet, 0.8 * c + 0.05 * ((nxt + prv) + (rgt + lft)) + growth * react, 0.0))
            return out

        def pig_copies(k):
            return ((None, pig_copy(k, section, 0, strip)), (has_lo, pig_copy(k, section, 1, strip - 1)),
                    (has_hi, pig_copy(k, section, 2, strip + 1)))

        @pl.loop(0, levels)
        def _(k):
            cs = [tracers[i, k] for i in range(nt)]
            packed = jnp.where(odd, col_recv[1, k], col_recv[0, k])
            growth = 0.1 * jnp.exp(0.1 * forcing[2, k] - 0.05 * forcing[3, k])
            v_edge = pltpu.roll(packed, yt - (2 * nt + 1), 1)
            new = tracer_step(k, cs, forcing[0, k], forcing[1, k], growth, row_recv[0, k, nt], row_recv[1, k, nt], v_edge,
                              row_recv, packed)
            pigment = 0.25 * (new[0] * new[0] + new[1] * new[1])
            pig_s[k] = pigment
            for present, copy in pig_copies(k):
                if present is None:
                    copy.start()
                else:
                    pl.when(present)(copy.start)
            for i in range(nt):
                held[i, k] = new[i]
                row_send2[0, k, i] = new[i][0:1]
                row_send2[1, k, i] = new[i][tile - 1:tile]
            col_send2[k] = pack(new)

        run(exchange_b, False, "start")
        with scope('t_xb'):
            run(exchange_b, True, "recv")

        @pl.loop(0, levels)
        def _(k):
            origin = dev(three, strip)
            with scope("t_drive"):
                remote(drive_send.at[k, 0], drive.at[k], drive_ss.at[0, k], drive_rs.at[k], origin).wait_recv()
                remote(drive_row_send.at[k, 0], drive_row.at[k], drow_ss.at[0, k], drow_rs.at[k], origin).wait_recv()
            cs = [held[i, k] for i in range(nt)]
            packed = jnp.where(odd, col_recv2[1, k], col_recv2[0, k])
            growth = 0.1 * jnp.exp(drive[k, 2])
            new = tracer_step(k, cs, drive[k, 0], drive[k, 1], growth, drive_row[k, 0], drive_row[k, 1], drive[k, 3],
                              row_recv2, packed)
            light_s[k] = 0.25 * (new[0] * new[0] + new[1] * new[1])
            light_copy(k, section, left, strip).start()
            for i in range(nt):
                tracers_out[i, k] = new[i]

        @pl.loop(0, levels)
        def _(k):
            with scope("t_drive2"):
                remote(drive2_send.at[k, 0], forcing_out.at[:, k], drive2_ss.at[0, k], drive2_rs.at[k], dev(three, strip)).wait_recv()
            light_copy(k, section, left, strip).wait_send()
            for present, copy in pig_copies(k):
                if present is None:
                    copy.wait_send()
                else:
                    pl.when(present)(copy.wait_send)

        run(exchange_a, False, "send")
        run(exchange_b, False, "send")


def write_out(*refs):
    done = refs[-1]
    copies = [pltpu.make_async_copy(refs[i], refs[4 + i], done.at[i]) for i in range(4)]
    for copy in copies:
        copy.start()
    for copy in copies:
        copy.wait()


def solution(mesh):
    sizes = tuple(mesh.shape[a] for a in AXES)

    def on_device(flow, chl, tracers, forcing, ocean, bottom, reaction):
        levels, tile, cols = chl.shape
        nt, yt = tracers.shape[0], tracers.shape[3]
        f32 = jnp.float32

        def buf(*shape):
            return pltpu.VMEM(shape, f32)

        def sem(*shape):
            return pltpu.SemaphoreType.DMA(shape)

        wide = 2 * tile
        scratch = [
            buf(*flow.shape), buf(*chl.shape), buf(*tracers.shape), buf(*forcing.shape),
            pltpu.VMEM((3, tile, cols), jnp.int32), pltpu.VMEM((3, tile, cols), jnp.int32),
            pltpu.SMEM(reaction.shape, f32), sem(8),
            buf(*flow.shape), buf(*chl.shape), buf(*flow.shape), buf(*flow.shape), pltpu.VMEM((wide, cols), jnp.int32),
            buf(SUB, wide, cols), buf(wide, cols), buf(wide, cols),
            buf(SUB, wide, cols), buf(wide, cols), buf(wide, cols), buf(3, levels, wide, yt),
            buf(levels, 3, 4, tile, yt), buf(levels, 3, 2, 1, yt), buf(levels, 3, 4, tile, yt),
            buf(2, levels, nt + 1, 1, yt), buf(levels, tile, yt), buf(2, levels, nt + 1, 1, yt), buf(2, levels, tile, yt),
            buf(2, levels, nt, 1, yt), buf(levels, tile, yt), buf(2, levels, nt, 1, yt), buf(2, levels, tile, yt),
            buf(nt, levels, tile, yt), buf(levels, tile, yt),
            buf(levels, 4, tile, yt), buf(levels, 2, 1, yt), buf(levels, tile, yt),
            sem(2, levels), sem(2, levels), sem(2, levels), sem(2, levels), sem(2, levels), sem(2, levels),
            sem(2), sem(2), sem(2), sem(2),
            sem(2), sem(2), sem(2), sem(2),
            sem(3, levels), sem(3, 3, levels),
            sem(3, levels), sem(levels), sem(3, levels), sem(levels), sem(3, levels), sem(levels),
            sem(levels), sem(3, levels), pltpu.SemaphoreType.REGULAR,
        ]
        vmem = pl.BlockSpec(memory_space=pltpu.VMEM)
        shapes = [x.shape for x in (flow, chl, tracers, forcing)]
        room = 67043328 - 4 * sum(math.prod(x) for x in shapes) - 2**16
        results = pl.pallas_call(
            functools.partial(kernel, sizes),
            out_shape=[pltpu.VMEM(x, f32) for x in shapes],
            in_specs=[pl.BlockSpec(memory_space=pltpu.HBM)] * 7,
            out_specs=[vmem] * 4,
            scratch_shapes=scratch,
            compiler_params=pltpu.CompilerParams(collective_id=0, has_side_effects=True, vmem_limit_bytes=room),
        )(flow, chl, tracers, forcing, ocean, bottom, reaction)
        return pl.pallas_call(
            write_out,
            out_shape=[jax.ShapeDtypeStruct(x, f32) for x in shapes],
            in_specs=[vmem] * 4,
            out_specs=[pl.BlockSpec(memory_space=pltpu.HBM)] * 4,
            scratch_shapes=[sem(4)],
            compiler_params=pltpu.CompilerParams(vmem_limit_bytes=4 * 2**20),
        )(*results)

    rows4 = P(None, None, AXES, None)
    rows3 = P(None, AXES, None)
    return jax.shard_map(on_device, mesh=mesh, in_specs=(rows4, rows3, rows4, rows4, P(), P(), P()),
                         out_specs=(rows4, rows3, rows4, rows4), check_vma=False)
```

```python
import functools
import math

import jax
import jax.numpy as jnp
from jax import lax
from jax.experimental import pallas as pl
from jax.experimental.pallas import tpu as pltpu
from jax.sharding import PartitionSpec as P

SUB = 4
MESH = pl.DeviceIdType.MESH
AXES = ("comp", "gy", "gx")


def substep(state, above, heat, wet, first, last):
    u, v, t, s = state
    rows, cols = u.shape
    p = above + 0.2 * (s - t)

    def row_next(x):
        return pltpu.roll(x, rows - 1, 0)

    def row_prev(x):
        return pltpu.roll(x, 1, 0)

    def col_next(x):
        return jnp.where(last, 0.0, pltpu.roll(x, cols - 1, 1))

    def col_prev(x):
        return jnp.where(first, 0.0, pltpu.roll(x, 1, 1))

    um, up, vm, vp = 1.0 - u, 1.0 + u, 1.0 - v, 1.0 + v
    new_u = 0.79 * u + 0.1 * v + 0.05 * (row_next(u - p) + row_prev(u + p) + col_next(u) + col_prev(u))
    new_v = 0.79 * v - 0.1 * u + 0.05 * (row_next(v) + row_prev(v) + col_next(v - p) + col_prev(v + p))
    new_t = 0.8 * t + 0.05 * (row_next(t * um) + row_prev(t * up) + col_next(t * vm) + col_prev(t * vp)) + heat
    new_s = 0.8 * s + 0.05 * (row_next(s * um) + row_prev(s * up) + col_next(s * vm) + col_prev(s * vp))
    return tuple(jnp.where(wet, x, 0.0) for x in (new_u, new_v, new_t, new_s)), p


D_HALO, D_MID, D_PIG = 0, 1, 2
T_DRIVE = 2
D_LIGHT, D_HALO_S, D_MID_S, D_DRIVE_S, D_DRIVE2_S, D_LOAD, D_MASK = range(7)
(T_ROW, T_COL, T_ROW2, T_COL2, T_ROW_S, T_ROW2_S, T_COL_S, T_COL2_S, T_PIG_S, T_SIDE_S, T_LIGHT_S, T_DRIVE2,
 T_LOAD, T_MASK, T_FORCE, T_REACT, T_HALO_S, T_MID_S) = (0, 1, 2, 3, 4, 5, 6, 8, 10, 11, 12, 13, 14, 15, 16, 17, 18, 19)
N_ONE = 20


def kernel(sizes, flow_h, chl_h, tracers_h, forcing_h, ocean_h, bottom_h, reaction_h,
           flow_out, light_out, tracers_out, forcing_out,
           flow, gflow, mid, gmid, masks, tracers, forcing, reaction, depth, total, optical, light, total2, optical2, light2, pig,
           drive_send, drive2_send, row_send, col_send, row_recv, col_recv, row_send2, col_send2, row_recv2, col_recv2,
           held, pig_s, drive, light_s, level_sem, one_sem, ready):
    n_comp, n_gy, n_gx = sizes
    grid = n_gy * n_gx
    every = n_comp * grid
    group = every // 4
    _, levels, tile, cols = mid.shape
    half = tile // 2
    wide = 2 * tile
    nt = tracers.shape[0]
    yt = tracers.shape[3]
    position = (lax.axis_index("comp") * grid + lax.axis_index("gy") * n_gx + lax.axis_index("gx")).astype(jnp.int32)
    moved = lax.rem(position + 1, jnp.int32(every))
    strip = lax.rem(moved, jnp.int32(group))
    section = lax.div(moved, jnp.int32(group))
    is_dyn = section == 3
    has_lo = strip > 0
    has_hi = strip < group - 1
    has_left = section > 0
    has_right = section < 2

    def dev(sec, row):
        pos = lax.rem(sec * group + row + (every - 1), jnp.int32(every))
        return (lax.div(pos, jnp.int32(grid)), lax.rem(lax.div(pos, jnp.int32(n_gx)), jnp.int32(n_gy)),
                lax.rem(pos, jnp.int32(n_gx)))

    def remote(src, dst, send_sem, recv_sem, target):
        return pltpu.make_async_remote_copy(src_ref=src, dst_ref=dst, send_sem=send_sem, recv_sem=recv_sem,
                                            device_id=target, device_id_type=MESH)

    three = jnp.int32(3)
    scope = jax.named_scope
    barrier = pltpu.get_barrier_semaphore()

    def load(i, src, dst):
        return pltpu.make_async_copy(src, dst, one_sem.at[i])

    def mask_loads(sem, part, offset):
        begin = pl.multiple_of(jnp.clip(strip + offset, 0, group - 1) * tile, tile)
        return [load(sem, h.at[pl.ds(begin, tile), :], masks.at[part, m]) for m, h in enumerate((ocean_h, bottom_h))]

    def greet(sem, sec, row):
        pl.semaphore_signal(sem, inc=1, device_id=dev(sec, row), device_id_type=MESH)

    sides = ((0, -1, has_lo), (1, 1, has_hi))
    lo_n = has_lo.astype(jnp.int32)
    hi_n = has_hi.astype(jnp.int32)

    both = has_lo & has_hi
    rows_drive = 3 * tile + 2

    def for_sides(act):
        pl.when(both)(lambda: act(True))
        pl.when(jnp.logical_not(both))(lambda: act(False))

    def pig_copy(k, sec, part, row):
        from_rows = (pl.ds(0, tile), pl.ds(0, half), pl.ds(half, half))[part]
        to_rows = (pl.ds(0, tile), pl.ds(tile, half), pl.ds(tile + half, half))[part]
        return remote(pig_s.at[k, from_rows], pig.at[sec, k, to_rows], one_sem.at[T_PIG_S if part == 0 else T_SIDE_S],
                      level_sem.at[D_PIG, k], dev(three, row))

    def light_copy(k, sec, begin, row):
        return remote(light_s.at[k], light_out.at[k, :, pl.ds(begin, yt)], one_sem.at[T_LIGHT_S], one_sem.at[D_LIGHT],
                      dev(three, row))

    other = dev(lax.rem(section + 1, jnp.int32(4)), strip)

    def recv(dst, sem):
        remote(dst, dst, sem, sem, other).wait_recv()

    def sent(src, sem):
        remote(src, src, sem, sem, other).wait_send()

    halo_of = ((flow, gflow, D_HALO_S, D_HALO), (mid, gmid, D_MID_S, D_MID))

    def halo_copy(what, k, side, offset):
        own, ghost, send, come = halo_of[what]
        place = pl.ds(half * side, half)
        to = strip + offset
        where = dev(three * jnp.minimum(to, 1), to)
        return remote(own.at[:, k, place, :], ghost.at[:, k, place, :], one_sem.at[send], level_sem.at[come, k], where)

    def relay_copy(what, k):
        _, ghost, _, come = halo_of[what]
        place = pl.ds(0, half)
        return remote(ghost.at[:, k, place, :], ghost.at[:, k, place, :], one_sem.at[(T_HALO_S, T_MID_S)[what]],
                      level_sem.at[come, k], dev(three, strip))

    @pl.when(is_dyn)
    def _():
        loads = [load(D_LOAD, flow_h, flow.at[0:4]), load(D_LOAD, chl_h, flow.at[4])]
        for part in range(3):
            loads.extend(mask_loads(D_MASK, part, part - 1))
        for copy in loads:
            copy.start()
        for _, offset, present in sides:
            @pl.when(present)
            def _():
                greet(barrier, three, strip + offset)
        for place, present in ((half, has_lo), (0, has_hi)):
            @pl.when(jnp.logical_not(present))
            def _():
                for f in range(5):
                    gflow[f, :, place:place + half, :] = jnp.zeros((levels, half, cols), jnp.float32)
                for f in range(4):
                    gmid[f, :, place:place + half, :] = jnp.zeros((levels, half, cols), jnp.float32)
                for sec in range(3):
                    pig[sec, :, tile + place:tile + place + half, :] = jnp.zeros((levels, half, yt), jnp.float32)
        total[...] = jnp.zeros_like(total)
        total2[...] = jnp.zeros_like(total2)
        optical[...] = jnp.zeros_like(optical)
        optical2[...] = jnp.zeros_like(optical2)
        light[...] = jnp.ones_like(light)
        light2[...] = jnp.ones_like(light2)
        with scope("d_load"):
            load(D_LOAD, flow, flow).wait()
            load(D_MASK, masks, masks).wait()
        with scope("d_bar"):
            pl.semaphore_wait(barrier, 3 + 4 * lo_n + 4 * hi_n)

        def drive_copy(k, sec):
            return remote(drive_send.at[k, sec, pl.ds(0, rows_drive)], drive.at[k, pl.ds(0, rows_drive)],
                          one_sem.at[D_DRIVE_S], level_sem.at[T_DRIVE, k], dev(jnp.int32(sec), strip))

        def edge_copy(k, sec, side, offset):
            return remote(drive_send.at[k, sec, pl.ds(side * (tile - 1), 1)], drive.at[k, pl.ds(rows_drive + 1 - side, 1)],
                          one_sem.at[D_DRIVE_S], level_sem.at[T_DRIVE, k], dev(jnp.int32(sec), strip + offset))

        def drive2_copy(k, sec):
            return remote(drive2_send.at[k, sec], forcing_out.at[:, k], one_sem.at[D_DRIVE2_S], one_sem.at[T_DRIVE2],
                          dev(jnp.int32(sec), strip))

        @pl.loop(0, levels)
        def _(k):
            for side, offset, present in sides:
                @pl.when(present)
                def _():
                    halo_copy(0, k, side, offset).start()

        for sec in range(3):
            greet(ready, jnp.int32(sec), strip)
            for _, offset, present in sides:
                @pl.when(present)
                def _():
                    greet(ready, jnp.int32(sec), strip + offset)

        def deep_of(part):
            return jnp.where(masks[part, 0] == 1, masks[part, 1], 0)

        row_d = lax.broadcasted_iota(jnp.int32, (tile, cols), 0)
        depth[0:tile, :] = deep_of(1)
        depth[tile:wide, :] = jnp.where(row_d < half, deep_of(2) * hi_n, deep_of(0) * lo_n)
        tracers_out[...] = jnp.zeros_like(tracers_out)
        forcing_out[...] = jnp.zeros_like(forcing_out)

        on_diagonal = lax.broadcasted_iota(jnp.int32, (tile, yt), 0) == lax.broadcasted_iota(jnp.int32, (tile, yt), 1)
        lane_d = lax.broadcasted_iota(jnp.int32, (wide, cols), 1)

        def phase(k, now, pigment, sums, opt_s, light_ref):
            first, last = lane_d == 0, lane_d == cols - 1
            opt = opt_s[...] + (0.05 + 0.3 * pigment)
            lower = jnp.exp(-opt)
            heat = 0.5 * (light_ref[...] - lower)
            opt_s[...] = opt
            light_ref[...] = lower
            wet = k < depth[...]
            sum_u = None
            for n in range(SUB):
                now, p = substep(now, sums[n], heat, wet, first, last)
                sums[n] = p
                sum_u = now[0] if n == 0 else sum_u + now[0]
                sum_v = now[1] if n == 0 else sum_v + now[1]
            return now, sum_u * (1.0 / SUB), sum_v[0:tile] * (1.0 / SUB)

        @pl.loop(0, levels)
        def _(k):
            with scope("d_halo"):
                for_sides(lambda two: recv(gflow.at[:, k, pl.ds(0, tile if two else half), :], level_sem.at[D_HALO, k]))
            now = tuple(jnp.concatenate([flow[f, k], gflow[f, k]], axis=0) for f in range(4))
            now, mean_u, mean_v = phase(k, now, jnp.concatenate([flow[4, k], gflow[4, k]], axis=0), total, optical, light)
            for f in range(4):
                mid[f, k] = now[f][0:tile]
            for side, offset, present in sides:
                @pl.when(present)
                def _():
                    halo_copy(1, k, side, offset).start()
            mix = 0.1 * now[2][0:tile] - 0.05 * now[3][0:tile]
            for sec in range(3):
                here = slice(sec * yt, (sec + 1) * yt)
                drive_send[k, sec, 0:tile] = mean_u[0:tile, here]
                drive_send[k, sec, tile:2 * tile] = mean_v[:, here]
                drive_send[k, sec, 2 * tile:3 * tile] = mix[:, here]
                for at, edge, inside in ((0, sec * yt - 1, sec > 0), (1, (sec + 1) * yt, sec < 2)):
                    if inside:
                        spread = jnp.where(on_diagonal, mean_v[:, edge:edge + 1], 0.0)
                        drive_send[k, sec, 3 * tile + at:3 * tile + at + 1] = jnp.sum(spread, axis=0, keepdims=True)
                    else:
                        drive_send[k, sec, 3 * tile + at:3 * tile + at + 1] = jnp.zeros((1, yt), jnp.float32)
            for sec in range(3):
                drive_copy(k, sec).start()
            for side, offset, present in sides:
                @pl.when(present)
                def _():
                    for sec in range(3):
                        edge_copy(k, sec, side, offset).start()

        @pl.loop(0, levels)
        def _(k):
            with scope("d_mid"):
                for_sides(lambda two: recv(gmid.at[:, k, pl.ds(0, tile if two else half), :], level_sem.at[D_MID, k]))
            with scope("d_pig"):
                for_sides(lambda two: recv(pig.at[:, k, pl.ds(0, wide if two else tile + half), :], level_sem.at[D_PIG, k]))
            now = tuple(jnp.concatenate([mid[f, k], gmid[f, k]], axis=0) for f in range(4))
            pigment = jnp.concatenate([pig[sec, k] for sec in range(3)], axis=1)
            now, mean_u, mean_v = phase(k, now, pigment, total2, optical2, light2)
            items = (mean_u[0:tile], mean_v, now[2][0:tile], now[3][0:tile])
            for sec in range(3):
                for f in range(4):
                    drive2_send[k, sec, f] = items[f][:, sec * yt:(sec + 1) * yt]
            drive2_copy(k, 0).start()
            for f in range(4):
                flow_out[f, k] = now[f][0:tile]

        for sec in (1, 2):
            @pl.loop(0, levels)
            def _(k):
                drive2_copy(k, sec).start()

        with scope("d_light"):
            recv(light_out, one_sem.at[D_LIGHT])
        with scope("d_sends"):
            for_sides(lambda two: sent(flow.at[:, :, pl.ds(0, tile if two else half), :], one_sem.at[D_HALO_S]))
            for_sides(lambda two: sent(mid.at[:, :, pl.ds(0, tile if two else half), :], one_sem.at[D_MID_S]))
            for_sides(lambda two: sent(drive_send.at[:, :, pl.ds(0, rows_drive + (2 if two else 1)), :], one_sem.at[D_DRIVE_S]))
            sent(drive2_send, one_sem.at[D_DRIVE2_S])

    @pl.when(jnp.logical_not(is_dyn))
    def _():
        loads = [load(T_LOAD, tracers_h, tracers), load(T_FORCE, forcing_h, forcing), load(T_REACT, reaction_h, reaction)]
        loads.extend(mask_loads(T_MASK, 1, 0))
        for copy in loads:
            copy.start()
        for _, offset, present in sides:
            @pl.when(present)
            def _():
                greet(barrier, section, strip + offset)
                greet(barrier, three, strip + offset)
        greet(barrier, three, strip)
        beside = ((0, -1, has_left), (1, 1, has_right))
        for _, offset, present in beside:
            @pl.when(present)
            def _():
                greet(barrier, section + offset, strip)
        for side, present in ((0, has_lo), (1, has_hi)):
            @pl.when(jnp.logical_not(present))
            def _():
                drive[:, rows_drive + side:rows_drive + side + 1] = jnp.zeros((levels, 1, yt), jnp.float32)
        for side, present, bufs in ((0, has_lo, (row_recv, row_recv2)), (1, has_hi, (row_recv, row_recv2)),
                                    (0, has_left, (col_recv, col_recv2)), (1, has_right, (col_recv, col_recv2))):
            @pl.when(jnp.logical_not(present))
            def _():
                for buf in bufs:
                    buf[side] = jnp.zeros(buf.shape[1:], jnp.float32)

        lane = lax.broadcasted_iota(jnp.int32, (tile, yt), 1)
        row = lax.broadcasted_iota(jnp.int32, (tile, yt), 0)
        pair = lax.div(lane, jnp.int32(2))
        odd = lax.rem(lane, jnp.int32(2)) == 1
        relays = (section == 0) & (strip == 0)

        flow_out[...] = jnp.zeros_like(flow_out)
        light_out[...] = jnp.zeros_like(light_out)
        with scope('t_load'):
            for copy in loads[:3]:
                copy.wait()
            load(T_MASK, masks.at[1], masks.at[1]).wait()

        def pack(items):
            packed = jnp.zeros((tile, yt), jnp.float32)
            for i, x in enumerate(items):
                packed = jnp.where(pair == i, pltpu.roll(x, 2 * i + 1, 1), packed)
            return packed

        @pl.loop(0, levels)
        def _(k):
            items = [tracers[i, k] for i in range(nt)]
            col_send[k] = pack(items + [forcing[1, k]])
            for i, x in enumerate(items + [forcing[0, k]]):
                row_send[0, k, i] = x[0:1]
                row_send[1, k, i] = x[tile - 1:tile]

        left = pl.multiple_of(section * yt, yt)
        deep = jnp.where(masks[1, 0, :, pl.ds(left, yt)] == 1, masks[1, 1, :, pl.ds(left, yt)], 0)
        with scope('t_bar'):
            pl.semaphore_wait(barrier, lo_n + hi_n + has_left.astype(jnp.int32) + has_right.astype(jnp.int32))

        def row_copies(s_buf, r_buf, ss, rs):
            return [(present, remote(s_buf.at[side], r_buf.at[1 - side], one_sem.at[ss], one_sem.at[rs], dev(section, strip + offset)))
                    for side, offset, present in sides]

        def col_copies(s_buf, r_buf, ss, rs):
            return [(present, remote(s_buf, r_buf.at[1 - side], one_sem.at[ss + side], one_sem.at[rs], dev(section + offset, strip)))
                    for side, offset, present in beside]

        exchange_a = ((row_send, row_recv, T_ROW_S, T_ROW), (col_send, col_recv, T_COL_S, T_COL))
        exchange_b = ((row_send2, row_recv2, T_ROW2_S, T_ROW2), (col_send2, col_recv2, T_COL2_S, T_COL2))

        def start(exchange):
            for present, copy in row_copies(*exchange[0]) + col_copies(*exchange[1]):
                pl.when(present)(copy.start)

        def arrive(exchange):
            (_, rows, _, rs), (_, ends, _, cs) = exchange
            for_sides(lambda two: recv(rows if two else rows.at[0], one_sem.at[rs]))
            middle = has_left & has_right
            pl.when(middle)(lambda: recv(ends, one_sem.at[cs]))
            pl.when(jnp.logical_not(middle))(lambda: recv(ends.at[0], one_sem.at[cs]))

        def finish(exchange):
            for_sides(lambda two: sent(exchange[0][0] if two else exchange[0][0].at[0], one_sem.at[exchange[0][2]]))
            for present, copy in col_copies(*exchange[1]):
                pl.when(present)(copy.wait_send)

        def relay(what):
            @pl.when(relays)
            def _():
                @pl.loop(0, levels)
                def _(k):
                    recv(halo_of[what][1].at[:, k, pl.ds(0, half), :], level_sem.at[halo_of[what][3], k])
                    relay_copy(what, k).start()

        with scope("t_ready"):
            start(exchange_a)
            pl.semaphore_wait(ready, 1 + lo_n + hi_n)
        with scope("t_relay"):
            relay(0)
        with scope("t_xa"):
            arrive(exchange_a)

        def tracer_step(k, cs, u, v, growth, u_lo, u_hi, v_edge, rows_of, packed):
            um, up, vm, vp = 1.0 - u, 1.0 + u, 1.0 - v, 1.0 + v
            hi_m, lo_p = 1.0 - u_hi, 1.0 + u_lo
            edge_m, edge_p = 1.0 - v_edge, 1.0 + v_edge
            wet = k < deep
            out = []
            for i in range(nt):
                c = cs[i]
                react = reaction[i, 0] * cs[0]
                for b in range(1, nt):
                    react = react + reaction[i, b] * cs[b]
                nxt = jnp.where(row == tile - 1, rows_of[1, k, i] * hi_m, pltpu.roll(c * um, tile - 1, 0))
                prv = jnp.where(row == 0, rows_of[0, k, i] * lo_p, pltpu.roll(c * up, 1, 0))
                edge = pltpu.roll(packed, yt - (2 * i + 1), 1)
                rgt = pltpu.roll(jnp.where(lane == 0, edge * edge_m, c * vm), yt - 1, 1)
                lft = pltpu.roll(jnp.where(lane == yt - 1, edge * edge_p, c * vp), 1, 1)
                out.append(jnp.where(wet, 0.8 * c + 0.05 * ((nxt + prv) + (rgt + lft)) + growth * react, 0.0))
            return out

        def pig_copies(k):
            return ((None, pig_copy(k, section, 0, strip)), (has_lo, pig_copy(k, section, 1, strip - 1)),
                    (has_hi, pig_copy(k, section, 2, strip + 1)))

        @pl.loop(0, levels)
        def _(k):
            cs = [tracers[i, k] for i in range(nt)]
            packed = jnp.where(odd, col_recv[1, k], col_recv[0, k])
            growth = 0.1 * jnp.exp(0.1 * forcing[2, k] - 0.05 * forcing[3, k])
            v_edge = pltpu.roll(packed, yt - (2 * nt + 1), 1)
            new = tracer_step(k, cs, forcing[0, k], forcing[1, k], growth, row_recv[0, k, nt], row_recv[1, k, nt], v_edge,
                              row_recv, packed)
            pigment = 0.25 * (new[0] * new[0] + new[1] * new[1])
            pig_s[k] = pigment
            for present, copy in pig_copies(k):
                if present is None:
                    copy.start()
                else:
                    pl.when(present)(copy.start)
            for i in range(nt):
                held[i, k] = new[i]
                row_send2[0, k, i] = new[i][0:1]
                row_send2[1, k, i] = new[i][tile - 1:tile]
            col_send2[k] = pack(new)

        start(exchange_b)
        with scope("t_relay2"):
            relay(1)
        with scope('t_xb'):
            arrive(exchange_b)

        @pl.loop(0, levels)
        def _(k):
            with scope("t_drive"):
                for_sides(lambda two: recv(drive.at[k, pl.ds(0, rows_drive + (2 if two else 1))], level_sem.at[T_DRIVE, k]))
            cs = [held[i, k] for i in range(nt)]
            packed = jnp.where(odd, col_recv2[1, k], col_recv2[0, k])
            growth = 0.1 * jnp.exp(drive[k, 2 * tile:3 * tile])
            ends = [jnp.sum(jnp.where(lane == row, drive[k, 3 * tile + at:3 * tile + at + 1], 0.0), axis=1, keepdims=True)
                    for at in range(2)]
            v_edge = jnp.where(lane == 0, ends[1], ends[0])
            new = tracer_step(k, cs, drive[k, 0:tile], drive[k, tile:2 * tile], growth, drive[k, rows_drive:rows_drive + 1],
                              drive[k, rows_drive + 1:rows_drive + 2], v_edge, row_recv2, packed)
            light_s[k] = 0.25 * (new[0] * new[0] + new[1] * new[1])
            light_copy(k, section, left, strip).start()
            for i in range(nt):
                tracers_out[i, k] = new[i]

        with scope("t_drive2"):
            recv(forcing_out, one_sem.at[T_DRIVE2])
        sent(light_s, one_sem.at[T_LIGHT_S])
        sent(pig_s, one_sem.at[T_PIG_S])
        for_sides(lambda two: sent(pig_s if two else pig_s.at[:, pl.ds(0, half)], one_sem.at[T_SIDE_S]))
        finish(exchange_a)
        finish(exchange_b)

        @pl.when(relays)
        def _():
            for what in range(2):
                sent(halo_of[what][1].at[:, :, pl.ds(0, half), :], one_sem.at[(T_HALO_S, T_MID_S)[what]])


def write_out(*refs):
    done = refs[-1]
    copies = [pltpu.make_async_copy(refs[i], refs[4 + i], done.at[i]) for i in range(4)]
    for copy in copies:
        copy.start()
    for copy in copies:
        copy.wait()


def solution(mesh):
    sizes = tuple(mesh.shape[a] for a in AXES)

    def on_device(flow, chl, tracers, forcing, ocean, bottom, reaction):
        levels, tile, cols = chl.shape
        nt, yt = tracers.shape[0], tracers.shape[3]
        f32 = jnp.float32

        def buf(*shape):
            return pltpu.VMEM(shape, f32)

        def sem(*shape):
            return pltpu.SemaphoreType.DMA(shape)

        wide = 2 * tile
        scratch = [
            buf(5, levels, tile, cols), buf(5, levels, tile, cols), buf(*flow.shape), buf(*flow.shape),
            pltpu.VMEM((3, 2, tile, cols), jnp.int32), buf(*tracers.shape), buf(*forcing.shape), pltpu.SMEM(reaction.shape, f32),
            pltpu.VMEM((wide, cols), jnp.int32), buf(SUB, wide, cols), buf(wide, cols), buf(wide, cols),
            buf(SUB, wide, cols), buf(wide, cols), buf(wide, cols), buf(3, levels, wide, yt),
            buf(levels, 3, 4 * tile, yt), buf(levels, 3, 4, tile, yt),
            buf(2, levels, nt + 1, 1, yt), buf(levels, tile, yt), buf(2, levels, nt + 1, 1, yt), buf(2, levels, tile, yt),
            buf(2, levels, nt, 1, yt), buf(levels, tile, yt), buf(2, levels, nt, 1, yt), buf(2, levels, tile, yt),
            buf(nt, levels, tile, yt), buf(levels, tile, yt),
            buf(levels, 4 * tile, yt), buf(levels, tile, yt),
            sem(3, levels), sem(N_ONE), pltpu.SemaphoreType.REGULAR,
        ]
        vmem = pl.BlockSpec(memory_space=pltpu.VMEM)
        shapes = [x.shape for x in (flow, chl, tracers, forcing)]
        room = 67043328 - 4 * sum(math.prod(x) for x in shapes) - 2**16
        results = pl.pallas_call(
            functools.partial(kernel, sizes),
            out_shape=[pltpu.VMEM(x, f32) for x in shapes],
            in_specs=[pl.BlockSpec(memory_space=pltpu.HBM)] * 7,
            out_specs=[vmem] * 4,
            scratch_shapes=scratch,
            compiler_params=pltpu.CompilerParams(collective_id=0, has_side_effects=True, vmem_limit_bytes=room),
        )(flow, chl, tracers, forcing, ocean, bottom, reaction)
        return pl.pallas_call(
            write_out,
            out_shape=[jax.ShapeDtypeStruct(x, f32) for x in shapes],
            in_specs=[vmem] * 4,
            out_specs=[pl.BlockSpec(memory_space=pltpu.HBM)] * 4,
            scratch_shapes=[sem(4)],
            compiler_params=pltpu.CompilerParams(vmem_limit_bytes=4 * 2**20),
        )(*results)

    rows4 = P(None, None, AXES, None)
    rows3 = P(None, AXES, None)
    return jax.shard_map(on_device, mesh=mesh, in_specs=(rows4, rows3, rows4, rows4, P(), P(), P()),
                         out_specs=(rows4, rows3, rows4, rows4), check_vma=False)
```

```python
import functools
import math

import jax
import jax.numpy as jnp
from jax import lax
from jax.experimental import pallas as pl
from jax.experimental.pallas import tpu as pltpu
from jax.sharding import PartitionSpec as P

SUB = 4
MESH = pl.DeviceIdType.MESH
AXES = ("comp", "gy", "gx")


def substep(state, above, heat, wet, first, last, lanes):
    u, v, t, s = state
    rows, cols = u.shape
    p = above + 0.2 * (s - t)

    def row_next(x):
        return pltpu.roll(x, rows - 1, 0)

    def row_prev(x):
        return pltpu.roll(x, 1, 0)

    def col_shift(x, shift, at_edge, step):
        turned = [pltpu.roll(x[:, a:a + lanes], shift, 1) for a in range(0, cols, lanes)]
        beside = [turned[i + step] if 0 <= i + step < len(turned) else 0.0 for i in range(len(turned))]
        return jnp.concatenate([jnp.where(at_edge, b, x) for x, b in zip(turned, beside)], axis=1)

    def col_next(x):
        return col_shift(x, lanes - 1, last, 1)

    def col_prev(x):
        return col_shift(x, 1, first, -1)

    um, up, vm, vp = 1.0 - u, 1.0 + u, 1.0 - v, 1.0 + v
    new_u = 0.79 * u + 0.1 * v + 0.05 * (row_next(u - p) + row_prev(u + p) + col_next(u) + col_prev(u))
    new_v = 0.79 * v - 0.1 * u + 0.05 * (row_next(v) + row_prev(v) + col_next(v - p) + col_prev(v + p))
    new_t = 0.8 * t + 0.05 * (row_next(t * um) + row_prev(t * up) + col_next(t * vm) + col_prev(t * vp)) + heat
    new_s = 0.8 * s + 0.05 * (row_next(s * um) + row_prev(s * up) + col_next(s * vm) + col_prev(s * vp))
    return tuple(jnp.where(wet, x, 0.0) for x in (new_u, new_v, new_t, new_s)), p


D_HALO, D_MID, D_PIG = 0, 1, 2
T_DRIVE, T_ROW2, T_COL2 = 2, 3, 4
D_LIGHT, D_HALO_S, D_MID_S, D_DRIVE_S, D_DRIVE2_S, D_LOAD, D_MASK = range(7)
(T_ROW, T_COL, T_ROW_S, T_ROW2_S, T_COL_S, T_COL2_S, T_PIG_S, T_SIDE_S, T_LIGHT_S, T_DRIVE2,
 T_LOAD, T_MASK, T_FORCE, T_REACT, T_MID_S) = (0, 1, 2, 3, 4, 6, 8, 9, 10, 11, 12, 13, 14, 15, 16)
N_ONE = 17


def kernel(sizes, flow_h, chl_h, tracers_h, forcing_h, ocean_h, bottom_h, reaction_h,
           flow_out, light_out, tracers_out, forcing_out,
           flow, gflow, mid, gmid, masks, tracers, forcing, reaction, depth, total, optical, light, total2, optical2, light2, pig,
           drive_send, drive2_send, row_send, col_send, row_recv, col_recv, row_send2, col_send2, row_recv2, col_recv2,
           held, pig_s, drive, light_s, level_sem, one_sem, ready):
    n_comp, n_gy, n_gx = sizes
    grid = n_gy * n_gx
    every = n_comp * grid
    group = every // 4
    _, levels, tile, cols = mid.shape
    half = tile // 2
    wide = 2 * tile
    nt = tracers.shape[0]
    yt = tracers.shape[3]
    position = (lax.axis_index("comp") * grid + lax.axis_index("gy") * n_gx + lax.axis_index("gx")).astype(jnp.int32)
    moved = lax.rem(position + 1, jnp.int32(every))
    strip = lax.rem(moved, jnp.int32(group))
    section = lax.div(moved, jnp.int32(group))
    is_dyn = section == 3
    has_lo = strip > 0
    has_hi = strip < group - 1
    has_left = section > 0
    has_right = section < 2

    def dev(sec, row):
        pos = lax.rem(sec * group + row + (every - 1), jnp.int32(every))
        return (lax.div(pos, jnp.int32(grid)), lax.rem(lax.div(pos, jnp.int32(n_gx)), jnp.int32(n_gy)),
                lax.rem(pos, jnp.int32(n_gx)))

    def remote(src, dst, send_sem, recv_sem, target):
        return pltpu.make_async_remote_copy(src_ref=src, dst_ref=dst, send_sem=send_sem, recv_sem=recv_sem,
                                            device_id=target, device_id_type=MESH)

    three = jnp.int32(3)
    scope = jax.named_scope
    barrier = pltpu.get_barrier_semaphore()

    def load(i, src, dst):
        return pltpu.make_async_copy(src, dst, one_sem.at[i])

    def mask_loads(sem, part, offset):
        begin = pl.multiple_of(jnp.clip(strip + offset, 0, group - 1) * tile, tile)
        return [load(sem, h.at[pl.ds(begin, tile), :], masks.at[part, m]) for m, h in enumerate((ocean_h, bottom_h))]

    def greet(sem, sec, row):
        pl.semaphore_signal(sem, inc=1, device_id=dev(sec, row), device_id_type=MESH)

    sides = ((0, -1, has_lo), (1, 1, has_hi))
    lo_n = has_lo.astype(jnp.int32)
    hi_n = has_hi.astype(jnp.int32)

    both = has_lo & has_hi
    rows_drive = 3 * tile + 2

    def for_sides(act):
        pl.when(both)(lambda: act(True))
        pl.when(jnp.logical_not(both))(lambda: act(False))

    def pig_copy(k, sec, part, row):
        from_rows = (pl.ds(0, tile), pl.ds(0, half), pl.ds(half, half))[part]
        to_rows = (pl.ds(0, tile), pl.ds(tile, half), pl.ds(tile + half, half))[part]
        return remote(pig_s.at[k, from_rows], pig.at[sec, k, to_rows], one_sem.at[T_PIG_S if part == 0 else T_SIDE_S],
                      level_sem.at[D_PIG, k], dev(three, row))

    def light_copy(k, sec, begin, row):
        return remote(light_s.at[k], light_out.at[k, :, pl.ds(begin, yt)], one_sem.at[T_LIGHT_S], one_sem.at[D_LIGHT],
                      dev(three, row))

    other = dev(lax.rem(section + 1, jnp.int32(4)), strip)

    def recv(dst, sem):
        remote(dst, dst, sem, sem, other).wait_recv()

    def sent(src, sem):
        remote(src, src, sem, sem, other).wait_send()

    halo_of = ((flow, gflow, D_HALO_S, D_HALO), (mid, gmid, D_MID_S, D_MID))

    def halo_copy(what, k, side, offset):
        own, ghost, send, come = halo_of[what]
        place = pl.ds(half * side, half)
        to = strip + offset
        where = dev(three * jnp.minimum(to, 1) if what == 1 else three, to)
        return remote(own.at[:, k, place, :], ghost.at[:, k, place, :], one_sem.at[send], level_sem.at[come, k], where)

    def relay_copy(k):
        place = pl.ds(0, half)
        return remote(gmid.at[:, k, place, :], gmid.at[:, k, place, :], one_sem.at[T_MID_S], level_sem.at[D_MID, k],
                      dev(three, strip))

    @pl.when(is_dyn)
    def _():
        loads = [load(D_LOAD, flow_h, flow.at[0:4]), load(D_LOAD, chl_h, flow.at[4])]
        for part in range(3):
            loads.extend(mask_loads(D_MASK, part, part - 1))
        for copy in loads:
            copy.start()
        for _, offset, present in sides:
            @pl.when(present)
            def _():
                greet(barrier, three, strip + offset)
        for place, present in ((half, has_lo), (0, has_hi)):
            @pl.when(jnp.logical_not(present))
            def _():
                for f in range(5):
                    gflow[f, :, place:place + half, :] = jnp.zeros((levels, half, cols), jnp.float32)
                for f in range(4):
                    gmid[f, :, place:place + half, :] = jnp.zeros((levels, half, cols), jnp.float32)
                for sec in range(3):
                    pig[sec, :, tile + place:tile + place + half, :] = jnp.zeros((levels, half, yt), jnp.float32)
        total[...] = jnp.zeros_like(total)
        total2[...] = jnp.zeros_like(total2)
        optical[...] = jnp.zeros_like(optical)
        optical2[...] = jnp.zeros_like(optical2)
        light[...] = jnp.ones_like(light)
        light2[...] = jnp.ones_like(light2)
        with scope("d_load"):
            load(D_LOAD, flow, flow).wait()
            load(D_MASK, masks, masks).wait()
        with scope("d_bar"):
            pl.semaphore_wait(barrier, 3 + 4 * lo_n + 4 * hi_n)

        def drive_copy(k, sec):
            return remote(drive_send.at[k, sec, pl.ds(0, rows_drive)], drive.at[k, pl.ds(0, rows_drive)],
                          one_sem.at[D_DRIVE_S], level_sem.at[T_DRIVE, k], dev(jnp.int32(sec), strip))

        def edge_copy(k, sec, side, offset):
            return remote(drive_send.at[k, sec, pl.ds(side * (tile - 1), 1)], drive.at[k, pl.ds(rows_drive + 1 - side, 1)],
                          one_sem.at[D_DRIVE_S], level_sem.at[T_DRIVE, k], dev(jnp.int32(sec), strip + offset))

        def drive2_copy(k, sec):
            return remote(drive2_send.at[k, sec], forcing_out.at[:, k], one_sem.at[D_DRIVE2_S], one_sem.at[T_DRIVE2],
                          dev(jnp.int32(sec), strip))

        @pl.loop(0, levels)
        def _(k):
            for side, offset, present in sides:
                @pl.when(present)
                def _():
                    halo_copy(0, k, side, offset).start()

        for sec in range(3):
            greet(ready, jnp.int32(sec), strip)
            for _, offset, present in sides:
                @pl.when(present)
                def _():
                    greet(ready, jnp.int32(sec), strip + offset)

        def deep_of(part):
            return jnp.where(masks[part, 0] == 1, masks[part, 1], 0)

        row_d = lax.broadcasted_iota(jnp.int32, (tile, cols), 0)
        depth[0:tile, :] = deep_of(1)
        depth[tile:wide, :] = jnp.where(row_d < half, deep_of(2) * hi_n, deep_of(0) * lo_n)
        tracers_out[...] = jnp.zeros_like(tracers_out)
        forcing_out[...] = jnp.zeros_like(forcing_out)

        on_diagonal = lax.broadcasted_iota(jnp.int32, (tile, yt), 0) == lax.broadcasted_iota(jnp.int32, (tile, yt), 1)
        lane_d = lax.broadcasted_iota(jnp.int32, (wide, yt), 1)

        def phase(k, now, pigment, sums, opt_s, light_ref):
            first, last = lane_d == 0, lane_d == yt - 1
            opt = opt_s[...] + (0.05 + 0.3 * pigment)
            lower = jnp.exp(-opt)
            heat = 0.5 * (light_ref[...] - lower)
            opt_s[...] = opt
            light_ref[...] = lower
            wet = k < depth[...]
            sum_u = None
            for n in range(SUB):
                now, p = substep(now, sums[n], heat, wet, first, last, yt)
                sums[n] = p
                sum_u = now[0] if n == 0 else sum_u + now[0]
                sum_v = now[1] if n == 0 else sum_v + now[1]
            return now, sum_u * (1.0 / SUB), sum_v[0:tile] * (1.0 / SUB)

        @pl.loop(0, levels)
        def _(k):
            with scope("d_halo"):
                for_sides(lambda two: recv(gflow.at[:, k, pl.ds(0, tile if two else half), :], level_sem.at[D_HALO, k]))
            now = tuple(jnp.concatenate([flow[f, k], gflow[f, k]], axis=0) for f in range(4))
            now, mean_u, mean_v = phase(k, now, jnp.concatenate([flow[4, k], gflow[4, k]], axis=0), total, optical, light)
            for f in range(4):
                mid[f, k] = now[f][0:tile]
            for side, offset, present in sides:
                @pl.when(present)
                def _():
                    halo_copy(1, k, side, offset).start()
            mix = 0.1 * now[2][0:tile] - 0.05 * now[3][0:tile]
            for sec in range(3):
                here = slice(sec * yt, (sec + 1) * yt)
                drive_send[k, sec, 0:tile] = mean_u[0:tile, here]
                drive_send[k, sec, tile:2 * tile] = mean_v[:, here]
                drive_send[k, sec, 2 * tile:3 * tile] = mix[:, here]
                for at, edge, inside in ((0, sec * yt - 1, sec > 0), (1, (sec + 1) * yt, sec < 2)):
                    if inside:
                        spread = jnp.where(on_diagonal, mean_v[:, edge:edge + 1], 0.0)
                        drive_send[k, sec, 3 * tile + at:3 * tile + at + 1] = jnp.sum(spread, axis=0, keepdims=True)
                    else:
                        drive_send[k, sec, 3 * tile + at:3 * tile + at + 1] = jnp.zeros((1, yt), jnp.float32)
            for sec in range(3):
                drive_copy(k, sec).start()
            for side, offset, present in sides:
                @pl.when(present)
                def _():
                    for sec in range(3):
                        edge_copy(k, sec, side, offset).start()

        @pl.loop(0, levels)
        def _(k):
            with scope("d_mid"):
                for_sides(lambda two: recv(gmid.at[:, k, pl.ds(0, tile if two else half), :], level_sem.at[D_MID, k]))
            with scope("d_pig"):
                for_sides(lambda two: recv(pig.at[:, k, pl.ds(0, wide if two else tile + half), :], level_sem.at[D_PIG, k]))
            now = tuple(jnp.concatenate([mid[f, k], gmid[f, k]], axis=0) for f in range(4))
            pigment = jnp.concatenate([pig[sec, k] for sec in range(3)], axis=1)
            now, mean_u, mean_v = phase(k, now, pigment, total2, optical2, light2)
            items = (mean_u[0:tile], mean_v, now[2][0:tile], now[3][0:tile])
            for sec in range(3):
                for f in range(4):
                    drive2_send[k, sec, f] = items[f][:, sec * yt:(sec + 1) * yt]
            drive2_copy(k, 0).start()
            for f in range(4):
                flow_out[f, k] = now[f][0:tile]

        for sec in (1, 2):
            @pl.loop(0, levels)
            def _(k):
                drive2_copy(k, sec).start()

        with scope("d_light"):
            recv(light_out, one_sem.at[D_LIGHT])
        with scope("d_sends"):
            for_sides(lambda two: sent(flow.at[:, :, pl.ds(0, tile if two else half), :], one_sem.at[D_HALO_S]))
            for_sides(lambda two: sent(mid.at[:, :, pl.ds(0, tile if two else half), :], one_sem.at[D_MID_S]))
            for_sides(lambda two: sent(drive_send.at[:, :, pl.ds(0, rows_drive + (2 if two else 1)), :], one_sem.at[D_DRIVE_S]))
            sent(drive2_send, one_sem.at[D_DRIVE2_S])

    @pl.when(jnp.logical_not(is_dyn))
    def _():
        loads = [load(T_LOAD, tracers_h, tracers), load(T_FORCE, forcing_h, forcing), load(T_REACT, reaction_h, reaction)]
        loads.extend(mask_loads(T_MASK, 1, 0))
        for copy in loads:
            copy.start()
        for _, offset, present in sides:
            @pl.when(present)
            def _():
                greet(barrier, section, strip + offset)
                greet(barrier, three, strip + offset)
        greet(barrier, three, strip)
        beside = ((0, -1, has_left), (1, 1, has_right))
        for _, offset, present in beside:
            @pl.when(present)
            def _():
                greet(barrier, section + offset, strip)
        for side, present in ((0, has_lo), (1, has_hi)):
            @pl.when(jnp.logical_not(present))
            def _():
                drive[:, rows_drive + side:rows_drive + side + 1] = jnp.zeros((levels, 1, yt), jnp.float32)
        for side, present, bufs in ((0, has_lo, (row_recv, row_recv2)), (1, has_hi, (row_recv, row_recv2)),
                                    (0, has_left, (col_recv, col_recv2)), (1, has_right, (col_recv, col_recv2))):
            @pl.when(jnp.logical_not(present))
            def _():
                for buf in bufs:
                    buf[side] = jnp.zeros(buf.shape[1:], jnp.float32)

        lane = lax.broadcasted_iota(jnp.int32, (tile, yt), 1)
        row = lax.broadcasted_iota(jnp.int32, (tile, yt), 0)
        pair = lax.div(lane, jnp.int32(2))
        odd = lax.rem(lane, jnp.int32(2)) == 1
        relays = (section == 0) & (strip == 0)

        flow_out[...] = jnp.zeros_like(flow_out)
        light_out[...] = jnp.zeros_like(light_out)
        with scope('t_load'):
            for copy in loads[:3]:
                copy.wait()
            load(T_MASK, masks.at[1], masks.at[1]).wait()

        def pack(items):
            packed = jnp.zeros((tile, yt), jnp.float32)
            for i, x in enumerate(items):
                packed = jnp.where(pair == i, pltpu.roll(x, 2 * i + 1, 1), packed)
            return packed

        @pl.loop(0, levels)
        def _(k):
            items = [tracers[i, k] for i in range(nt)]
            col_send[k] = pack(items + [forcing[1, k]])
            for i, x in enumerate(items + [forcing[0, k]]):
                row_send[0, k, i] = x[0:1]
                row_send[1, k, i] = x[tile - 1:tile]

        left = pl.multiple_of(section * yt, yt)
        deep = jnp.where(masks[1, 0, :, pl.ds(left, yt)] == 1, masks[1, 1, :, pl.ds(left, yt)], 0)
        with scope('t_bar'):
            pl.semaphore_wait(barrier, lo_n + hi_n + has_left.astype(jnp.int32) + has_right.astype(jnp.int32))

        def copies(rows_s, rows_r, cols_s, cols_r, row_ss, row_rs, col_ss, col_rs):
            for side, offset, present in sides:
                yield present, remote(rows_s.at[side], rows_r.at[1 - side], one_sem.at[row_ss], row_rs, dev(section, strip + offset))
            for side, offset, present in beside:
                yield present, remote(cols_s, cols_r.at[1 - side], one_sem.at[col_ss + side], col_rs, dev(section + offset, strip))

        def exchange_a():
            return copies(row_send, row_recv, col_send, col_recv, T_ROW_S, one_sem.at[T_ROW], T_COL_S, one_sem.at[T_COL])

        def exchange_b(k):
            return copies(row_send2.at[:, k], row_recv2.at[:, k], col_send2.at[k], col_recv2.at[:, k],
                          T_ROW2_S, level_sem.at[T_ROW2, k], T_COL2_S, level_sem.at[T_COL2, k])

        def start(exchange):
            for present, copy in exchange:
                pl.when(present)(copy.start)

        def arrive(rows_r, cols_r, row_rs, col_rs):
            for_sides(lambda two: recv(rows_r if two else rows_r.at[0], row_rs))
            middle = has_left & has_right
            pl.when(middle)(lambda: recv(cols_r, col_rs))
            pl.when(jnp.logical_not(middle))(lambda: recv(cols_r.at[0], col_rs))

        def finish(rows_s, cols_s, row_ss, col_ss):
            for_sides(lambda two: sent(rows_s if two else rows_s.at[0], one_sem.at[row_ss]))
            for side, _, present in beside:
                pl.when(present)(lambda side=side: sent(cols_s, one_sem.at[col_ss + side]))

        with scope("t_ready"):
            start(exchange_a())
            pl.semaphore_wait(ready, 1 + lo_n + hi_n)
        with scope("t_xa"):
            arrive(row_recv, col_recv, one_sem.at[T_ROW], one_sem.at[T_COL])

        def tracer_step(k, cs, u, v, growth, u_lo, u_hi, v_edge, rows_of, packed):
            um, up, vm, vp = 1.0 - u, 1.0 + u, 1.0 - v, 1.0 + v
            hi_m, lo_p = 1.0 - u_hi, 1.0 + u_lo
            edge_m, edge_p = 1.0 - v_edge, 1.0 + v_edge
            wet = k < deep
            out = []
            for i in range(nt):
                c = cs[i]
                react = reaction[i, 0] * cs[0]
                for b in range(1, nt):
                    react = react + reaction[i, b] * cs[b]
                nxt = jnp.where(row == tile - 1, rows_of[1, k, i] * hi_m, pltpu.roll(c * um, tile - 1, 0))
                prv = jnp.where(row == 0, rows_of[0, k, i] * lo_p, pltpu.roll(c * up, 1, 0))
                edge = pltpu.roll(packed, yt - (2 * i + 1), 1)
                rgt = pltpu.roll(jnp.where(lane == 0, edge * edge_m, c * vm), yt - 1, 1)
                lft = pltpu.roll(jnp.where(lane == yt - 1, edge * edge_p, c * vp), 1, 1)
                out.append(jnp.where(wet, 0.8 * c + 0.05 * ((nxt + prv) + (rgt + lft)) + growth * react, 0.0))
            return out

        def pig_copies(k):
            return ((None, pig_copy(k, section, 0, strip)), (has_lo, pig_copy(k, section, 1, strip - 1)),
                    (has_hi, pig_copy(k, section, 2, strip + 1)))

        @pl.loop(0, levels)
        def _(k):
            cs = [tracers[i, k] for i in range(nt)]
            packed = jnp.where(odd, col_recv[1, k], col_recv[0, k])
            growth = 0.1 * jnp.exp(0.1 * forcing[2, k] - 0.05 * forcing[3, k])
            v_edge = pltpu.roll(packed, yt - (2 * nt + 1), 1)
            new = tracer_step(k, cs, forcing[0, k], forcing[1, k], growth, row_recv[0, k, nt], row_recv[1, k, nt], v_edge,
                              row_recv, packed)
            pigment = 0.25 * (new[0] * new[0] + new[1] * new[1])
            pig_s[k] = pigment
            for present, copy in pig_copies(k):
                if present is None:
                    copy.start()
                else:
                    pl.when(present)(copy.start)
            for i in range(nt):
                held[i, k] = new[i]
                row_send2[0, k, i] = new[i][0:1]
                row_send2[1, k, i] = new[i][tile - 1:tile]
            col_send2[k] = pack(new)
            start(exchange_b(k))

        with scope("t_relay2"):
            @pl.when(relays)
            def _():
                @pl.loop(0, levels)
                def _(k):
                    recv(gmid.at[:, k, pl.ds(0, half), :], level_sem.at[D_MID, k])
                    relay_copy(k).start()

        @pl.loop(0, levels)
        def _(k):
            with scope("t_xb"):
                arrive(row_recv2.at[:, k], col_recv2.at[:, k], level_sem.at[T_ROW2, k], level_sem.at[T_COL2, k])
            with scope("t_drive"):
                for_sides(lambda two: recv(drive.at[k, pl.ds(0, rows_drive + (2 if two else 1))], level_sem.at[T_DRIVE, k]))
            cs = [held[i, k] for i in range(nt)]
            packed = jnp.where(odd, col_recv2[1, k], col_recv2[0, k])
            growth = 0.1 * jnp.exp(drive[k, 2 * tile:3 * tile])
            ends = [jnp.sum(jnp.where(lane == row, drive[k, 3 * tile + at:3 * tile + at + 1], 0.0), axis=1, keepdims=True)
                    for at in range(2)]
            v_edge = jnp.where(lane == 0, ends[1], ends[0])
            new = tracer_step(k, cs, drive[k, 0:tile], drive[k, tile:2 * tile], growth, drive[k, rows_drive:rows_drive + 1],
                              drive[k, rows_drive + 1:rows_drive + 2], v_edge, row_recv2, packed)
            light_s[k] = 0.25 * (new[0] * new[0] + new[1] * new[1])
            light_copy(k, section, left, strip).start()
            for i in range(nt):
                tracers_out[i, k] = new[i]

        with scope("t_drive2"):
            recv(forcing_out, one_sem.at[T_DRIVE2])
        sent(light_s, one_sem.at[T_LIGHT_S])
        sent(pig_s, one_sem.at[T_PIG_S])
        for_sides(lambda two: sent(pig_s if two else pig_s.at[:, pl.ds(0, half)], one_sem.at[T_SIDE_S]))
        finish(row_send, col_send, T_ROW_S, T_COL_S)
        finish(row_send2, col_send2, T_ROW2_S, T_COL2_S)

        @pl.when(relays)
        def _():
            sent(gmid.at[:, :, pl.ds(0, half), :], one_sem.at[T_MID_S])


def write_out(*refs):
    done = refs[-1]
    copies = [pltpu.make_async_copy(refs[i], refs[4 + i], done.at[i]) for i in range(4)]
    for copy in copies:
        copy.start()
    for copy in copies:
        copy.wait()


def solution(mesh):
    sizes = tuple(mesh.shape[a] for a in AXES)

    def on_device(flow, chl, tracers, forcing, ocean, bottom, reaction):
        levels, tile, cols = chl.shape
        nt, yt = tracers.shape[0], tracers.shape[3]
        f32 = jnp.float32

        def buf(*shape):
            return pltpu.VMEM(shape, f32)

        def sem(*shape):
            return pltpu.SemaphoreType.DMA(shape)

        wide = 2 * tile
        scratch = [
            buf(5, levels, tile, cols), buf(5, levels, tile, cols), buf(*flow.shape), buf(*flow.shape),
            pltpu.VMEM((3, 2, tile, cols), jnp.int32), buf(*tracers.shape), buf(*forcing.shape), pltpu.SMEM(reaction.shape, f32),
            pltpu.VMEM((wide, cols), jnp.int32), buf(SUB, wide, cols), buf(wide, cols), buf(wide, cols),
            buf(SUB, wide, cols), buf(wide, cols), buf(wide, cols), buf(3, levels, wide, yt),
            buf(levels, 3, 4 * tile, yt), buf(levels, 3, 4, tile, yt),
            buf(2, levels, nt + 1, 1, yt), buf(levels, tile, yt), buf(2, levels, nt + 1, 1, yt), buf(2, levels, tile, yt),
            buf(2, levels, nt, 1, yt), buf(levels, tile, yt), buf(2, levels, nt, 1, yt), buf(2, levels, tile, yt),
            buf(nt, levels, tile, yt), buf(levels, tile, yt),
            buf(levels, 4 * tile, yt), buf(levels, tile, yt),
            sem(5, levels), sem(N_ONE), pltpu.SemaphoreType.REGULAR,
        ]
        vmem = pl.BlockSpec(memory_space=pltpu.VMEM)
        shapes = [x.shape for x in (flow, chl, tracers, forcing)]
        room = 67043328 - 4 * sum(math.prod(x) for x in shapes) - 2**16
        results = pl.pallas_call(
            functools.partial(kernel, sizes),
            out_shape=[pltpu.VMEM(x, f32) for x in shapes],
            in_specs=[pl.BlockSpec(memory_space=pltpu.HBM)] * 7,
            out_specs=[vmem] * 4,
            scratch_shapes=scratch,
            compiler_params=pltpu.CompilerParams(collective_id=0, has_side_effects=True, vmem_limit_bytes=room),
        )(flow, chl, tracers, forcing, ocean, bottom, reaction)
        return pl.pallas_call(
            write_out,
            out_shape=[jax.ShapeDtypeStruct(x, f32) for x in shapes],
            in_specs=[vmem] * 4,
            out_specs=[pl.BlockSpec(memory_space=pltpu.HBM)] * 4,
            scratch_shapes=[sem(4)],
            compiler_params=pltpu.CompilerParams(vmem_limit_bytes=4 * 2**20),
        )(*results)

    rows4 = P(None, None, AXES, None)
    rows3 = P(None, AXES, None)
    return jax.shard_map(on_device, mesh=mesh, in_specs=(rows4, rows3, rows4, rows4, P(), P(), P()),
                         out_specs=(rows4, rows3, rows4, rows4), check_vma=False)
```

```python
import functools
import math

import jax
import jax.numpy as jnp
from jax import lax
from jax.experimental import pallas as pl
from jax.experimental.pallas import tpu as pltpu
from jax.sharding import PartitionSpec as P

SUB = 4
MESH = pl.DeviceIdType.MESH
AXES = ("comp", "gy", "gx")


def substep(state, above, heat, wet, first, last, lanes):
    u, v, t, s = state
    rows, cols = u.shape
    p = above + 0.2 * (s - t)

    def row_next(x):
        return pltpu.roll(x, rows - 1, 0)

    def row_prev(x):
        return pltpu.roll(x, 1, 0)

    def col_shift(x, shift, at_edge, step):
        turned = [pltpu.roll(x[:, a:a + lanes], shift, 1) for a in range(0, cols, lanes)]
        beside = [turned[i + step] if 0 <= i + step < len(turned) else 0.0 for i in range(len(turned))]
        return jnp.concatenate([jnp.where(at_edge, b, x) for x, b in zip(turned, beside)], axis=1)

    def col_next(x):
        return col_shift(x, lanes - 1, last, 1)

    def col_prev(x):
        return col_shift(x, 1, first, -1)

    um, up, vm, vp = 1.0 - u, 1.0 + u, 1.0 - v, 1.0 + v
    new_u = 0.79 * u + 0.1 * v + 0.05 * (row_next(u - p) + row_prev(u + p) + col_next(u) + col_prev(u))
    new_v = 0.79 * v - 0.1 * u + 0.05 * (row_next(v) + row_prev(v) + col_next(v - p) + col_prev(v + p))
    new_t = 0.8 * t + 0.05 * (row_next(t * um) + row_prev(t * up) + col_next(t * vm) + col_prev(t * vp)) + heat
    new_s = 0.8 * s + 0.05 * (row_next(s * um) + row_prev(s * up) + col_next(s * vm) + col_prev(s * vp))
    return tuple(jnp.where(wet, x, 0.0) for x in (new_u, new_v, new_t, new_s)), p


D_HALO, D_MID, D_PIG = 0, 1, 2
T_DRIVE, T_ROW2, T_COL2 = 2, 3, 4
D_LIGHT, D_HALO_S, D_MID_S, D_DRIVE_S, D_DRIVE2_S, D_LOAD, D_MASK = range(7)
(T_ROW, T_COL, T_ROW_S, T_ROW2_S, T_COL_S, T_COL2_S, T_PIG_S, T_SIDE_S, T_LIGHT_S, T_DRIVE2,
 T_LOAD, T_MASK, T_FORCE, T_REACT, T_MID_S) = (0, 1, 2, 3, 4, 6, 8, 9, 10, 11, 12, 13, 14, 15, 16)
N_ONE = 17


def kernel(sizes, flow_h, chl_h, tracers_h, forcing_h, ocean_h, bottom_h, reaction_h,
           flow_out, light_out, tracers_out, forcing_out,
           flow, gflow, mid, gmid, masks, tracers, forcing, reaction, depth, total, optical, light, total2, optical2, light2, pig,
           drive_send, drive2_send, row_send, col_send, row_recv, col_recv, row_send2, col_send2, row_recv2, col_recv2,
           held, pig_s, drive, light_s, level_sem, one_sem, ready):
    n_comp, n_gy, n_gx = sizes
    grid = n_gy * n_gx
    every = n_comp * grid
    group = every // 4
    _, levels, tile, cols = mid.shape
    half = tile // 2
    wide = 2 * tile
    nt = tracers.shape[0]
    yt = tracers.shape[3]
    position = (lax.axis_index("comp") * grid + lax.axis_index("gy") * n_gx + lax.axis_index("gx")).astype(jnp.int32)
    moved = lax.rem(position + 1, jnp.int32(every))
    strip = lax.rem(moved, jnp.int32(group))
    section = lax.div(moved, jnp.int32(group))
    is_dyn = section == 3
    has_lo = strip > 0
    has_hi = strip < group - 1
    has_left = section > 0
    has_right = section < 2

    def dev(sec, row):
        pos = lax.rem(sec * group + row + (every - 1), jnp.int32(every))
        return (lax.div(pos, jnp.int32(grid)), lax.rem(lax.div(pos, jnp.int32(n_gx)), jnp.int32(n_gy)),
                lax.rem(pos, jnp.int32(n_gx)))

    def remote(src, dst, send_sem, recv_sem, target):
        return pltpu.make_async_remote_copy(src_ref=src, dst_ref=dst, send_sem=send_sem, recv_sem=recv_sem,
                                            device_id=target, device_id_type=MESH)

    three = jnp.int32(3)
    scope = jax.named_scope
    barrier = pltpu.get_barrier_semaphore()

    def load(i, src, dst):
        return pltpu.make_async_copy(src, dst, one_sem.at[i])

    def mask_loads(sem, part, offset):
        begin = pl.multiple_of(jnp.clip(strip + offset, 0, group - 1) * tile, tile)
        return [load(sem, h.at[pl.ds(begin, tile), :], masks.at[part, m]) for m, h in enumerate((ocean_h, bottom_h))]

    def greet(sem, sec, row):
        pl.semaphore_signal(sem, inc=1, device_id=dev(sec, row), device_id_type=MESH)

    sides = ((0, -1, has_lo), (1, 1, has_hi))
    lo_n = has_lo.astype(jnp.int32)
    hi_n = has_hi.astype(jnp.int32)

    both = has_lo & has_hi
    rows_drive = 3 * tile + 2

    def for_sides(act):
        pl.when(both)(lambda: act(True))
        pl.when(jnp.logical_not(both))(lambda: act(False))

    def pig_copy(k, sec, part, row):
        from_rows = (pl.ds(0, tile), pl.ds(0, half), pl.ds(half, half))[part]
        to_rows = (pl.ds(0, tile), pl.ds(tile, half), pl.ds(tile + half, half))[part]
        return remote(pig_s.at[k, from_rows], pig.at[sec, k, to_rows], one_sem.at[T_PIG_S if part == 0 else T_SIDE_S],
                      level_sem.at[D_PIG, k], dev(three, row))

    def light_copy(k, sec, begin, row):
        return remote(light_s.at[k], light_out.at[k, :, pl.ds(begin, yt)], one_sem.at[T_LIGHT_S], one_sem.at[D_LIGHT],
                      dev(three, row))

    other = dev(lax.rem(section + 1, jnp.int32(4)), strip)

    def recv(dst, sem):
        remote(dst, dst, sem, sem, other).wait_recv()

    def sent(src, sem):
        remote(src, src, sem, sem, other).wait_send()

    halo_of = ((flow, gflow, D_HALO_S, D_HALO), (mid, gmid, D_MID_S, D_MID))

    def halo_copy(what, k, side, offset):
        own, ghost, send, come = halo_of[what]
        place = pl.ds(half * side, half)
        to = strip + offset
        where = dev(three * jnp.minimum(to, 1) if what == 1 else three, to)
        return remote(own.at[:, k, place, :], ghost.at[:, k, place, :], one_sem.at[send], level_sem.at[come, k], where)

    def relay_copy(k):
        place = pl.ds(0, half)
        return remote(gmid.at[:, k, place, :], gmid.at[:, k, place, :], one_sem.at[T_MID_S], level_sem.at[D_MID, k],
                      dev(three, strip))

    @pl.when(is_dyn)
    def _():
        loads = [load(D_LOAD, flow_h, flow.at[0:4]), load(D_LOAD, chl_h, flow.at[4])]
        for part in range(3):
            loads.extend(mask_loads(D_MASK, part, part - 1))
        for copy in loads:
            copy.start()
        for _, offset, present in sides:
            @pl.when(present)
            def _():
                greet(barrier, three, strip + offset)
        for place, present in ((half, has_lo), (0, has_hi)):
            @pl.when(jnp.logical_not(present))
            def _():
                for f in range(5):
                    gflow[f, :, place:place + half, :] = jnp.zeros((levels, half, cols), jnp.float32)
                for f in range(4):
                    gmid[f, :, place:place + half, :] = jnp.zeros((levels, half, cols), jnp.float32)
                for sec in range(3):
                    pig[sec, :, tile + place:tile + place + half, :] = jnp.zeros((levels, half, yt), jnp.float32)
        total[...] = jnp.zeros_like(total)
        total2[...] = jnp.zeros_like(total2)
        optical[...] = jnp.zeros_like(optical)
        optical2[...] = jnp.zeros_like(optical2)
        light[...] = jnp.ones_like(light)
        light2[...] = jnp.ones_like(light2)
        with scope("d_load"):
            load(D_LOAD, flow, flow).wait()
            load(D_MASK, masks, masks).wait()
        with scope("d_bar"):
            pl.semaphore_wait(barrier, 3 + 4 * lo_n + 4 * hi_n)

        def drive_copy(k, sec):
            return remote(drive_send.at[k, sec, pl.ds(0, rows_drive)], drive.at[k, pl.ds(0, rows_drive)],
                          one_sem.at[D_DRIVE_S], level_sem.at[T_DRIVE, k], dev(jnp.int32(sec), strip))

        def edge_copy(k, sec, side, offset):
            return remote(drive_send.at[k, sec, pl.ds(side * (tile - 1), 1)], drive.at[k, pl.ds(rows_drive + 1 - side, 1)],
                          one_sem.at[D_DRIVE_S], level_sem.at[T_DRIVE, k], dev(jnp.int32(sec), strip + offset))

        def drive2_copy(k, sec):
            return remote(drive2_send.at[k, sec], forcing_out.at[:, k], one_sem.at[D_DRIVE2_S], one_sem.at[T_DRIVE2],
                          dev(jnp.int32(sec), strip))

        @pl.loop(0, levels)
        def _(k):
            for side, offset, present in sides:
                @pl.when(present)
                def _():
                    halo_copy(0, k, side, offset).start()

        for sec in range(3):
            greet(ready, jnp.int32(sec), strip)
            for _, offset, present in sides:
                @pl.when(present)
                def _():
                    greet(ready, jnp.int32(sec), strip + offset)

        def deep_of(part):
            return jnp.where(masks[part, 0] == 1, masks[part, 1], 0)

        row_d = lax.broadcasted_iota(jnp.int32, (tile, cols), 0)
        depth[0:tile, :] = deep_of(1)
        depth[tile:wide, :] = jnp.where(row_d < half, deep_of(2) * hi_n, deep_of(0) * lo_n)
        tracers_out[...] = jnp.zeros_like(tracers_out)
        forcing_out[...] = jnp.zeros_like(forcing_out)

        on_diagonal = lax.broadcasted_iota(jnp.int32, (tile, yt), 0) == lax.broadcasted_iota(jnp.int32, (tile, yt), 1)
        lane_d = lax.broadcasted_iota(jnp.int32, (wide, yt), 1)

        def phase(k, now, pigment, sums, opt_s, light_ref):
            first, last = lane_d == 0, lane_d == yt - 1
            opt = opt_s[...] + (0.05 + 0.3 * pigment)
            lower = jnp.exp(-opt)
            heat = 0.5 * (light_ref[...] - lower)
            opt_s[...] = opt
            light_ref[...] = lower
            wet = k < depth[...]
            sum_u = None
            for n in range(SUB):
                now, p = substep(now, sums[n], heat, wet, first, last, yt)
                sums[n] = p
                sum_u = now[0] if n == 0 else sum_u + now[0]
                sum_v = now[1] if n == 0 else sum_v + now[1]
            return now, sum_u * (1.0 / SUB), sum_v[0:tile] * (1.0 / SUB)

        @pl.loop(0, levels)
        def _(k):
            with scope("d_halo"):
                for_sides(lambda two: recv(gflow.at[:, k, pl.ds(0, tile if two else half), :], level_sem.at[D_HALO, k]))
            now = tuple(jnp.concatenate([flow[f, k], gflow[f, k]], axis=0) for f in range(4))
            now, mean_u, mean_v = phase(k, now, jnp.concatenate([flow[4, k], gflow[4, k]], axis=0), total, optical, light)
            for f in range(4):
                mid[f, k] = now[f][0:tile]
            for side, offset, present in sides:
                @pl.when(present)
                def _():
                    halo_copy(1, k, side, offset).start()
            mix = 0.1 * now[2][0:tile] - 0.05 * now[3][0:tile]
            for sec in range(3):
                here = slice(sec * yt, (sec + 1) * yt)
                drive_send[k, sec, 0:tile] = mean_u[0:tile, here]
                drive_send[k, sec, tile:2 * tile] = mean_v[:, here]
                drive_send[k, sec, 2 * tile:3 * tile] = mix[:, here]
                for at, edge, inside in ((0, sec * yt - 1, sec > 0), (1, (sec + 1) * yt, sec < 2)):
                    if inside:
                        spread = jnp.where(on_diagonal, mean_v[:, edge:edge + 1], 0.0)
                        drive_send[k, sec, 3 * tile + at:3 * tile + at + 1] = jnp.sum(spread, axis=0, keepdims=True)
                    else:
                        drive_send[k, sec, 3 * tile + at:3 * tile + at + 1] = jnp.zeros((1, yt), jnp.float32)
            for sec in range(3):
                drive_copy(k, sec).start()
            for side, offset, present in sides:
                @pl.when(present)
                def _():
                    for sec in range(3):
                        edge_copy(k, sec, side, offset).start()

        @pl.loop(0, levels)
        def _(k):
            with scope("d_mid"):
                for_sides(lambda two: recv(gmid.at[:, k, pl.ds(0, tile if two else half), :], level_sem.at[D_MID, k]))
            with scope("d_pig"):
                for_sides(lambda two: recv(pig.at[:, k, pl.ds(0, wide if two else tile + half), :], level_sem.at[D_PIG, k]))
            now = tuple(jnp.concatenate([mid[f, k], gmid[f, k]], axis=0) for f in range(4))
            pigment = jnp.concatenate([pig[sec, k] for sec in range(3)], axis=1)
            now, mean_u, mean_v = phase(k, now, pigment, total2, optical2, light2)
            items = (mean_u[0:tile], mean_v, now[2][0:tile], now[3][0:tile])
            for sec in range(3):
                for f in range(4):
                    drive2_send[k, sec, f] = items[f][:, sec * yt:(sec + 1) * yt]
            drive2_copy(k, 0).start()

            @pl.when(strip == 0)
            def _():
                for sec in (1, 2):
                    drive2_copy(k, sec).start()
            for f in range(4):
                flow_out[f, k] = now[f][0:tile]

        @pl.when(has_lo)
        def _():
            for sec in (1, 2):
                @pl.loop(0, levels)
                def _(k):
                    drive2_copy(k, sec).start()

        with scope("d_light"):
            recv(light_out, one_sem.at[D_LIGHT])
        with scope("d_sends"):
            for_sides(lambda two: sent(flow.at[:, :, pl.ds(0, tile if two else half), :], one_sem.at[D_HALO_S]))
            for_sides(lambda two: sent(mid.at[:, :, pl.ds(0, tile if two else half), :], one_sem.at[D_MID_S]))
            for_sides(lambda two: sent(drive_send.at[:, :, pl.ds(0, rows_drive + (2 if two else 1)), :], one_sem.at[D_DRIVE_S]))
            sent(drive2_send, one_sem.at[D_DRIVE2_S])

    @pl.when(jnp.logical_not(is_dyn))
    def _():
        loads = [load(T_LOAD, tracers_h, tracers), load(T_FORCE, forcing_h, forcing), load(T_REACT, reaction_h, reaction)]
        loads.extend(mask_loads(T_MASK, 1, 0))
        for copy in loads:
            copy.start()
        for _, offset, present in sides:
            @pl.when(present)
            def _():
                greet(barrier, section, strip + offset)
                greet(barrier, three, strip + offset)
        greet(barrier, three, strip)
        beside = ((0, -1, has_left), (1, 1, has_right))
        for _, offset, present in beside:
            @pl.when(present)
            def _():
                greet(barrier, section + offset, strip)
        for side, present in ((0, has_lo), (1, has_hi)):
            @pl.when(jnp.logical_not(present))
            def _():
                drive[:, rows_drive + side:rows_drive + side + 1] = jnp.zeros((levels, 1, yt), jnp.float32)
        for side, present, bufs in ((0, has_lo, (row_recv, row_recv2)), (1, has_hi, (row_recv, row_recv2)),
                                    (0, has_left, (col_recv, col_recv2)), (1, has_right, (col_recv, col_recv2))):
            @pl.when(jnp.logical_not(present))
            def _():
                for buf in bufs:
                    buf[side] = jnp.zeros(buf.shape[1:], jnp.float32)

        lane = lax.broadcasted_iota(jnp.int32, (tile, yt), 1)
        row = lax.broadcasted_iota(jnp.int32, (tile, yt), 0)
        pair = lax.div(lane, jnp.int32(2))
        odd = lax.rem(lane, jnp.int32(2)) == 1
        relays = (section == 0) & (strip == 0)

        flow_out[...] = jnp.zeros_like(flow_out)
        light_out[...] = jnp.zeros_like(light_out)
        with scope('t_load'):
            for copy in loads[:3]:
                copy.wait()
            load(T_MASK, masks.at[1], masks.at[1]).wait()

        def pack(items):
            packed = jnp.zeros((tile, yt), jnp.float32)
            for i, x in enumerate(items):
                packed = jnp.where(pair == i, pltpu.roll(x, 2 * i + 1, 1), packed)
            return packed

        @pl.loop(0, levels)
        def _(k):
            for i, x in enumerate([tracers[i, k] for i in range(nt)] + [forcing[0, k]]):
                row_send[0, k, i] = x[0:1]
                row_send[1, k, i] = x[tile - 1:tile]

        left = pl.multiple_of(section * yt, yt)
        deep = jnp.where(masks[1, 0, :, pl.ds(left, yt)] == 1, masks[1, 1, :, pl.ds(left, yt)], 0)
        with scope('t_bar'):
            pl.semaphore_wait(barrier, lo_n + hi_n + has_left.astype(jnp.int32) + has_right.astype(jnp.int32))

        def row_copies(rows_s, rows_r, row_ss, row_rs):
            for side, offset, present in sides:
                yield present, remote(rows_s.at[side], rows_r.at[1 - side], one_sem.at[row_ss], row_rs, dev(section, strip + offset))

        def col_copies(cols_s, cols_r, col_ss, col_rs):
            for side, offset, present in beside:
                yield present, remote(cols_s, cols_r.at[1 - side], one_sem.at[col_ss + side], col_rs, dev(section + offset, strip))

        def exchange_b(k):
            yield from row_copies(row_send2.at[:, k], row_recv2.at[:, k], T_ROW2_S, level_sem.at[T_ROW2, k])
            yield from col_copies(col_send2.at[k], col_recv2.at[:, k], T_COL2_S, level_sem.at[T_COL2, k])

        def start(exchange):
            for present, copy in exchange:
                pl.when(present)(copy.start)

        def arrive(rows_r, cols_r, row_rs, col_rs):
            for_sides(lambda two: recv(rows_r if two else rows_r.at[0], row_rs))
            middle = has_left & has_right
            pl.when(middle)(lambda: recv(cols_r, col_rs))
            pl.when(jnp.logical_not(middle))(lambda: recv(cols_r.at[0], col_rs))

        def finish(rows_s, cols_s, row_ss, col_ss):
            for_sides(lambda two: sent(rows_s if two else rows_s.at[0], one_sem.at[row_ss]))
            for side, _, present in beside:
                pl.when(present)(lambda side=side: sent(cols_s, one_sem.at[col_ss + side]))

        with scope("t_ready"):
            start(row_copies(row_send, row_recv, T_ROW_S, one_sem.at[T_ROW]))

            @pl.loop(0, levels)
            def _(k):
                col_send[k] = pack([tracers[i, k] for i in range(nt)] + [forcing[1, k]])
                start(col_copies(col_send.at[k], col_recv.at[:, k], T_COL_S, one_sem.at[T_COL]))

            pl.semaphore_wait(ready, 1 + lo_n + hi_n)
        with scope("t_xa"):
            arrive(row_recv, col_recv, one_sem.at[T_ROW], one_sem.at[T_COL])

        def tracer_step(k, which, cs, u, v, growth, u_lo, u_hi, v_edge, rows_of, packed):
            um, up, vm, vp = 1.0 - u, 1.0 + u, 1.0 - v, 1.0 + v
            hi_m, lo_p = 1.0 - u_hi, 1.0 + u_lo
            edge_m, edge_p = 1.0 - v_edge, 1.0 + v_edge
            wet = k < deep
            out = []
            for i in which:
                c = cs[i]
                react = reaction[i, 0] * cs[0]
                for b in range(1, nt):
                    react = react + reaction[i, b] * cs[b]
                nxt = jnp.where(row == tile - 1, rows_of[1, k, i] * hi_m, pltpu.roll(c * um, tile - 1, 0))
                prv = jnp.where(row == 0, rows_of[0, k, i] * lo_p, pltpu.roll(c * up, 1, 0))
                edge = pltpu.roll(packed, yt - (2 * i + 1), 1)
                rgt = pltpu.roll(jnp.where(lane == 0, edge * edge_m, c * vm), yt - 1, 1)
                lft = pltpu.roll(jnp.where(lane == yt - 1, edge * edge_p, c * vp), 1, 1)
                out.append(jnp.where(wet, 0.8 * c + 0.05 * ((nxt + prv) + (rgt + lft)) + growth * react, 0.0))
            return out

        def pig_copies(k):
            return ((None, pig_copy(k, section, 0, strip)), (has_lo, pig_copy(k, section, 1, strip - 1)),
                    (has_hi, pig_copy(k, section, 2, strip + 1)))

        def step_a(k, which):
            cs = [tracers[i, k] for i in range(nt)]
            packed = jnp.where(odd, col_recv[1, k], col_recv[0, k])
            growth = 0.1 * jnp.exp(0.1 * forcing[2, k] - 0.05 * forcing[3, k])
            v_edge = pltpu.roll(packed, yt - (2 * nt + 1), 1)
            return tracer_step(k, which, cs, forcing[0, k], forcing[1, k], growth, row_recv[0, k, nt], row_recv[1, k, nt], v_edge,
                               row_recv, packed)

        @pl.loop(0, levels)
        def _(k):
            new = step_a(k, range(2))
            pig_s[k] = 0.25 * (new[0] * new[0] + new[1] * new[1])
            for present, copy in pig_copies(k):
                if present is None:
                    copy.start()
                else:
                    pl.when(present)(copy.start)
            for i in range(2):
                held[i, k] = new[i]

        @pl.loop(0, levels)
        def _(k):
            new = [held[0, k], held[1, k]] + step_a(k, range(2, nt))
            for i in range(nt):
                held[i, k] = new[i]
                row_send2[0, k, i] = new[i][0:1]
                row_send2[1, k, i] = new[i][tile - 1:tile]
            col_send2[k] = pack(new)
            start(exchange_b(k))

        with scope("t_relay2"):
            @pl.when(relays)
            def _():
                @pl.loop(0, levels)
                def _(k):
                    recv(gmid.at[:, k, pl.ds(0, half), :], level_sem.at[D_MID, k])
                    relay_copy(k).start()

        @pl.loop(0, levels)
        def _(k):
            with scope("t_xb"):
                arrive(row_recv2.at[:, k], col_recv2.at[:, k], level_sem.at[T_ROW2, k], level_sem.at[T_COL2, k])
            with scope("t_drive"):
                for_sides(lambda two: recv(drive.at[k, pl.ds(0, rows_drive + (2 if two else 1))], level_sem.at[T_DRIVE, k]))
            cs = [held[i, k] for i in range(nt)]
            packed = jnp.where(odd, col_recv2[1, k], col_recv2[0, k])
            growth = 0.1 * jnp.exp(drive[k, 2 * tile:3 * tile])
            ends = [jnp.sum(jnp.where(lane == row, drive[k, 3 * tile + at:3 * tile + at + 1], 0.0), axis=1, keepdims=True)
                    for at in range(2)]
            v_edge = jnp.where(lane == 0, ends[1], ends[0])
            new = tracer_step(k, range(nt), cs, drive[k, 0:tile], drive[k, tile:2 * tile], growth, drive[k, rows_drive:rows_drive + 1],
                              drive[k, rows_drive + 1:rows_drive + 2], v_edge, row_recv2, packed)
            light_s[k] = 0.25 * (new[0] * new[0] + new[1] * new[1])
            light_copy(k, section, left, strip).start()
            for i in range(nt):
                tracers_out[i, k] = new[i]

        with scope("t_drive2"):
            recv(forcing_out, one_sem.at[T_DRIVE2])
        sent(light_s, one_sem.at[T_LIGHT_S])
        sent(pig_s, one_sem.at[T_PIG_S])
        for_sides(lambda two: sent(pig_s if two else pig_s.at[:, pl.ds(0, half)], one_sem.at[T_SIDE_S]))
        finish(row_send, col_send, T_ROW_S, T_COL_S)
        finish(row_send2, col_send2, T_ROW2_S, T_COL2_S)

        @pl.when(relays)
        def _():
            sent(gmid.at[:, :, pl.ds(0, half), :], one_sem.at[T_MID_S])


def write_out(*refs):
    done = refs[-1]
    copies = [pltpu.make_async_copy(refs[i], refs[4 + i], done.at[i]) for i in range(4)]
    for copy in copies:
        copy.start()
    for copy in copies:
        copy.wait()


def solution(mesh):
    sizes = tuple(mesh.shape[a] for a in AXES)

    def on_device(flow, chl, tracers, forcing, ocean, bottom, reaction):
        levels, tile, cols = chl.shape
        nt, yt = tracers.shape[0], tracers.shape[3]
        f32 = jnp.float32

        def buf(*shape):
            return pltpu.VMEM(shape, f32)

        def sem(*shape):
            return pltpu.SemaphoreType.DMA(shape)

        wide = 2 * tile
        scratch = [
            buf(5, levels, tile, cols), buf(5, levels, tile, cols), buf(*flow.shape), buf(*flow.shape),
            pltpu.VMEM((3, 2, tile, cols), jnp.int32), buf(*tracers.shape), buf(*forcing.shape), pltpu.SMEM(reaction.shape, f32),
            pltpu.VMEM((wide, cols), jnp.int32), buf(SUB, wide, cols), buf(wide, cols), buf(wide, cols),
            buf(SUB, wide, cols), buf(wide, cols), buf(wide, cols), buf(3, levels, wide, yt),
            buf(levels, 3, 4 * tile, yt), buf(levels, 3, 4, tile, yt),
            buf(2, levels, nt + 1, 1, yt), buf(levels, tile, yt), buf(2, levels, nt + 1, 1, yt), buf(2, levels, tile, yt),
            buf(2, levels, nt, 1, yt), buf(levels, tile, yt), buf(2, levels, nt, 1, yt), buf(2, levels, tile, yt),
            buf(nt, levels, tile, yt), buf(levels, tile, yt),
            buf(levels, 4 * tile, yt), buf(levels, tile, yt),
            sem(5, levels), sem(N_ONE), pltpu.SemaphoreType.REGULAR,
        ]
        vmem = pl.BlockSpec(memory_space=pltpu.VMEM)
        shapes = [x.shape for x in (flow, chl, tracers, forcing)]
        room = 67043328 - 4 * sum(math.prod(x) for x in shapes) - 2**16
        results = pl.pallas_call(
            functools.partial(kernel, sizes),
            out_shape=[pltpu.VMEM(x, f32) for x in shapes],
            in_specs=[pl.BlockSpec(memory_space=pltpu.HBM)] * 7,
            out_specs=[vmem] * 4,
            scratch_shapes=scratch,
            compiler_params=pltpu.CompilerParams(collective_id=0, has_side_effects=True, vmem_limit_bytes=room),
        )(flow, chl, tracers, forcing, ocean, bottom, reaction)
        return pl.pallas_call(
            write_out,
            out_shape=[jax.ShapeDtypeStruct(x, f32) for x in shapes],
            in_specs=[vmem] * 4,
            out_specs=[pl.BlockSpec(memory_space=pltpu.HBM)] * 4,
            scratch_shapes=[sem(4)],
            compiler_params=pltpu.CompilerParams(vmem_limit_bytes=4 * 2**20),
        )(*results)

    rows4 = P(None, None, AXES, None)
    rows3 = P(None, AXES, None)
    return jax.shard_map(on_device, mesh=mesh, in_specs=(rows4, rows3, rows4, rows4, P(), P(), P()),
                         out_specs=(rows4, rows3, rows4, rows4), check_vma=False)
```

```python
import functools
import math

import jax
import jax.numpy as jnp
from jax import lax
from jax.experimental import pallas as pl
from jax.experimental.pallas import tpu as pltpu
from jax.sharding import PartitionSpec as P

SUB = 4
MESH = pl.DeviceIdType.MESH
AXES = ("comp", "gy", "gx")


def substep(state, above, heat, wet, first, last, lanes):
    u, v, t, s = state
    rows, cols = u.shape
    p = above + 0.2 * (s - t)

    def row_next(x):
        return pltpu.roll(x, rows - 1, 0)

    def row_prev(x):
        return pltpu.roll(x, 1, 0)

    def col_shift(x, shift, at_edge, step):
        turned = [pltpu.roll(x[:, a:a + lanes], shift, 1) for a in range(0, cols, lanes)]
        beside = [turned[i + step] if 0 <= i + step < len(turned) else 0.0 for i in range(len(turned))]
        return jnp.concatenate([jnp.where(at_edge, b, x) for x, b in zip(turned, beside)], axis=1)

    def col_next(x):
        return col_shift(x, lanes - 1, last, 1)

    def col_prev(x):
        return col_shift(x, 1, first, -1)

    um, up, vm, vp = 1.0 - u, 1.0 + u, 1.0 - v, 1.0 + v
    new_u = wet * (15.8 * u + 2.0 * v + (row_next(u - p) + row_prev(u + p) + (col_next(u) + col_prev(u))))
    new_v = wet * (15.8 * v - 2.0 * u + (row_next(v) + row_prev(v) + (col_next(v - p) + col_prev(v + p))))
    new_t = wet * (16.0 * t + (row_next(t * um) + row_prev(t * up) + (col_next(t * vm) + col_prev(t * vp)))) + heat
    new_s = wet * (16.0 * s + (row_next(s * um) + row_prev(s * up) + (col_next(s * vm) + col_prev(s * vp))))
    return (new_u, new_v, new_t, new_s), p


D_HALO, D_MID, D_PIG = 0, 1, 2
T_DRIVE, T_ROW2, T_COL2 = 2, 3, 4
D_LIGHT, D_HALO_S, D_MID_S, D_DRIVE_S, D_DRIVE2_S, D_LOAD, D_MASK = range(7)
(T_ROW, T_COL, T_ROW_S, T_ROW2_S, T_COL_S, T_COL2_S, T_PIG_S, T_SIDE_S, T_LIGHT_S, T_DRIVE2,
 T_LOAD, T_MASK, T_FORCE, T_REACT, T_MID_S, T_LEAD, T_LEAD_S, T_EDGE) = (0, 1, 2, 3, 4, 6, 8, 9, 10, 11, 12, 13, 14, 15, 16, 17, 18, 19)
N_ONE = 21


def kernel(sizes, flow_h, chl_h, tracers_h, forcing_h, ocean_h, bottom_h, reaction_h,
           flow_out, light_out, tracers_out, forcing_out,
           flow, gflow, mid, gmid, masks, tracers, forcing, reaction, depth, total, optical, light, total2, optical2, light2, pig,
           drive_send, drive2_send, row_send, col_send, row_recv, col_recv, row_send2, col_send2, row_recv2, col_recv2,
           held, pig_s, drive, light_s, level_sem, one_sem, ready):
    n_comp, n_gy, n_gx = sizes
    grid = n_gy * n_gx
    every = n_comp * grid
    group = every // 4
    _, levels, tile, cols = mid.shape
    half = tile // 2
    wide = 2 * tile
    nt = tracers.shape[0]
    yt = tracers.shape[3]
    position = (lax.axis_index("comp") * grid + lax.axis_index("gy") * n_gx + lax.axis_index("gx")).astype(jnp.int32)
    moved = lax.rem(position + 1, jnp.int32(every))
    strip = lax.rem(moved, jnp.int32(group))
    section = lax.div(moved, jnp.int32(group))
    is_dyn = section == 3
    has_lo = strip > 0
    has_hi = strip < group - 1
    has_left = section > 0
    has_right = section < 2

    def dev(sec, row):
        pos = lax.rem(sec * group + row + (every - 1), jnp.int32(every))
        return (lax.div(pos, jnp.int32(grid)), lax.rem(lax.div(pos, jnp.int32(n_gx)), jnp.int32(n_gy)),
                lax.rem(pos, jnp.int32(n_gx)))

    def remote(src, dst, send_sem, recv_sem, target):
        return pltpu.make_async_remote_copy(src_ref=src, dst_ref=dst, send_sem=send_sem, recv_sem=recv_sem,
                                            device_id=target, device_id_type=MESH)

    three = jnp.int32(3)
    scope = jax.named_scope
    barrier = pltpu.get_barrier_semaphore()

    def load(i, src, dst):
        return pltpu.make_async_copy(src, dst, one_sem.at[i])

    def mask_loads(sem, part, offset):
        begin = pl.multiple_of(jnp.clip(strip + offset, 0, group - 1) * tile, tile)
        return [load(sem, h.at[pl.ds(begin, tile), :], masks.at[part, m]) for m, h in enumerate((ocean_h, bottom_h))]

    def greet(sem, sec, row):
        pl.semaphore_signal(sem, inc=1, device_id=dev(sec, row), device_id_type=MESH)

    sides = ((0, -1, has_lo), (1, 1, has_hi))
    lo_n = has_lo.astype(jnp.int32)
    hi_n = has_hi.astype(jnp.int32)

    both = has_lo & has_hi
    rows_drive = 3 * tile + 1
    batch = levels // 2 if levels % 2 == 0 else levels

    def for_sides(act):
        pl.when(both)(lambda: act(True))
        pl.when(jnp.logical_not(both))(lambda: act(False))

    def pig_copy(k, sec, part, row):
        from_rows = (pl.ds(0, tile), pl.ds(0, half), pl.ds(half, half))[part]
        to_rows = (pl.ds(0, tile), pl.ds(tile, half), pl.ds(tile + half, half))[part]
        return remote(pig_s.at[k, from_rows], pig.at[sec, k, to_rows], one_sem.at[T_PIG_S if part == 0 else T_SIDE_S],
                      level_sem.at[D_PIG, k], dev(three, row))

    def light_copy(k, sec, begin, row):
        return remote(light_s.at[k], light_out.at[k, :, pl.ds(begin, yt)], one_sem.at[T_LIGHT_S], one_sem.at[D_LIGHT],
                      dev(three, row))

    other = dev(lax.rem(section + 1, jnp.int32(4)), strip)

    def recv(dst, sem):
        remote(dst, dst, sem, sem, other).wait_recv()

    def sent(src, sem):
        remote(src, src, sem, sem, other).wait_send()

    halo_of = ((flow, gflow, D_HALO_S, D_HALO), (mid, gmid, D_MID_S, D_MID))

    def halo_copy(what, k, side, offset):
        own, ghost, send, come = halo_of[what]
        place = pl.ds(half * side, half)
        to = strip + offset
        where = dev(three * jnp.minimum(to, 1) if what == 1 else three, to)
        return remote(own.at[:, k, place, :], ghost.at[:, k, place, :], one_sem.at[send], level_sem.at[come, k], where)

    def relay_copy(k):
        place = pl.ds(0, half)
        return remote(gmid.at[:, k, place, :], gmid.at[:, k, place, :], one_sem.at[T_MID_S], level_sem.at[D_MID, k],
                      dev(three, strip))

    @pl.when(is_dyn)
    def _():
        loads = [load(D_LOAD, flow_h, flow.at[0:4]), load(D_LOAD, chl_h, flow.at[4])]
        for part in range(3):
            loads.extend(mask_loads(D_MASK, part, part - 1))
        for copy in loads:
            copy.start()
        for _, offset, present in sides:
            @pl.when(present)
            def _():
                greet(barrier, three, strip + offset)
        for place, present in ((half, has_lo), (0, has_hi)):
            @pl.when(jnp.logical_not(present))
            def _():
                for f in range(5):
                    gflow[f, :, place:place + half, :] = jnp.zeros((levels, half, cols), jnp.float32)
                for f in range(4):
                    gmid[f, :, place:place + half, :] = jnp.zeros((levels, half, cols), jnp.float32)
                for sec in range(3):
                    pig[sec, :, tile + place:tile + place + half, :] = jnp.zeros((levels, half, yt), jnp.float32)
        total[...] = jnp.zeros_like(total)
        total2[...] = jnp.zeros_like(total2)
        optical[...] = jnp.zeros_like(optical)
        optical2[...] = jnp.zeros_like(optical2)
        light[...] = jnp.ones_like(light)
        light2[...] = jnp.ones_like(light2)
        with scope("d_load"):
            load(D_LOAD, flow, flow).wait()
            load(D_MASK, masks, masks).wait()
        with scope("d_bar"):
            pl.semaphore_wait(barrier, 3 + 4 * lo_n + 4 * hi_n)

        def drive_copy(k, sec):
            return remote(drive_send.at[k, sec, pl.ds(0, rows_drive)], drive.at[k, pl.ds(0, rows_drive)],
                          one_sem.at[D_DRIVE_S], level_sem.at[T_DRIVE, k], dev(jnp.int32(sec), strip))

        def edge_copy(k, sec, side, offset):
            span = pl.ds(k + 1 - batch, batch)
            return remote(drive_send.at[span, sec, pl.ds(side * (tile - 1), 1)], drive.at[span, pl.ds(rows_drive + 1 - side, 1)],
                          one_sem.at[D_DRIVE_S], one_sem.at[T_EDGE + lax.div(k, jnp.int32(batch))],
                          dev(jnp.int32(sec), strip + offset))

        def drive2_copy(k, sec):
            return remote(drive2_send.at[k, sec], forcing_out.at[:, k], one_sem.at[D_DRIVE2_S], one_sem.at[T_DRIVE2],
                          dev(jnp.int32(sec), strip))

        @pl.loop(0, levels)
        def _(k):
            for side, offset, present in sides:
                @pl.when(present)
                def _():
                    halo_copy(0, k, side, offset).start()

        for sec in range(3):
            greet(ready, jnp.int32(sec), strip)
            for _, offset, present in sides:
                @pl.when(present)
                def _():
                    greet(ready, jnp.int32(sec), strip + offset)

        def deep_of(part):
            return jnp.where(masks[part, 0] == 1, masks[part, 1], 0)

        row_d = lax.broadcasted_iota(jnp.int32, (tile, cols), 0)
        depth[0:tile, :] = deep_of(1)
        depth[tile:wide, :] = jnp.where(row_d < half, deep_of(2) * hi_n, deep_of(0) * lo_n)
        tracers_out[...] = jnp.zeros_like(tracers_out)
        forcing_out[...] = jnp.zeros_like(forcing_out)

        lane_row = lax.broadcasted_iota(jnp.int32, (tile, yt), 1) - lax.broadcasted_iota(jnp.int32, (tile, yt), 0)
        on_diagonal = [lane_row == tile * c for c in range(4)]
        lane_d = lax.broadcasted_iota(jnp.int32, (wide, yt), 1)

        def phase(k, now, pigment, sums, opt_s, light_ref):
            first, last = lane_d == 0, lane_d == yt - 1
            opt = opt_s[...] + (0.05 + 0.3 * pigment)
            lower = jnp.exp(-opt)
            heat = 0.5 * (light_ref[...] - lower)
            opt_s[...] = opt
            light_ref[...] = lower
            sea = k < depth[...]
            wet = jnp.where(sea, 0.05, 0.0)
            heat = jnp.where(sea, heat, 0.0)
            sum_u = None
            for n in range(SUB):
                now, p = substep(now, sums[n], heat, wet, first, last, yt)
                sums[n] = p
                sum_u = now[0] if n == 0 else sum_u + now[0]
                sum_v = now[1] if n == 0 else sum_v + now[1]
            return now, sum_u * (1.0 / SUB), sum_v[0:tile] * (1.0 / SUB)

        @pl.loop(0, levels)
        def _(k):
            with scope("d_halo"):
                for_sides(lambda two: recv(gflow.at[:, k, pl.ds(0, tile if two else half), :], level_sem.at[D_HALO, k]))
            now = tuple(jnp.concatenate([flow[f, k], gflow[f, k]], axis=0) for f in range(4))
            now, mean_u, mean_v = phase(k, now, jnp.concatenate([flow[4, k], gflow[4, k]], axis=0), total, optical, light)
            for f in range(4):
                mid[f, k] = now[f][0:tile]
            for side, offset, present in sides:
                @pl.when(present)
                def _():
                    halo_copy(1, k, side, offset).start()
            mix = 0.1 * now[2][0:tile] - 0.05 * now[3][0:tile]
            spread = jnp.zeros((tile, yt), jnp.float32)
            for c, edge in enumerate((yt - 1, yt, 2 * yt - 1, 2 * yt)):
                spread = jnp.where(on_diagonal[c], mean_v[:, edge:edge + 1], spread)
            turned = jnp.sum(spread, axis=0, keepdims=True)
            for sec in range(3):
                here = slice(sec * yt, (sec + 1) * yt)
                drive_send[k, sec, 0:tile] = mean_u[0:tile, here]
                drive_send[k, sec, tile:2 * tile] = mean_v[:, here]
                drive_send[k, sec, 2 * tile:3 * tile] = mix[:, here]
                drive_send[k, sec, 3 * tile:rows_drive] = turned
            for sec in range(3):
                drive_copy(k, sec).start()
            for side, offset, present in sides:
                @pl.when(present & (lax.rem(k, jnp.int32(batch)) == batch - 1))
                def _():
                    for sec in range(3):
                        edge_copy(k, sec, side, offset).start()

        @pl.loop(0, levels)
        def _(k):
            with scope("d_mid"):
                for_sides(lambda two: recv(gmid.at[:, k, pl.ds(0, tile if two else half), :], level_sem.at[D_MID, k]))
            with scope("d_pig"):
                for_sides(lambda two: recv(pig.at[:, k, pl.ds(0, wide if two else tile + half), :], level_sem.at[D_PIG, k]))
            now = tuple(jnp.concatenate([mid[f, k], gmid[f, k]], axis=0) for f in range(4))
            pigment = jnp.concatenate([pig[sec, k] for sec in range(3)], axis=1)
            now, mean_u, mean_v = phase(k, now, pigment, total2, optical2, light2)
            items = (mean_u[0:tile], mean_v, now[2][0:tile], now[3][0:tile])
            for sec in range(3):
                for f in range(4):
                    drive2_send[k, sec, f] = items[f][:, sec * yt:(sec + 1) * yt]
            drive2_copy(k, 0).start()

            @pl.when(strip == 0)
            def _():
                for sec in (1, 2):
                    drive2_copy(k, sec).start()
            for f in range(4):
                flow_out[f, k] = now[f][0:tile]

        @pl.when(has_lo)
        def _():
            for sec in (1, 2):
                @pl.loop(0, levels)
                def _(k):
                    drive2_copy(k, sec).start()

        with scope("d_light"):
            recv(light_out, one_sem.at[D_LIGHT])
        with scope("d_sends"):
            for_sides(lambda two: sent(flow.at[:, :, pl.ds(0, tile if two else half), :], one_sem.at[D_HALO_S]))
            for_sides(lambda two: sent(mid.at[:, :, pl.ds(0, tile if two else half), :], one_sem.at[D_MID_S]))
            for_sides(lambda two: sent(drive_send.at[:, :, pl.ds(0, rows_drive + (2 if two else 1)), :], one_sem.at[D_DRIVE_S]))
            sent(drive2_send, one_sem.at[D_DRIVE2_S])

    @pl.when(jnp.logical_not(is_dyn))
    def _():
        loads = [load(T_LOAD, tracers_h, tracers), load(T_FORCE, forcing_h, forcing), load(T_REACT, reaction_h, reaction)]
        loads.extend(mask_loads(T_MASK, 1, 0))
        for copy in loads:
            copy.start()
        for _, offset, present in sides:
            @pl.when(present)
            def _():
                greet(barrier, section, strip + offset)
                greet(barrier, three, strip + offset)
        greet(barrier, three, strip)
        beside = ((0, -1, has_left), (1, 1, has_right))
        for _, offset, present in beside:
            @pl.when(present)
            def _():
                greet(barrier, section + offset, strip)
        for side, present in ((0, has_lo), (1, has_hi)):
            @pl.when(jnp.logical_not(present))
            def _():
                drive[:, rows_drive + side:rows_drive + side + 1] = jnp.zeros((levels, 1, yt), jnp.float32)
        for side, present, bufs in ((0, has_lo, (row_recv, row_recv2)), (1, has_hi, (row_recv, row_recv2)),
                                    (0, has_left, (col_recv, col_recv2)), (1, has_right, (col_recv, col_recv2))):
            @pl.when(jnp.logical_not(present))
            def _():
                for buf in bufs:
                    buf[side] = jnp.zeros(buf.shape[1:], jnp.float32)

        lane = lax.broadcasted_iota(jnp.int32, (tile, yt), 1)
        row = lax.broadcasted_iota(jnp.int32, (tile, yt), 0)
        pair = lax.div(lane, jnp.int32(2))
        odd = lax.rem(lane, jnp.int32(2)) == 1
        relays = (section == 0) & (strip == 0)

        flow_out[...] = jnp.zeros_like(flow_out)
        light_out[...] = jnp.zeros_like(light_out)
        with scope('t_load'):
            for copy in loads[:3]:
                copy.wait()
            load(T_MASK, masks.at[1], masks.at[1]).wait()

        def pack(items):
            packed = jnp.zeros((tile, yt), jnp.float32)
            for i, x in enumerate(items):
                packed = jnp.where(pair == i, pltpu.roll(x, 2 * i + 1, 1), packed)
            return packed

        @pl.loop(0, levels)
        def _(k):
            for i, x in enumerate([forcing[0, k]] + [tracers[i, k] for i in range(nt)]):
                row_send[0, k, i] = x[0:1]
                row_send[1, k, i] = x[tile - 1:tile]

        left = pl.multiple_of(section * yt, yt)
        deep = jnp.where(masks[1, 0, :, pl.ds(left, yt)] == 1, masks[1, 1, :, pl.ds(left, yt)], 0)
        with scope('t_bar'):
            pl.semaphore_wait(barrier, lo_n + hi_n + has_left.astype(jnp.int32) + has_right.astype(jnp.int32))

        def row_copies(rows_s, rows_r, row_ss, row_rs):
            for side, offset, present in sides:
                yield present, remote(rows_s.at[side], rows_r.at[1 - side], one_sem.at[row_ss], row_rs, dev(section, strip + offset))

        def col_copies(cols_s, cols_r, col_ss, col_rs):
            for side, offset, present in beside:
                yield present, remote(cols_s, cols_r.at[1 - side], one_sem.at[col_ss + side], col_rs, dev(section + offset, strip))

        def exchange_b(k):
            yield from row_copies(row_send2.at[:, k], row_recv2.at[:, k], T_ROW2_S, level_sem.at[T_ROW2, k])
            yield from col_copies(col_send2.at[k], col_recv2.at[:, k], T_COL2_S, level_sem.at[T_COL2, k])

        def start(exchange):
            for present, copy in exchange:
                pl.when(present)(copy.start)

        def arrive_rows(rows_r, row_rs):
            for_sides(lambda two: recv(rows_r if two else rows_r.at[0], row_rs))

        def arrive_cols(cols_r, col_rs):
            middle = has_left & has_right
            pl.when(middle)(lambda: recv(cols_r, col_rs))
            pl.when(jnp.logical_not(middle))(lambda: recv(cols_r.at[0], col_rs))

        def finish_rows(rows_s, row_ss):
            for_sides(lambda two: sent(rows_s if two else rows_s.at[0], one_sem.at[row_ss]))

        def finish_cols(cols_s, col_ss):
            for side, _, present in beside:
                pl.when(present)(lambda side=side: sent(cols_s, one_sem.at[col_ss + side]))

        with scope("t_ready"):
            for part, send, come in ((pl.ds(0, 3), T_LEAD_S, T_LEAD), (pl.ds(3, nt - 2), T_ROW_S, T_ROW)):
                start(row_copies(row_send.at[:, :, part], row_recv.at[:, :, part], send, one_sem.at[come]))

            @pl.loop(0, levels)
            def _(k):
                col_send[k] = pack([tracers[i, k] for i in range(nt)] + [forcing[1, k]])
                start(col_copies(col_send.at[k], col_recv.at[:, k], T_COL_S, one_sem.at[T_COL]))

            pl.semaphore_wait(ready, 1 + lo_n + hi_n)
        with scope("t_xa"):
            arrive_rows(row_recv.at[:, :, pl.ds(0, 3)], one_sem.at[T_LEAD])
            arrive_cols(col_recv, one_sem.at[T_COL])

        def tracer_step(k, which, cs, u, v, growth, u_lo, u_hi, v_edge, rows_of, packed):
            um, up, vm, vp = 1.0 - u, 1.0 + u, 1.0 - v, 1.0 + v
            hi_m, lo_p = 1.0 - u_hi, 1.0 + u_lo
            edge_m, edge_p = 1.0 - v_edge, 1.0 + v_edge
            wet = k < deep
            out = []
            for i in which:
                c = cs[i]
                react = reaction[i, 0] * cs[0]
                for b in range(1, nt):
                    react = react + reaction[i, b] * cs[b]
                nxt = jnp.where(row == tile - 1, rows_of[1, k, i] * hi_m, pltpu.roll(c * um, tile - 1, 0))
                prv = jnp.where(row == 0, rows_of[0, k, i] * lo_p, pltpu.roll(c * up, 1, 0))
                edge = pltpu.roll(packed, yt - (2 * i + 1), 1)
                rgt = pltpu.roll(jnp.where(lane == 0, edge * edge_m, c * vm), yt - 1, 1)
                lft = pltpu.roll(jnp.where(lane == yt - 1, edge * edge_p, c * vp), 1, 1)
                out.append(jnp.where(wet, 0.8 * c + 0.05 * ((nxt + prv) + (rgt + lft)) + growth * react, 0.0))
            return out

        def pig_copies(k):
            return ((None, pig_copy(k, section, 0, strip)), (has_lo, pig_copy(k, section, 1, strip - 1)),
                    (has_hi, pig_copy(k, section, 2, strip + 1)))

        def step_a(k, which):
            cs = [tracers[i, k] for i in range(nt)]
            packed = jnp.where(odd, col_recv[1, k], col_recv[0, k])
            growth = 0.1 * jnp.exp(0.1 * forcing[2, k] - 0.05 * forcing[3, k])
            v_edge = pltpu.roll(packed, yt - (2 * nt + 1), 1)
            return tracer_step(k, which, cs, forcing[0, k], forcing[1, k], growth, row_recv[0, k, 0], row_recv[1, k, 0], v_edge,
                               row_recv.at[:, :, pl.ds(1, nt)], packed)

        @pl.loop(0, levels)
        def _(k):
            new = step_a(k, range(2))
            pig_s[k] = 0.25 * (new[0] * new[0] + new[1] * new[1])
            for present, copy in pig_copies(k):
                if present is None:
                    copy.start()
                else:
                    pl.when(present)(copy.start)
            for i in range(2):
                held[i, k] = new[i]

        with scope("t_rest"):
            arrive_rows(row_recv.at[:, :, pl.ds(3, nt - 2)], one_sem.at[T_ROW])

        @pl.loop(0, levels)
        def _(k):
            new = [held[0, k], held[1, k]] + step_a(k, range(2, nt))
            for i in range(nt):
                held[i, k] = new[i]
                row_send2[0, k, i] = new[i][0:1]
                row_send2[1, k, i] = new[i][tile - 1:tile]
            col_send2[k] = pack(new)
            start(exchange_b(k))

        with scope("t_relay"):
            @pl.when(relays)
            def _():
                @pl.loop(0, levels)
                def _(k):
                    recv(gmid.at[:, k, pl.ds(0, half), :], level_sem.at[D_MID, k])
                    relay_copy(k).start()

        @pl.loop(0, levels)
        def _(k):
            with scope("t_xb"):
                arrive_rows(row_recv2.at[:, k], level_sem.at[T_ROW2, k])
                arrive_cols(col_recv2.at[:, k], level_sem.at[T_COL2, k])
            with scope("t_drive"):
                recv(drive.at[k, pl.ds(0, rows_drive)], level_sem.at[T_DRIVE, k])

                @pl.when(lax.rem(k, jnp.int32(batch)) == 0)
                def _():
                    come = one_sem.at[T_EDGE + lax.div(k, jnp.int32(batch))]
                    for_sides(lambda two: recv(drive.at[pl.ds(k, batch), pl.ds(rows_drive, 2 if two else 1)], come))
            cs = [held[i, k] for i in range(nt)]
            packed = jnp.where(odd, col_recv2[1, k], col_recv2[0, k])
            growth = 0.1 * jnp.exp(drive[k, 2 * tile:3 * tile])
            turned = drive[k, 3 * tile:rows_drive]
            ends = [jnp.sum(jnp.where(lane - row == tile * c, turned, 0.0), axis=1, keepdims=True)
                    for c in (2 * section - 2, 2 * section + 1)]
            v_edge = jnp.where(lane == 0, ends[1], ends[0])
            new = tracer_step(k, range(nt), cs, drive[k, 0:tile], drive[k, tile:2 * tile], growth, drive[k, rows_drive:rows_drive + 1],
                              drive[k, rows_drive + 1:rows_drive + 2], v_edge, row_recv2, packed)
            light_s[k] = 0.25 * (new[0] * new[0] + new[1] * new[1])
            light_copy(k, section, left, strip).start()
            for i in range(nt):
                tracers_out[i, k] = new[i]

        with scope("t_drive2"):
            recv(forcing_out, one_sem.at[T_DRIVE2])
        sent(light_s, one_sem.at[T_LIGHT_S])
        sent(pig_s, one_sem.at[T_PIG_S])
        for_sides(lambda two: sent(pig_s if two else pig_s.at[:, pl.ds(0, half)], one_sem.at[T_SIDE_S]))
        finish_rows(row_send.at[:, :, pl.ds(0, 3)], T_LEAD_S)
        finish_rows(row_send.at[:, :, pl.ds(3, nt - 2)], T_ROW_S)
        finish_rows(row_send2, T_ROW2_S)
        finish_cols(col_send, T_COL_S)
        finish_cols(col_send2, T_COL2_S)

        @pl.when(relays)
        def _():
            sent(gmid.at[:, :, pl.ds(0, half), :], one_sem.at[T_MID_S])


def write_out(*refs):
    done = refs[-1]
    copies = [pltpu.make_async_copy(refs[i], refs[4 + i], done.at[i]) for i in range(4)]
    for copy in copies:
        copy.start()
    for copy in copies:
        copy.wait()


def solution(mesh):
    sizes = tuple(mesh.shape[a] for a in AXES)

    def on_device(flow, chl, tracers, forcing, ocean, bottom, reaction):
        levels, tile, cols = chl.shape
        nt, yt = tracers.shape[0], tracers.shape[3]
        f32 = jnp.float32

        def buf(*shape):
            return pltpu.VMEM(shape, f32)

        def sem(*shape):
            return pltpu.SemaphoreType.DMA(shape)

        wide = 2 * tile
        scratch = [
            buf(5, levels, tile, cols), buf(5, levels, tile, cols), buf(*flow.shape), buf(*flow.shape),
            pltpu.VMEM((3, 2, tile, cols), jnp.int32), buf(*tracers.shape), buf(*forcing.shape), pltpu.SMEM(reaction.shape, f32),
            pltpu.VMEM((wide, cols), jnp.int32), buf(SUB, wide, cols), buf(wide, cols), buf(wide, cols),
            buf(SUB, wide, cols), buf(wide, cols), buf(wide, cols), buf(3, levels, wide, yt),
            buf(levels, 3, 4 * tile, yt), buf(levels, 3, 4, tile, yt),
            buf(2, levels, nt + 1, 1, yt), buf(levels, tile, yt), buf(2, levels, nt + 1, 1, yt), buf(2, levels, tile, yt),
            buf(2, levels, nt, 1, yt), buf(levels, tile, yt), buf(2, levels, nt, 1, yt), buf(2, levels, tile, yt),
            buf(nt, levels, tile, yt), buf(levels, tile, yt),
            buf(levels, 4 * tile, yt), buf(levels, tile, yt),
            sem(5, levels), sem(N_ONE), pltpu.SemaphoreType.REGULAR,
        ]
        vmem = pl.BlockSpec(memory_space=pltpu.VMEM)
        shapes = [x.shape for x in (flow, chl, tracers, forcing)]
        room = 67043328 - 4 * sum(math.prod(x) for x in shapes) - 2**16
        results = pl.pallas_call(
            functools.partial(kernel, sizes),
            out_shape=[pltpu.VMEM(x, f32) for x in shapes],
            in_specs=[pl.BlockSpec(memory_space=pltpu.HBM)] * 7,
            out_specs=[vmem] * 4,
            scratch_shapes=scratch,
            compiler_params=pltpu.CompilerParams(collective_id=0, has_side_effects=True, vmem_limit_bytes=room),
        )(flow, chl, tracers, forcing, ocean, bottom, reaction)
        return pl.pallas_call(
            write_out,
            out_shape=[jax.ShapeDtypeStruct(x, f32) for x in shapes],
            in_specs=[vmem] * 4,
            out_specs=[pl.BlockSpec(memory_space=pltpu.HBM)] * 4,
            scratch_shapes=[sem(4)],
            compiler_params=pltpu.CompilerParams(vmem_limit_bytes=4 * 2**20),
        )(*results)

    rows4 = P(None, None, AXES, None)
    rows3 = P(None, AXES, None)
    return jax.shard_map(on_device, mesh=mesh, in_specs=(rows4, rows3, rows4, rows4, P(), P(), P()),
                         out_specs=(rows4, rows3, rows4, rows4), check_vma=False)
```

```python
import functools
import math

import jax
import jax.numpy as jnp
from jax import lax
from jax.experimental import pallas as pl
from jax.experimental.pallas import tpu as pltpu
from jax.sharding import PartitionSpec as P

SUB = 4
AHEAD = 1
MESH = pl.DeviceIdType.MESH
AXES = ("comp", "gy", "gx")


def substep(state, above, heat, wet, first, last, lanes):
    u, v, t, s = state
    rows, cols = u.shape
    p = above + 0.2 * (s - t)

    def row_next(x):
        return pltpu.roll(x, rows - 1, 0)

    def row_prev(x):
        return pltpu.roll(x, 1, 0)

    def col_shift(x, shift, at_edge, step):
        turned = [pltpu.roll(x[:, a:a + lanes], shift, 1) for a in range(0, cols, lanes)]
        beside = [turned[i + step] if 0 <= i + step < len(turned) else 0.0 for i in range(len(turned))]
        return jnp.concatenate([jnp.where(at_edge, b, x) for x, b in zip(turned, beside)], axis=1)

    def col_next(x):
        return col_shift(x, lanes - 1, last, 1)

    def col_prev(x):
        return col_shift(x, 1, first, -1)

    um, up, vm, vp = 1.0 - u, 1.0 + u, 1.0 - v, 1.0 + v
    new_u = wet * (15.8 * u + 2.0 * v + (row_next(u - p) + row_prev(u + p) + (col_next(u) + col_prev(u))))
    new_v = wet * (15.8 * v - 2.0 * u + (row_next(v) + row_prev(v) + (col_next(v - p) + col_prev(v + p))))
    new_t = wet * (16.0 * t + (row_next(t * um) + row_prev(t * up) + (col_next(t * vm) + col_prev(t * vp)))) + heat
    new_s = wet * (16.0 * s + (row_next(s * um) + row_prev(s * up) + (col_next(s * vm) + col_prev(s * vp))))
    return (new_u, new_v, new_t, new_s), p


D_HALO, D_MID, D_PIG = 0, 1, 2
T_EDGES2, T_DRIVE = 0, 2
D_LIGHT, D_LOAD, D_MASK, D_DRIVE_S, D_DRIVE2_S = range(5)
D_HALO_S, D_MID_S = D_LOAD, D_MASK
T_ROW, T_COL, T_LEAD, T_DRIVE2, T_EDGE, _, T_LOAD, T_FORCE, T_REACT, T_MASK, T_COL_S, T_COL2_S, T_MID_S, N_ONE = range(14)
T_ROW_S, T_ROW2_S, T_PIG_S, T_LIGHT_S = T_LOAD, T_FORCE, T_REACT, T_MASK


def pair_of(levels):
    return 2 if levels % 2 == 0 else 1


def kernel(sizes, flow_h, chl_h, tracers_h, forcing_h, ocean_h, bottom_h, reaction_h,
           flow_out, light_out, tracers_out, forcing_out,
           flow, gflow, mid, gmid, masks, tracers, forcing, reaction, depth, total, optical, light, total2, optical2, light2, pig,
           drive_send, drive2_send, row_send, col_send, row_recv, col_recv, row_send2, col_send2, row_recv2, col_recv2,
           held, pig_s, drive, light_s, level_sem, one_sem, ready):
    n_comp, n_gy, n_gx = sizes
    grid = n_gy * n_gx
    every = n_comp * grid
    group = every // 4
    _, levels, tile, cols = mid.shape
    half = tile // 2
    wide = 2 * tile
    nt = tracers.shape[0]
    yt = tracers.shape[3]
    position = (lax.axis_index("comp") * grid + lax.axis_index("gy") * n_gx + lax.axis_index("gx")).astype(jnp.int32)
    moved = lax.rem(position + 1, jnp.int32(every))
    strip = lax.rem(moved, jnp.int32(group))
    section = lax.div(moved, jnp.int32(group))
    is_dyn = section == 3
    has_lo = strip > 0
    has_hi = strip < group - 1
    has_left = section > 0
    has_right = section < 2

    def dev(sec, row):
        pos = lax.rem(sec * group + row + (every - 1), jnp.int32(every))
        return (lax.div(pos, jnp.int32(grid)), lax.rem(lax.div(pos, jnp.int32(n_gx)), jnp.int32(n_gy)),
                lax.rem(pos, jnp.int32(n_gx)))

    def remote(src, dst, send_sem, recv_sem, target):
        return pltpu.make_async_remote_copy(src_ref=src, dst_ref=dst, send_sem=send_sem, recv_sem=recv_sem,
                                            device_id=target, device_id_type=MESH)

    three = jnp.int32(3)
    scope = jax.named_scope
    barrier = pltpu.get_barrier_semaphore()

    def load(i, src, dst):
        return pltpu.make_async_copy(src, dst, one_sem.at[i])

    def mask_loads(sem, part, offset):
        begin = pl.multiple_of(jnp.clip(strip + offset, 0, group - 1) * tile, tile)
        return [load(sem, h.at[pl.ds(begin, tile), :], masks.at[part, m]) for m, h in enumerate((ocean_h, bottom_h))]

    def greet(sem, sec, row):
        pl.semaphore_signal(sem, inc=1, device_id=dev(sec, row), device_id_type=MESH)

    sides = ((0, -1, has_lo), (1, 1, has_hi))
    lo_n = has_lo.astype(jnp.int32)
    hi_n = has_hi.astype(jnp.int32)

    both = has_lo & has_hi
    rows_drive = 3 * tile + 1
    batch = levels // 2 if levels % 2 == 0 else levels

    def for_sides(act):
        pl.when(both)(lambda: act(True))
        pl.when(jnp.logical_not(both))(lambda: act(False))

    def pig_copy(k, sec, part, row):
        from_rows = (pl.ds(0, tile), pl.ds(0, half), pl.ds(half, half))[part]
        to_rows = (pl.ds(0, tile), pl.ds(tile, half), pl.ds(tile + half, half))[part]
        return remote(pig_s.at[k, from_rows], pig.at[sec, k, to_rows], one_sem.at[T_PIG_S],
                      level_sem.at[D_PIG, k], dev(three, row))

    def light_copy(k, sec, begin, row):
        return remote(light_s.at[k], light_out.at[k, :, pl.ds(begin, yt)], one_sem.at[T_LIGHT_S], one_sem.at[D_LIGHT],
                      dev(three, row))

    other = dev(lax.rem(section + 1, jnp.int32(4)), strip)

    def recv(dst, sem):
        remote(dst, dst, sem, sem, other).wait_recv()

    def sent(src, sem):
        remote(src, src, sem, sem, other).wait_send()

    halo_of = ((flow, gflow, D_HALO_S, D_HALO), (mid, gmid, D_MID_S, D_MID))

    def halo_copy(what, k, side, offset):
        own, ghost, send, come = halo_of[what]
        place = pl.ds(half * side, half)
        to = strip + offset
        where = dev(three * jnp.minimum(to, 1) if what == 1 else three, to)
        return remote(own.at[:, k, place, :], ghost.at[:, k, place, :], one_sem.at[send], level_sem.at[come, k], where)

    def relay_copy(k):
        place = pl.ds(0, half)
        return remote(gmid.at[:, k, place, :], gmid.at[:, k, place, :], one_sem.at[T_MID_S], level_sem.at[D_MID, k],
                      dev(three, strip))

    @pl.when(is_dyn)
    def _():
        loads = [load(D_LOAD, flow_h, flow.at[0:4]), load(D_LOAD, chl_h, flow.at[4])]
        for part in range(3):
            loads.extend(mask_loads(D_MASK, part, part - 1))
        for copy in loads:
            copy.start()
        for _, offset, present in sides:
            @pl.when(present)
            def _():
                greet(barrier, three, strip + offset)
        for place, present in ((half, has_lo), (0, has_hi)):
            @pl.when(jnp.logical_not(present))
            def _():
                for f in range(5):
                    gflow[f, :, place:place + half, :] = jnp.zeros((levels, half, cols), jnp.float32)
                for f in range(4):
                    gmid[f, :, place:place + half, :] = jnp.zeros((levels, half, cols), jnp.float32)
                for sec in range(3):
                    pig[sec, :, tile + place:tile + place + half, :] = jnp.zeros((levels, half, yt), jnp.float32)
        total[...] = jnp.zeros_like(total)
        total2[...] = jnp.zeros_like(total2)
        optical[...] = jnp.zeros_like(optical)
        optical2[...] = jnp.zeros_like(optical2)
        light[...] = jnp.ones_like(light)
        light2[...] = jnp.ones_like(light2)
        with scope("d_load"):
            load(D_LOAD, flow, flow).wait()
            load(D_MASK, masks, masks).wait()
        with scope("d_bar"):
            pl.semaphore_wait(barrier, 3 + 4 * lo_n + 4 * hi_n)

        def drive_copy(k, sec):
            return remote(drive_send.at[k, sec, pl.ds(0, rows_drive)], drive.at[k, pl.ds(0, rows_drive)],
                          one_sem.at[D_DRIVE_S], level_sem.at[T_DRIVE, k], dev(jnp.int32(sec), strip))

        def edge_copy(k, sec, side, offset):
            span = pl.ds(k + 1 - batch, batch)
            return remote(drive_send.at[span, sec, pl.ds(side * (tile - 1), 1)], drive.at[span, pl.ds(rows_drive + 1 - side, 1)],
                          one_sem.at[D_DRIVE_S], one_sem.at[T_EDGE + lax.div(k, jnp.int32(batch))],
                          dev(jnp.int32(sec), strip + offset))

        def drive2_copy(k, sec):
            return remote(drive2_send.at[k, sec], forcing_out.at[:, k], one_sem.at[D_DRIVE2_S], one_sem.at[T_DRIVE2],
                          dev(jnp.int32(sec), strip))

        @pl.loop(0, levels)
        def _(k):
            for side, offset, present in sides:
                @pl.when(present)
                def _():
                    halo_copy(0, k, side, offset).start()

        for sec in range(3):
            greet(ready, jnp.int32(sec), strip)
            for _, offset, present in sides:
                @pl.when(present)
                def _():
                    greet(ready, jnp.int32(sec), strip + offset)

        def deep_of(part):
            return jnp.where(masks[part, 0] == 1, masks[part, 1], 0)

        row_d = lax.broadcasted_iota(jnp.int32, (tile, cols), 0)
        depth[0:tile, :] = deep_of(1)
        depth[tile:wide, :] = jnp.where(row_d < half, deep_of(2) * hi_n, deep_of(0) * lo_n)
        tracers_out[...] = jnp.zeros_like(tracers_out)
        forcing_out[...] = jnp.zeros_like(forcing_out)

        lane_row = lax.broadcasted_iota(jnp.int32, (tile, yt), 1) - lax.broadcasted_iota(jnp.int32, (tile, yt), 0)
        on_diagonal = [lane_row == tile * c for c in range(4)]
        lane_d = lax.broadcasted_iota(jnp.int32, (wide, yt), 1)

        def phase(k, now, pigment, sums, opt_s, light_ref):
            first, last = lane_d == 0, lane_d == yt - 1
            opt = opt_s[...] + (0.05 + 0.3 * pigment)
            lower = jnp.exp(-opt)
            heat = 0.5 * (light_ref[...] - lower)
            opt_s[...] = opt
            light_ref[...] = lower
            sea = k < depth[...]
            wet = jnp.where(sea, 0.05, 0.0)
            heat = jnp.where(sea, heat, 0.0)
            sum_u = None
            for n in range(SUB):
                now, p = substep(now, sums[n], heat, wet, first, last, yt)
                sums[n] = p
                sum_u = now[0] if n == 0 else sum_u + now[0]
                sum_v = now[1] if n == 0 else sum_v + now[1]
            return now, sum_u * (1.0 / SUB), sum_v[0:tile] * (1.0 / SUB)

        @pl.loop(0, levels)
        def _(k):
            with scope("d_halo"):
                for_sides(lambda two: recv(gflow.at[:, k, pl.ds(0, tile if two else half), :], level_sem.at[D_HALO, k]))
            now = tuple(jnp.concatenate([flow[f, k], gflow[f, k]], axis=0) for f in range(4))
            now, mean_u, mean_v = phase(k, now, jnp.concatenate([flow[4, k], gflow[4, k]], axis=0), total, optical, light)
            for f in range(4):
                mid[f, k] = now[f][0:tile]
            for side, offset, present in sides:
                @pl.when(present)
                def _():
                    halo_copy(1, k, side, offset).start()
            mix = 0.1 * now[2][0:tile] - 0.05 * now[3][0:tile]
            spread = jnp.zeros((tile, yt), jnp.float32)
            for c, edge in enumerate((yt - 1, yt, 2 * yt - 1, 2 * yt)):
                spread = jnp.where(on_diagonal[c], mean_v[:, edge:edge + 1], spread)
            turned = jnp.sum(spread, axis=0, keepdims=True)
            for sec in range(3):
                here = slice(sec * yt, (sec + 1) * yt)
                drive_send[k, sec, 0:tile] = mean_u[0:tile, here]
                drive_send[k, sec, tile:2 * tile] = mean_v[:, here]
                drive_send[k, sec, 2 * tile:3 * tile] = mix[:, here]
                drive_send[k, sec, 3 * tile:rows_drive] = turned
            for sec in range(3):
                drive_copy(k, sec).start()
            for side, offset, present in sides:
                @pl.when(present & (lax.rem(k, jnp.int32(batch)) == batch - 1))
                def _():
                    for sec in range(3):
                        edge_copy(k, sec, side, offset).start()

        @pl.loop(0, levels)
        def _(k):
            with scope("d_mid"):
                for_sides(lambda two: recv(gmid.at[:, k, pl.ds(0, tile if two else half), :], level_sem.at[D_MID, k]))
            with scope("d_pig"):
                for_sides(lambda two: recv(pig.at[:, k, pl.ds(0, wide if two else tile + half), :], level_sem.at[D_PIG, k]))
            now = tuple(jnp.concatenate([mid[f, k], gmid[f, k]], axis=0) for f in range(4))
            pigment = jnp.concatenate([pig[sec, k] for sec in range(3)], axis=1)
            now, mean_u, mean_v = phase(k, now, pigment, total2, optical2, light2)
            items = (mean_u[0:tile], mean_v, now[2][0:tile], now[3][0:tile])
            for sec in range(3):
                for f in range(4):
                    drive2_send[k, sec, f] = items[f][:, sec * yt:(sec + 1) * yt]
            drive2_copy(k, 0).start()

            pl.when((k < AHEAD) | (strip == 0))(lambda: drive2_copy(k, 1).start())
            pl.when(strip == 0)(lambda: drive2_copy(k, 2).start())
            for f in range(4):
                flow_out[f, k] = now[f][0:tile]

        @pl.when(has_lo)
        def _():
            for sec, begin in ((1, AHEAD), (2, 0)):
                @pl.loop(begin, levels)
                def _(k):
                    drive2_copy(k, sec).start()

        with scope("d_light"):
            recv(light_out, one_sem.at[D_LIGHT])
        with scope("d_sends"):
            for_sides(lambda two: sent(flow.at[:, :, pl.ds(0, tile if two else half), :], one_sem.at[D_HALO_S]))
            for_sides(lambda two: sent(mid.at[:, :, pl.ds(0, tile if two else half), :], one_sem.at[D_MID_S]))
            for_sides(lambda two: sent(drive_send.at[:, :, pl.ds(0, rows_drive + (2 if two else 1)), :], one_sem.at[D_DRIVE_S]))
            sent(drive2_send, one_sem.at[D_DRIVE2_S])

    @pl.when(jnp.logical_not(is_dyn))
    def _():
        loads = [load(T_LOAD, tracers_h, tracers), load(T_FORCE, forcing_h, forcing), load(T_REACT, reaction_h, reaction)]
        loads.extend(mask_loads(T_MASK, 1, 0))
        for copy in loads:
            copy.start()
        for _, offset, present in sides:
            @pl.when(present)
            def _():
                greet(barrier, section, strip + offset)
                greet(barrier, three, strip + offset)
        greet(barrier, three, strip)
        beside = ((0, -1, has_left), (1, 1, has_right))
        for _, offset, present in beside:
            @pl.when(present)
            def _():
                greet(barrier, section + offset, strip)
        for side, present in ((0, has_lo), (1, has_hi)):
            @pl.when(jnp.logical_not(present))
            def _():
                drive[:, rows_drive + side:rows_drive + side + 1] = jnp.zeros((levels, 1, yt), jnp.float32)
        for side, present, bufs in ((0, has_lo, (row_recv, row_recv2)), (1, has_hi, (row_recv, row_recv2)),
                                    (0, has_left, (col_recv, col_recv2)), (1, has_right, (col_recv, col_recv2))):
            @pl.when(jnp.logical_not(present))
            def _():
                for buf in bufs:
                    buf[side] = jnp.zeros(buf.shape[1:], jnp.float32)

        lane = lax.broadcasted_iota(jnp.int32, (tile, yt), 1)
        row = lax.broadcasted_iota(jnp.int32, (tile, yt), 0)
        pair = lax.div(lane, jnp.int32(2))
        odd = lax.rem(lane, jnp.int32(2)) == 1
        relays = (section == 0) & (strip == 0)

        flow_out[...] = jnp.zeros_like(flow_out)
        light_out[...] = jnp.zeros_like(light_out)
        with scope('t_load'):
            for copy in loads[:3]:
                copy.wait()
            load(T_MASK, masks.at[1], masks.at[1]).wait()

        def pack(items):
            packed = jnp.zeros((tile, yt), jnp.float32)
            for i, x in enumerate(items):
                packed = jnp.where(pair == i, pltpu.roll(x, 2 * i + 1, 1), packed)
            return packed

        @pl.loop(0, levels)
        def _(k):
            for i, x in enumerate([forcing[0, k]] + [tracers[i, k] for i in range(nt)]):
                row_send[0, k, i] = x[0:1]
                row_send[1, k, i] = x[tile - 1:tile]

        left = pl.multiple_of(section * yt, yt)
        deep = jnp.where(masks[1, 0, :, pl.ds(left, yt)] == 1, masks[1, 1, :, pl.ds(left, yt)], 0)
        with scope('t_bar'):
            pl.semaphore_wait(barrier, lo_n + hi_n + has_left.astype(jnp.int32) + has_right.astype(jnp.int32))

        def row_copies(rows_s, rows_r, row_ss, row_rs):
            for side, offset, present in sides:
                yield present, remote(rows_s.at[side], rows_r.at[1 - side], one_sem.at[row_ss], row_rs, dev(section, strip + offset))

        def col_copies(cols_s, cols_r, col_ss, col_rs):
            for side, offset, present in beside:
                yield present, remote(cols_s, cols_r.at[1 - side], one_sem.at[col_ss], col_rs, dev(section + offset, strip))

        joint = pair_of(levels)

        def second_sems(k):
            at = lax.div(k, jnp.int32(joint))
            return level_sem.at[T_EDGES2, at], level_sem.at[T_EDGES2, levels // joint + at]

        def exchange_b(k):
            rows_come, cols_come = second_sems(k)
            yield from row_copies(row_send2.at[:, k], row_recv2.at[:, k], T_ROW2_S, rows_come)
            yield from col_copies(col_send2.at[k], col_recv2.at[:, k], T_COL2_S, cols_come)

        def start(exchange):
            for present, copy in exchange:
                pl.when(present)(copy.start)

        def arrive_rows(rows_r, row_rs):
            for_sides(lambda two: recv(rows_r if two else rows_r.at[0], row_rs))

        def arrive_cols(cols_r, col_rs):
            middle = has_left & has_right
            pl.when(middle)(lambda: recv(cols_r, col_rs))
            pl.when(jnp.logical_not(middle))(lambda: recv(cols_r.at[0], col_rs))

        def finish_rows(rows_s, row_ss):
            for_sides(lambda two: sent(rows_s if two else rows_s.at[0], one_sem.at[row_ss]))

        def finish_cols(cols_s, twice, col_ss):
            middle = has_left & has_right
            pl.when(middle)(lambda: sent(twice, one_sem.at[col_ss]))
            pl.when(jnp.logical_not(middle))(lambda: sent(cols_s, one_sem.at[col_ss]))

        with scope("t_ready"):
            for part, send, come in ((pl.ds(0, 3), T_ROW_S, T_LEAD), (pl.ds(3, nt - 2), T_ROW_S, T_ROW)):
                start(row_copies(row_send.at[:, :, part], row_recv.at[:, :, part], send, one_sem.at[come]))

            @pl.loop(0, levels)
            def _(k):
                col_send[k] = pack([tracers[i, k] for i in range(nt)] + [forcing[1, k]])
                start(col_copies(col_send.at[k], col_recv.at[:, k], T_COL_S, one_sem.at[T_COL]))

            pl.semaphore_wait(ready, 1 + lo_n + hi_n)
        with scope("t_xa"):
            arrive_rows(row_recv.at[:, :, pl.ds(0, 3)], one_sem.at[T_LEAD])
            arrive_cols(col_recv, one_sem.at[T_COL])

        def tracer_step(k, which, cs, u, v, growth, u_lo, u_hi, v_edge, rows_of, packed):
            um, up, vm, vp = 1.0 - u, 1.0 + u, 1.0 - v, 1.0 + v
            hi_m, lo_p = 1.0 - u_hi, 1.0 + u_lo
            edge_m, edge_p = 1.0 - v_edge, 1.0 + v_edge
            wet = k < deep
            out = []
            for i in which:
                c = cs[i]
                react = reaction[i, 0] * cs[0]
                for b in range(1, nt):
                    react = react + reaction[i, b] * cs[b]
                nxt = jnp.where(row == tile - 1, rows_of[1, k, i] * hi_m, pltpu.roll(c * um, tile - 1, 0))
                prv = jnp.where(row == 0, rows_of[0, k, i] * lo_p, pltpu.roll(c * up, 1, 0))
                edge = pltpu.roll(packed, yt - (2 * i + 1), 1)
                rgt = pltpu.roll(jnp.where(lane == 0, edge * edge_m, c * vm), yt - 1, 1)
                lft = pltpu.roll(jnp.where(lane == yt - 1, edge * edge_p, c * vp), 1, 1)
                out.append(jnp.where(wet, 0.8 * c + 0.05 * ((nxt + prv) + (rgt + lft)) + growth * react, 0.0))
            return out

        def pig_copies(k):
            return ((None, pig_copy(k, section, 0, strip)), (has_lo, pig_copy(k, section, 1, strip - 1)),
                    (has_hi, pig_copy(k, section, 2, strip + 1)))

        def step_a(k, which):
            cs = [tracers[i, k] for i in range(nt)]
            packed = jnp.where(odd, col_recv[1, k], col_recv[0, k])
            growth = 0.1 * jnp.exp(0.1 * forcing[2, k] - 0.05 * forcing[3, k])
            v_edge = pltpu.roll(packed, yt - (2 * nt + 1), 1)
            return tracer_step(k, which, cs, forcing[0, k], forcing[1, k], growth, row_recv[0, k, 0], row_recv[1, k, 0], v_edge,
                               row_recv.at[:, :, pl.ds(1, nt)], packed)

        @pl.loop(0, levels)
        def _(k):
            new = step_a(k, range(2))
            pig_s[k] = 0.25 * (new[0] * new[0] + new[1] * new[1])
            for present, copy in pig_copies(k):
                if present is None:
                    copy.start()
                else:
                    pl.when(present)(copy.start)
            for i in range(2):
                held[i, k] = new[i]

        with scope("t_rest"):
            arrive_rows(row_recv.at[:, :, pl.ds(3, nt - 2)], one_sem.at[T_ROW])

        @pl.loop(0, levels)
        def _(k):
            new = [held[0, k], held[1, k]] + step_a(k, range(2, nt))
            for i in range(nt):
                held[i, k] = new[i]
                row_send2[0, k, i] = new[i][0:1]
                row_send2[1, k, i] = new[i][tile - 1:tile]
            col_send2[k] = pack(new)
            start(exchange_b(k))

        with scope("t_relay"):
            @pl.when(relays)
            def _():
                @pl.loop(0, levels)
                def _(k):
                    recv(gmid.at[:, k, pl.ds(0, half), :], level_sem.at[D_MID, k])
                    relay_copy(k).start()

        @pl.loop(0, levels)
        def _(k):
            with scope("t_xb"):
                @pl.when(lax.rem(k, jnp.int32(joint)) == 0)
                def _():
                    rows_come, cols_come = second_sems(k)
                    arrive_rows(row_recv2.at[:, pl.ds(k, joint)], rows_come)
                    arrive_cols(col_recv2.at[:, pl.ds(k, joint)], cols_come)
            with scope("t_drive"):
                recv(drive.at[k, pl.ds(0, rows_drive)], level_sem.at[T_DRIVE, k])

                @pl.when(lax.rem(k, jnp.int32(batch)) == 0)
                def _():
                    come = one_sem.at[T_EDGE + lax.div(k, jnp.int32(batch))]
                    for_sides(lambda two: recv(drive.at[pl.ds(k, batch), pl.ds(rows_drive, 2 if two else 1)], come))
            cs = [held[i, k] for i in range(nt)]
            packed = jnp.where(odd, col_recv2[1, k], col_recv2[0, k])
            growth = 0.1 * jnp.exp(drive[k, 2 * tile:3 * tile])
            turned = drive[k, 3 * tile:rows_drive]
            ends = [jnp.sum(jnp.where(lane - row == tile * c, turned, 0.0), axis=1, keepdims=True)
                    for c in (2 * section - 2, 2 * section + 1)]
            v_edge = jnp.where(lane == 0, ends[1], ends[0])
            new = tracer_step(k, range(nt), cs, drive[k, 0:tile], drive[k, tile:2 * tile], growth, drive[k, rows_drive:rows_drive + 1],
                              drive[k, rows_drive + 1:rows_drive + 2], v_edge, row_recv2, packed)
            light_s[k] = 0.25 * (new[0] * new[0] + new[1] * new[1])
            light_copy(k, section, left, strip).start()
            for i in range(nt):
                tracers_out[i, k] = new[i]

        with scope("t_drive2"):
            recv(forcing_out, one_sem.at[T_DRIVE2])
        sent(light_s, one_sem.at[T_LIGHT_S])
        for_sides(lambda two: sent(col_recv.at[:, :, pl.ds(0, tile if two else 3 * tile // 4)], one_sem.at[T_PIG_S]))
        finish_rows(row_send, T_ROW_S)
        finish_rows(row_send2, T_ROW2_S)
        finish_cols(col_send, col_recv, T_COL_S)
        finish_cols(col_send2, col_recv2, T_COL2_S)

        @pl.when(relays)
        def _():
            sent(gmid.at[:, :, pl.ds(0, half), :], one_sem.at[T_MID_S])


def write_out(*refs):
    done = refs[-1]
    copies = [pltpu.make_async_copy(refs[i], refs[4 + i], done.at[i]) for i in range(4)]
    for copy in copies:
        copy.start()
    for copy in copies:
        copy.wait()


def solution(mesh):
    sizes = tuple(mesh.shape[a] for a in AXES)

    def on_device(flow, chl, tracers, forcing, ocean, bottom, reaction):
        levels, tile, cols = chl.shape
        nt, yt = tracers.shape[0], tracers.shape[3]
        f32 = jnp.float32

        def buf(*shape):
            return pltpu.VMEM(shape, f32)

        def sem(*shape):
            return pltpu.SemaphoreType.DMA(shape)

        wide = 2 * tile
        scratch = [
            buf(5, levels, tile, cols), buf(5, levels, tile, cols), buf(*flow.shape), buf(*flow.shape),
            pltpu.VMEM((3, 2, tile, cols), jnp.int32), buf(*tracers.shape), buf(*forcing.shape), pltpu.SMEM(reaction.shape, f32),
            pltpu.VMEM((wide, cols), jnp.int32), buf(SUB, wide, cols), buf(wide, cols), buf(wide, cols),
            buf(SUB, wide, cols), buf(wide, cols), buf(wide, cols), buf(3, levels, wide, yt),
            buf(levels, 3, 4 * tile, yt), buf(levels, 3, 4, tile, yt),
            buf(2, levels, nt + 1, 1, yt), buf(levels, tile, yt), buf(2, levels, nt + 1, 1, yt), buf(2, levels, tile, yt),
            buf(2, levels, nt, 1, yt), buf(levels, tile, yt), buf(2, levels, nt, 1, yt), buf(2, levels, tile, yt),
            buf(nt, levels, tile, yt), buf(levels, tile, yt),
            buf(levels, 4 * tile, yt), buf(levels, tile, yt),
            sem(3, max(levels, 2 * levels // pair_of(levels))), sem(N_ONE), pltpu.SemaphoreType.REGULAR,
        ]
        vmem = pl.BlockSpec(memory_space=pltpu.VMEM)
        shapes = [x.shape for x in (flow, chl, tracers, forcing)]
        room = 67043328 - 4 * sum(math.prod(x) for x in shapes) - 2**16
        results = pl.pallas_call(
            functools.partial(kernel, sizes),
            out_shape=[pltpu.VMEM(x, f32) for x in shapes],
            in_specs=[pl.BlockSpec(memory_space=pltpu.HBM)] * 7,
            out_specs=[vmem] * 4,
            scratch_shapes=scratch,
            compiler_params=pltpu.CompilerParams(collective_id=0, has_side_effects=True, vmem_limit_bytes=room),
        )(flow, chl, tracers, forcing, ocean, bottom, reaction)
        return pl.pallas_call(
            write_out,
            out_shape=[jax.ShapeDtypeStruct(x, f32) for x in shapes],
            in_specs=[vmem] * 4,
            out_specs=[pl.BlockSpec(memory_space=pltpu.HBM)] * 4,
            scratch_shapes=[sem(4)],
            compiler_params=pltpu.CompilerParams(vmem_limit_bytes=4 * 2**20),
        )(*results)

    rows4 = P(None, None, AXES, None)
    rows3 = P(None, AXES, None)
    return jax.shard_map(on_device, mesh=mesh, in_specs=(rows4, rows3, rows4, rows4, P(), P(), P()),
                         out_specs=(rows4, rows3, rows4, rows4), check_vma=False)
```

```python
import functools
import math

import jax
import jax.numpy as jnp
from jax import lax
from jax.experimental import pallas as pl
from jax.experimental.pallas import tpu as pltpu
from jax.sharding import PartitionSpec as P

SUB = 4
AHEAD = 1
MESH = pl.DeviceIdType.MESH
AXES = ("comp", "gy", "gx")


def substep(state, above, heat, wet, first, last, lanes):
    u, v, t, s = state
    rows, cols = u.shape
    p = above + 0.2 * (s - t)

    def row_next(x):
        return pltpu.roll(x, rows - 1, 0)

    def row_prev(x):
        return pltpu.roll(x, 1, 0)

    def col_shift(x, shift, at_edge, step):
        turned = [pltpu.roll(x[:, a:a + lanes], shift, 1) for a in range(0, cols, lanes)]
        beside = [turned[i + step] if 0 <= i + step < len(turned) else 0.0 for i in range(len(turned))]
        return jnp.concatenate([jnp.where(at_edge, b, x) for x, b in zip(turned, beside)], axis=1)

    def col_next(x):
        return col_shift(x, lanes - 1, last, 1)

    def col_prev(x):
        return col_shift(x, 1, first, -1)

    um, up, vm, vp = 1.0 - u, 1.0 + u, 1.0 - v, 1.0 + v
    new_u = wet * (15.8 * u + 2.0 * v + (row_next(u - p) + row_prev(u + p) + (col_next(u) + col_prev(u))))
    new_v = wet * (15.8 * v - 2.0 * u + (row_next(v) + row_prev(v) + (col_next(v - p) + col_prev(v + p))))
    new_t = wet * (16.0 * t + (row_next(t * um) + row_prev(t * up) + (col_next(t * vm) + col_prev(t * vp)))) + heat
    new_s = wet * (16.0 * s + (row_next(s * um) + row_prev(s * up) + (col_next(s * vm) + col_prev(s * vp))))
    return (new_u, new_v, new_t, new_s), p


D_HALO, D_MID, D_PIG = 0, 1, 2
T_EDGES2, T_DRIVE = 0, 2
D_LIGHT, D_LOAD, D_MASK, D_DRIVE_S, D_DRIVE2_S = range(5)
D_HALO_S, D_MID_S = D_LOAD, D_MASK
T_ROW, T_COL, T_LEAD, T_DRIVE2, T_EDGE, _, T_LOAD, T_FORCE, T_REACT, T_MASK, T_COL_S, T_COL2_S, T_MID_S, N_ONE = range(14)
T_ROW_S, T_ROW2_S, T_PIG_S, T_LIGHT_S = T_LOAD, T_FORCE, T_REACT, T_MASK


def pair_of(levels):
    return 2 if levels % 2 == 0 else 1


def kernel(sizes, flow_h, chl_h, tracers_h, forcing_h, ocean_h, bottom_h, reaction_h,
           flow_out, light_out, tracers_out, forcing_out,
           flow, gflow, mid, gmid, masks, tracers, forcing, reaction, depth, total, optical, light, total2, optical2, light2, pig,
           drive_send, drive2_send, row_send, col_send, row_recv, col_recv, row_send2, col_send2, row_recv2, col_recv2,
           held, pig_s, drive, light_s, level_sem, one_sem, ready):
    n_comp, n_gy, n_gx = sizes
    grid = n_gy * n_gx
    every = n_comp * grid
    group = every // 4
    _, levels, tile, cols = mid.shape
    half = tile // 2
    wide = 2 * tile
    nt = tracers.shape[0]
    yt = tracers.shape[3]
    position = (lax.axis_index("comp") * grid + lax.axis_index("gy") * n_gx + lax.axis_index("gx")).astype(jnp.int32)
    moved = lax.rem(position + 1, jnp.int32(every))
    strip = lax.rem(moved, jnp.int32(group))
    section = lax.div(moved, jnp.int32(group))
    is_dyn = section == 3
    has_lo = strip > 0
    has_hi = strip < group - 1
    has_left = section > 0
    has_right = section < 2

    def dev(sec, row):
        pos = lax.rem(sec * group + row + (every - 1), jnp.int32(every))
        return (lax.div(pos, jnp.int32(grid)), lax.rem(lax.div(pos, jnp.int32(n_gx)), jnp.int32(n_gy)),
                lax.rem(pos, jnp.int32(n_gx)))

    def remote(src, dst, send_sem, recv_sem, target):
        return pltpu.make_async_remote_copy(src_ref=src, dst_ref=dst, send_sem=send_sem, recv_sem=recv_sem,
                                            device_id=target, device_id_type=MESH)

    three = jnp.int32(3)
    scope = jax.named_scope
    barrier = pltpu.get_barrier_semaphore()

    def load(i, src, dst):
        return pltpu.make_async_copy(src, dst, one_sem.at[i])

    def mask_loads(sem, part, offset):
        begin = pl.multiple_of(jnp.clip(strip + offset, 0, group - 1) * tile, tile)
        return [load(sem, h.at[pl.ds(begin, tile), :], masks.at[part, m]) for m, h in enumerate((ocean_h, bottom_h))]

    def greet(sem, sec, row):
        pl.semaphore_signal(sem, inc=1, device_id=dev(sec, row), device_id_type=MESH)

    sides = ((0, -1, has_lo), (1, 1, has_hi))
    lo_n = has_lo.astype(jnp.int32)
    hi_n = has_hi.astype(jnp.int32)

    both = has_lo & has_hi
    rows_drive = 3 * tile + 1
    batch = levels // 2 if levels % 2 == 0 else levels

    def for_sides(act):
        pl.when(both)(lambda: act(True))
        pl.when(jnp.logical_not(both))(lambda: act(False))

    def pig_copy(k, sec, part, row):
        from_rows = (pl.ds(0, tile), pl.ds(0, half), pl.ds(half, half))[part]
        to_rows = (pl.ds(0, tile), pl.ds(tile, half), pl.ds(tile + half, half))[part]
        return remote(pig_s.at[k, from_rows], pig.at[sec, k, to_rows], one_sem.at[T_PIG_S],
                      level_sem.at[D_PIG, k], dev(three, row))

    def light_copy(k, sec, begin, row):
        return remote(light_s.at[k], light_out.at[k, :, pl.ds(begin, yt)], one_sem.at[T_LIGHT_S], one_sem.at[D_LIGHT],
                      dev(three, row))

    other = dev(lax.rem(section + 1, jnp.int32(4)), strip)

    def recv(dst, sem):
        remote(dst, dst, sem, sem, other).wait_recv()

    def sent(src, sem):
        remote(src, src, sem, sem, other).wait_send()

    halo_of = ((flow, gflow, D_HALO_S, D_HALO), (mid, gmid, D_MID_S, D_MID))

    def halo_copy(what, k, side, offset):
        own, ghost, send, come = halo_of[what]
        place = pl.ds(half * side, half)
        to = strip + offset
        where = dev(three * jnp.minimum(to, 1) if what == 1 else three, to)
        return remote(own.at[:, k, place, :], ghost.at[:, k, place, :], one_sem.at[send], level_sem.at[come, k], where)

    def relay_copy(k):
        place = pl.ds(0, half)
        return remote(gmid.at[:, k, place, :], gmid.at[:, k, place, :], one_sem.at[T_MID_S], level_sem.at[D_MID, k],
                      dev(three, strip))

    @pl.when(is_dyn)
    def _():
        for copy in (load(D_LOAD, flow_h, flow.at[0:4]), load(D_LOAD, chl_h, flow.at[4])):
            copy.start()
        for _, offset, present in sides:
            @pl.when(present)
            def _():
                greet(barrier, three, strip + offset)
        for part in range(3):
            for copy in mask_loads(D_MASK, part, part - 1):
                copy.start()
        for place, present in ((half, has_lo), (0, has_hi)):
            @pl.when(jnp.logical_not(present))
            def _():
                for f in range(5):
                    gflow[f, :, place:place + half, :] = jnp.zeros((levels, half, cols), jnp.float32)
                for f in range(4):
                    gmid[f, :, place:place + half, :] = jnp.zeros((levels, half, cols), jnp.float32)
                for sec in range(3):
                    pig[sec, :, tile + place:tile + place + half, :] = jnp.zeros((levels, half, yt), jnp.float32)
        total[...] = jnp.zeros_like(total)
        total2[...] = jnp.zeros_like(total2)
        optical[...] = jnp.zeros_like(optical)
        optical2[...] = jnp.zeros_like(optical2)
        light[...] = jnp.ones_like(light)
        light2[...] = jnp.ones_like(light2)
        with scope("d_load"):
            load(D_LOAD, flow, flow).wait()
        with scope("d_bar"):
            pl.semaphore_wait(barrier, 3 + 4 * lo_n + 4 * hi_n)

        def drive_copy(k, sec):
            return remote(drive_send.at[k, sec, pl.ds(0, rows_drive)], drive.at[k, pl.ds(0, rows_drive)],
                          one_sem.at[D_DRIVE_S], level_sem.at[T_DRIVE, k], dev(jnp.int32(sec), strip))

        def edge_copy(k, sec, side, offset):
            span = pl.ds(k + 1 - batch, batch)
            return remote(drive_send.at[span, sec, pl.ds(side * (tile - 1), 1)], drive.at[span, pl.ds(rows_drive + 1 - side, 1)],
                          one_sem.at[D_DRIVE_S], one_sem.at[T_EDGE + lax.div(k, jnp.int32(batch))],
                          dev(jnp.int32(sec), strip + offset))

        def drive2_copy(k, sec):
            return remote(drive2_send.at[k, sec], forcing_out.at[:, k], one_sem.at[D_DRIVE2_S], one_sem.at[T_DRIVE2],
                          dev(jnp.int32(sec), strip))

        @pl.loop(0, levels)
        def _(k):
            for side, offset, present in sides:
                @pl.when(present)
                def _():
                    halo_copy(0, k, side, offset).start()

        for sec in range(3):
            greet(ready, jnp.int32(sec), strip)
            for _, offset, present in sides:
                @pl.when(present)
                def _():
                    greet(ready, jnp.int32(sec), strip + offset)

        load(D_MASK, masks, masks).wait()

        def deep_of(part):
            return jnp.where(masks[part, 0] == 1, masks[part, 1], 0)

        row_d = lax.broadcasted_iota(jnp.int32, (tile, cols), 0)
        depth[0:tile, :] = deep_of(1)
        depth[tile:wide, :] = jnp.where(row_d < half, deep_of(2) * hi_n, deep_of(0) * lo_n)
        tracers_out[...] = jnp.zeros_like(tracers_out)
        forcing_out[...] = jnp.zeros_like(forcing_out)

        lane_row = lax.broadcasted_iota(jnp.int32, (tile, yt), 1) - lax.broadcasted_iota(jnp.int32, (tile, yt), 0)
        on_diagonal = [lane_row == tile * c for c in range(4)]
        lane_d = lax.broadcasted_iota(jnp.int32, (wide, yt), 1)

        def phase(k, now, pigment, sums, opt_s, light_ref):
            first, last = lane_d == 0, lane_d == yt - 1
            opt = opt_s[...] + (0.05 + 0.3 * pigment)
            lower = jnp.exp(-opt)
            heat = 0.5 * (light_ref[...] - lower)
            opt_s[...] = opt
            light_ref[...] = lower
            sea = k < depth[...]
            wet = jnp.where(sea, 0.05, 0.0)
            heat = jnp.where(sea, heat, 0.0)
            sum_u = None
            for n in range(SUB):
                now, p = substep(now, sums[n], heat, wet, first, last, yt)
                sums[n] = p
                sum_u = now[0] if n == 0 else sum_u + now[0]
                sum_v = now[1] if n == 0 else sum_v + now[1]
            return now, sum_u * (1.0 / SUB), sum_v[0:tile] * (1.0 / SUB)

        @pl.loop(0, levels)
        def _(k):
            with scope("d_halo"):
                for_sides(lambda two: recv(gflow.at[:, k, pl.ds(0, tile if two else half), :], level_sem.at[D_HALO, k]))
            now = tuple(jnp.concatenate([flow[f, k], gflow[f, k]], axis=0) for f in range(4))
            now, mean_u, mean_v = phase(k, now, jnp.concatenate([flow[4, k], gflow[4, k]], axis=0), total, optical, light)
            for f in range(4):
                mid[f, k] = now[f][0:tile]
            for side, offset, present in sides:
                @pl.when(present)
                def _():
                    halo_copy(1, k, side, offset).start()
            mix = 0.1 * now[2][0:tile] - 0.05 * now[3][0:tile]
            spread = jnp.zeros((tile, yt), jnp.float32)
            for c, edge in enumerate((yt - 1, yt, 2 * yt - 1, 2 * yt)):
                spread = jnp.where(on_diagonal[c], mean_v[:, edge:edge + 1], spread)
            turned = jnp.sum(spread, axis=0, keepdims=True)
            for sec in range(3):
                here = slice(sec * yt, (sec + 1) * yt)
                drive_send[k, sec, 0:tile] = mean_u[0:tile, here]
                drive_send[k, sec, tile:2 * tile] = mean_v[:, here]
                drive_send[k, sec, 2 * tile:3 * tile] = mix[:, here]
                drive_send[k, sec, 3 * tile:rows_drive] = turned
            for sec in range(3):
                drive_copy(k, sec).start()
            for side, offset, present in sides:
                @pl.when(present & (lax.rem(k, jnp.int32(batch)) == batch - 1))
                def _():
                    for sec in range(3):
                        edge_copy(k, sec, side, offset).start()

        @pl.loop(0, levels)
        def _(k):
            with scope("d_mid"):
                for_sides(lambda two: recv(gmid.at[:, k, pl.ds(0, tile if two else half), :], level_sem.at[D_MID, k]))
            with scope("d_pig"):
                for_sides(lambda two: recv(pig.at[:, k, pl.ds(0, wide if two else tile + half), :], level_sem.at[D_PIG, k]))
            now = tuple(jnp.concatenate([mid[f, k], gmid[f, k]], axis=0) for f in range(4))
            pigment = jnp.concatenate([pig[sec, k] for sec in range(3)], axis=1)
            now, mean_u, mean_v = phase(k, now, pigment, total2, optical2, light2)
            items = (mean_u[0:tile], mean_v, now[2][0:tile], now[3][0:tile])
            for sec in range(3):
                for f in range(4):
                    drive2_send[k, sec, f] = items[f][:, sec * yt:(sec + 1) * yt]
            drive2_copy(k, 0).start()

            pl.when((k < AHEAD) | (strip == 0))(lambda: drive2_copy(k, 1).start())
            pl.when(strip == 0)(lambda: drive2_copy(k, 2).start())
            for f in range(4):
                flow_out[f, k] = now[f][0:tile]

        @pl.when(has_lo)
        def _():
            for sec, begin in ((1, AHEAD), (2, 0)):
                @pl.loop(begin, levels)
                def _(k):
                    drive2_copy(k, sec).start()

        with scope("d_light"):
            recv(light_out, one_sem.at[D_LIGHT])
        with scope("d_sends"):
            for_sides(lambda two: sent(flow.at[:, :, pl.ds(0, tile if two else half), :], one_sem.at[D_HALO_S]))
            for_sides(lambda two: sent(mid.at[:, :, pl.ds(0, tile if two else half), :], one_sem.at[D_MID_S]))
            for_sides(lambda two: sent(drive_send.at[:, :, pl.ds(0, rows_drive + (2 if two else 1)), :], one_sem.at[D_DRIVE_S]))
            sent(drive2_send, one_sem.at[D_DRIVE2_S])

    @pl.when(jnp.logical_not(is_dyn))
    def _():
        for _, offset, present in sides:
            @pl.when(present)
            def _():
                greet(barrier, section, strip + offset)
                greet(barrier, three, strip + offset)
        greet(barrier, three, strip)
        beside = ((0, -1, has_left), (1, 1, has_right))
        for _, offset, present in beside:
            @pl.when(present)
            def _():
                greet(barrier, section + offset, strip)
        loads = [load(T_LOAD, tracers_h, tracers), load(T_FORCE, forcing_h, forcing), load(T_REACT, reaction_h, reaction)]
        loads.extend(mask_loads(T_MASK, 1, 0))
        for copy in loads:
            copy.start()
        for side, present in ((0, has_lo), (1, has_hi)):
            @pl.when(jnp.logical_not(present))
            def _():
                drive[:, rows_drive + side:rows_drive + side + 1] = jnp.zeros((levels, 1, yt), jnp.float32)
        for side, present, bufs in ((0, has_lo, (row_recv, row_recv2)), (1, has_hi, (row_recv, row_recv2)),
                                    (0, has_left, (col_recv, col_recv2)), (1, has_right, (col_recv, col_recv2))):
            @pl.when(jnp.logical_not(present))
            def _():
                for buf in bufs:
                    buf[side] = jnp.zeros(buf.shape[1:], jnp.float32)

        lane = lax.broadcasted_iota(jnp.int32, (tile, yt), 1)
        row = lax.broadcasted_iota(jnp.int32, (tile, yt), 0)
        pair = lax.div(lane, jnp.int32(2))
        odd = lax.rem(lane, jnp.int32(2)) == 1
        relays = (section == 0) & (strip == 0)

        flow_out[...] = jnp.zeros_like(flow_out)
        light_out[...] = jnp.zeros_like(light_out)
        with scope('t_load'):
            for copy in loads[:3]:
                copy.wait()
            load(T_MASK, masks.at[1], masks.at[1]).wait()

        def pack(items):
            packed = jnp.zeros((tile, yt), jnp.float32)
            for i, x in enumerate(items):
                packed = jnp.where(pair == i, pltpu.roll(x, 2 * i + 1, 1), packed)
            return packed

        @pl.loop(0, levels)
        def _(k):
            for i, x in enumerate([forcing[0, k]] + [tracers[i, k] for i in range(nt)]):
                row_send[0, k, i] = x[0:1]
                row_send[1, k, i] = x[tile - 1:tile]

        left = pl.multiple_of(section * yt, yt)
        deep = jnp.where(masks[1, 0, :, pl.ds(left, yt)] == 1, masks[1, 1, :, pl.ds(left, yt)], 0)
        with scope('t_bar'):
            pl.semaphore_wait(barrier, lo_n + hi_n + has_left.astype(jnp.int32) + has_right.astype(jnp.int32))

        def row_copies(rows_s, rows_r, row_ss, row_rs):
            for side, offset, present in sides:
                yield present, remote(rows_s.at[side], rows_r.at[1 - side], one_sem.at[row_ss], row_rs, dev(section, strip + offset))

        def col_copies(cols_s, cols_r, col_ss, col_rs):
            for side, offset, present in beside:
                yield present, remote(cols_s, cols_r.at[1 - side], one_sem.at[col_ss], col_rs, dev(section + offset, strip))

        joint = pair_of(levels)

        def second_sems(k):
            at = lax.div(k, jnp.int32(joint))
            return level_sem.at[T_EDGES2, at], level_sem.at[T_EDGES2, levels // joint + at]

        def exchange_b(k):
            rows_come, cols_come = second_sems(k)
            yield from row_copies(row_send2.at[:, k], row_recv2.at[:, k], T_ROW2_S, rows_come)
            yield from col_copies(col_send2.at[k], col_recv2.at[:, k], T_COL2_S, cols_come)

        def start(exchange):
            for present, copy in exchange:
                pl.when(present)(copy.start)

        def arrive_rows(rows_r, row_rs):
            for_sides(lambda two: recv(rows_r if two else rows_r.at[0], row_rs))

        def arrive_cols(cols_r, col_rs):
            middle = has_left & has_right
            pl.when(middle)(lambda: recv(cols_r, col_rs))
            pl.when(jnp.logical_not(middle))(lambda: recv(cols_r.at[0], col_rs))

        def finish_rows(rows_s, row_ss):
            for_sides(lambda two: sent(rows_s if two else rows_s.at[0], one_sem.at[row_ss]))

        def finish_cols(cols_s, twice, col_ss):
            middle = has_left & has_right
            pl.when(middle)(lambda: sent(twice, one_sem.at[col_ss]))
            pl.when(jnp.logical_not(middle))(lambda: sent(cols_s, one_sem.at[col_ss]))

        with scope("t_ready"):
            for part, send, come in ((pl.ds(0, 3), T_ROW_S, T_LEAD), (pl.ds(3, nt - 2), T_ROW_S, T_ROW)):
                start(row_copies(row_send.at[:, :, part], row_recv.at[:, :, part], send, one_sem.at[come]))

            @pl.loop(0, levels)
            def _(k):
                col_send[k] = pack([tracers[i, k] for i in range(nt)] + [forcing[1, k]])
                start(col_copies(col_send.at[k], col_recv.at[:, k], T_COL_S, one_sem.at[T_COL]))

            pl.semaphore_wait(ready, 1 + lo_n + hi_n)
        with scope("t_xa"):
            arrive_rows(row_recv.at[:, :, pl.ds(0, 3)], one_sem.at[T_LEAD])
            arrive_cols(col_recv, one_sem.at[T_COL])

        def tracer_step(k, which, cs, u, v, growth, u_lo, u_hi, v_edge, rows_of, packed):
            um, up, vm, vp = 1.0 - u, 1.0 + u, 1.0 - v, 1.0 + v
            hi_m, lo_p = 1.0 - u_hi, 1.0 + u_lo
            edge_m, edge_p = 1.0 - v_edge, 1.0 + v_edge
            wet = k < deep
            out = []
            for i in which:
                c = cs[i]
                react = reaction[i, 0] * cs[0]
                for b in range(1, nt):
                    react = react + reaction[i, b] * cs[b]
                nxt = jnp.where(row == tile - 1, rows_of[1, k, i] * hi_m, pltpu.roll(c * um, tile - 1, 0))
                prv = jnp.where(row == 0, rows_of[0, k, i] * lo_p, pltpu.roll(c * up, 1, 0))
                edge = pltpu.roll(packed, yt - (2 * i + 1), 1)
                rgt = pltpu.roll(jnp.where(lane == 0, edge * edge_m, c * vm), yt - 1, 1)
                lft = pltpu.roll(jnp.where(lane == yt - 1, edge * edge_p, c * vp), 1, 1)
                out.append(jnp.where(wet, 0.8 * c + 0.05 * ((nxt + prv) + (rgt + lft)) + growth * react, 0.0))
            return out

        def pig_copies(k):
            return ((None, pig_copy(k, section, 0, strip)), (has_lo, pig_copy(k, section, 1, strip - 1)),
                    (has_hi, pig_copy(k, section, 2, strip + 1)))

        def send_pigment(k):
            for present, copy in pig_copies(k):
                if present is None:
                    copy.start()
                else:
                    pl.when(present)(copy.start)

        def step_a(k, which):
            cs = [tracers[i, k] for i in range(nt)]
            packed = jnp.where(odd, col_recv[1, k], col_recv[0, k])
            growth = 0.1 * jnp.exp(0.1 * forcing[2, k] - 0.05 * forcing[3, k])
            v_edge = pltpu.roll(packed, yt - (2 * nt + 1), 1)
            return tracer_step(k, which, cs, forcing[0, k], forcing[1, k], growth, row_recv[0, k, 0], row_recv[1, k, 0], v_edge,
                               row_recv.at[:, :, pl.ds(1, nt)], packed)

        @pl.loop(0, levels)
        def _(k):
            new = step_a(k, range(2))
            pig_s[k] = 0.25 * (new[0] * new[0] + new[1] * new[1])
            pl.when(has_hi | (k < 4))(lambda: send_pigment(k))
            for i in range(2):
                held[i, k] = new[i]

        with scope("t_rest"):
            arrive_rows(row_recv.at[:, :, pl.ds(3, nt - 2)], one_sem.at[T_ROW])

        @pl.loop(0, levels)
        def _(k):
            new = [held[0, k], held[1, k]] + step_a(k, range(2, nt))
            for i in range(nt):
                held[i, k] = new[i]
                row_send2[0, k, i] = new[i][0:1]
                row_send2[1, k, i] = new[i][tile - 1:tile]
            col_send2[k] = pack(new)
            start(exchange_b(k))

        @pl.when(jnp.logical_not(has_hi))
        def _():
            pl.loop(4, levels)(send_pigment)

        with scope("t_relay"):
            @pl.when(relays)
            def _():
                @pl.loop(0, levels)
                def _(k):
                    recv(gmid.at[:, k, pl.ds(0, half), :], level_sem.at[D_MID, k])
                    relay_copy(k).start()

        @pl.loop(0, levels)
        def _(k):
            with scope("t_xb"):
                @pl.when(lax.rem(k, jnp.int32(joint)) == 0)
                def _():
                    rows_come, cols_come = second_sems(k)
                    arrive_rows(row_recv2.at[:, pl.ds(k, joint)], rows_come)
                    arrive_cols(col_recv2.at[:, pl.ds(k, joint)], cols_come)
            with scope("t_drive"):
                recv(drive.at[k, pl.ds(0, rows_drive)], level_sem.at[T_DRIVE, k])

                @pl.when(lax.rem(k, jnp.int32(batch)) == 0)
                def _():
                    come = one_sem.at[T_EDGE + lax.div(k, jnp.int32(batch))]
                    for_sides(lambda two: recv(drive.at[pl.ds(k, batch), pl.ds(rows_drive, 2 if two else 1)], come))
            cs = [held[i, k] for i in range(nt)]
            packed = jnp.where(odd, col_recv2[1, k], col_recv2[0, k])
            growth = 0.1 * jnp.exp(drive[k, 2 * tile:3 * tile])
            turned = drive[k, 3 * tile:rows_drive]
            ends = [jnp.sum(jnp.where(lane - row == tile * c, turned, 0.0), axis=1, keepdims=True)
                    for c in (2 * section - 2, 2 * section + 1)]
            v_edge = jnp.where(lane == 0, ends[1], ends[0])
            new = tracer_step(k, range(nt), cs, drive[k, 0:tile], drive[k, tile:2 * tile], growth, drive[k, rows_drive:rows_drive + 1],
                              drive[k, rows_drive + 1:rows_drive + 2], v_edge, row_recv2, packed)
            light_s[k] = 0.25 * (new[0] * new[0] + new[1] * new[1])
            light_copy(k, section, left, strip).start()
            for i in range(nt):
                tracers_out[i, k] = new[i]

        with scope("t_drive2"):
            recv(forcing_out, one_sem.at[T_DRIVE2])
        sent(light_s, one_sem.at[T_LIGHT_S])
        for_sides(lambda two: sent(col_recv.at[:, :, pl.ds(0, tile if two else 3 * tile // 4)], one_sem.at[T_PIG_S]))
        finish_rows(row_send, T_ROW_S)
        finish_rows(row_send2, T_ROW2_S)
        finish_cols(col_send, col_recv, T_COL_S)
        finish_cols(col_send2, col_recv2, T_COL2_S)

        @pl.when(relays)
        def _():
            sent(gmid.at[:, :, pl.ds(0, half), :], one_sem.at[T_MID_S])


def write_out(*refs):
    done = refs[-1]
    copies = [pltpu.make_async_copy(refs[i], refs[4 + i], done.at[i]) for i in range(4)]
    for copy in copies:
        copy.start()
    for copy in copies:
        copy.wait()


def solution(mesh):
    sizes = tuple(mesh.shape[a] for a in AXES)

    def on_device(flow, chl, tracers, forcing, ocean, bottom, reaction):
        levels, tile, cols = chl.shape
        nt, yt = tracers.shape[0], tracers.shape[3]
        f32 = jnp.float32

        def buf(*shape):
            return pltpu.VMEM(shape, f32)

        def sem(*shape):
            return pltpu.SemaphoreType.DMA(shape)

        wide = 2 * tile
        scratch = [
            buf(5, levels, tile, cols), buf(5, levels, tile, cols), buf(*flow.shape), buf(*flow.shape),
            pltpu.VMEM((3, 2, tile, cols), jnp.int32), buf(*tracers.shape), buf(*forcing.shape), pltpu.SMEM(reaction.shape, f32),
            pltpu.VMEM((wide, cols), jnp.int32), buf(SUB, wide, cols), buf(wide, cols), buf(wide, cols),
            buf(SUB, wide, cols), buf(wide, cols), buf(wide, cols), buf(3, levels, wide, yt),
            buf(levels, 3, 4 * tile, yt), buf(levels, 3, 4, tile, yt),
            buf(2, levels, nt + 1, 1, yt), buf(levels, tile, yt), buf(2, levels, nt + 1, 1, yt), buf(2, levels, tile, yt),
            buf(2, levels, nt, 1, yt), buf(levels, tile, yt), buf(2, levels, nt, 1, yt), buf(2, levels, tile, yt),
            buf(nt, levels, tile, yt), buf(levels, tile, yt),
            buf(levels, 4 * tile, yt), buf(levels, tile, yt),
            sem(3, max(levels, 2 * levels // pair_of(levels))), sem(N_ONE), pltpu.SemaphoreType.REGULAR,
        ]
        vmem = pl.BlockSpec(memory_space=pltpu.VMEM)
        shapes = [x.shape for x in (flow, chl, tracers, forcing)]
        room = 67043328 - 4 * sum(math.prod(x) for x in shapes) - 2**16
        results = pl.pallas_call(
            functools.partial(kernel, sizes),
            out_shape=[pltpu.VMEM(x, f32) for x in shapes],
            in_specs=[pl.BlockSpec(memory_space=pltpu.HBM)] * 7,
            out_specs=[vmem] * 4,
            scratch_shapes=scratch,
            compiler_params=pltpu.CompilerParams(collective_id=0, has_side_effects=True, vmem_limit_bytes=room),
        )(flow, chl, tracers, forcing, ocean, bottom, reaction)
        return pl.pallas_call(
            write_out,
            out_shape=[jax.ShapeDtypeStruct(x, f32) for x in shapes],
            in_specs=[vmem] * 4,
            out_specs=[pl.BlockSpec(memory_space=pltpu.HBM)] * 4,
            scratch_shapes=[sem(4)],
            compiler_params=pltpu.CompilerParams(vmem_limit_bytes=4 * 2**20),
        )(*results)

    rows4 = P(None, None, AXES, None)
    rows3 = P(None, AXES, None)
    return jax.shard_map(on_device, mesh=mesh, in_specs=(rows4, rows3, rows4, rows4, P(), P(), P()),
                         out_specs=(rows4, rows3, rows4, rows4), check_vma=False)
```

```python
import functools
import math

import jax
import jax.numpy as jnp
from jax import lax
from jax.experimental import pallas as pl
from jax.experimental.pallas import tpu as pltpu
from jax.sharding import PartitionSpec as P

SUB = 4
AHEAD = 1
MESH = pl.DeviceIdType.MESH
AXES = ("comp", "gy", "gx")


def substep(state, above, heat, wet, first, last, lanes):
    u, v, t, s = state
    rows, cols = u.shape
    p = above + 0.2 * (s - t)

    def row_next(x):
        return pltpu.roll(x, rows - 1, 0)

    def row_prev(x):
        return pltpu.roll(x, 1, 0)

    def col_shift(x, shift, at_edge, step):
        turned = [pltpu.roll(x[:, a:a + lanes], shift, 1) for a in range(0, cols, lanes)]
        beside = [turned[i + step] if 0 <= i + step < len(turned) else 0.0 for i in range(len(turned))]
        return jnp.concatenate([jnp.where(at_edge, b, x) for x, b in zip(turned, beside)], axis=1)

    def col_next(x):
        return col_shift(x, lanes - 1, last, 1)

    def col_prev(x):
        return col_shift(x, 1, first, -1)

    um, up, vm, vp = 1.0 - u, 1.0 + u, 1.0 - v, 1.0 + v
    new_u = wet * (15.8 * u + 2.0 * v + (row_next(u - p) + row_prev(u + p) + (col_next(u) + col_prev(u))))
    new_v = wet * (15.8 * v - 2.0 * u + (row_next(v) + row_prev(v) + (col_next(v - p) + col_prev(v + p))))
    new_t = wet * (16.0 * t + (row_next(t * um) + row_prev(t * up) + (col_next(t * vm) + col_prev(t * vp)))) + heat
    new_s = wet * (16.0 * s + (row_next(s * um) + row_prev(s * up) + (col_next(s * vm) + col_prev(s * vp))))
    return (new_u, new_v, new_t, new_s), p


D_HALO, D_MID, D_PIG = 0, 1, 2
T_EDGES2, T_DRIVE = 0, 2
D_LIGHT, D_LOAD, D_MASK, D_DRIVE_S, D_DRIVE2_S = range(5)
D_HALO_S, D_MID_S = D_LOAD, D_MASK
T_ROW, T_COL, T_LEAD, T_DRIVE2, T_EDGE, _, T_LOAD, T_FORCE, T_REACT, T_MASK, T_COL_S, T_COL2_S, T_MID_S, N_ONE = range(14)
T_ROW_S, T_ROW2_S, T_PIG_S, T_LIGHT_S = T_LOAD, T_FORCE, T_REACT, T_MASK


def pair_of(levels):
    return 2 if levels % 2 == 0 else 1


def kernel(sizes, flow_h, chl_h, tracers_h, forcing_h, ocean_h, bottom_h, reaction_h,
           flow_out, light_out, tracers_out, forcing_out,
           flow, gflow, mid, gmid, masks, tracers, forcing, reaction, depth, total, optical, light, total2, optical2, light2, pig,
           drive_send, drive2_send, row_send, col_send, row_recv, col_recv, row_send2, col_send2, row_recv2, col_recv2,
           held, pig_s, drive, light_s, level_sem, one_sem, ready):
    n_comp, n_gy, n_gx = sizes
    grid = n_gy * n_gx
    every = n_comp * grid
    group = every // 4
    _, levels, tile, cols = mid.shape
    half = tile // 2
    wide = 2 * tile
    nt = tracers.shape[0]
    yt = tracers.shape[3]
    position = (lax.axis_index("comp") * grid + lax.axis_index("gy") * n_gx + lax.axis_index("gx")).astype(jnp.int32)
    moved = lax.rem(position + 1, jnp.int32(every))
    strip = lax.rem(moved, jnp.int32(group))
    section = lax.div(moved, jnp.int32(group))
    is_dyn = section == 3
    has_lo = strip > 0
    has_hi = strip < group - 1
    has_left = section > 0
    has_right = section < 2

    def dev(sec, row):
        pos = lax.rem(sec * group + row + (every - 1), jnp.int32(every))
        return (lax.div(pos, jnp.int32(grid)), lax.rem(lax.div(pos, jnp.int32(n_gx)), jnp.int32(n_gy)),
                lax.rem(pos, jnp.int32(n_gx)))

    def remote(src, dst, send_sem, recv_sem, target):
        return pltpu.make_async_remote_copy(src_ref=src, dst_ref=dst, send_sem=send_sem, recv_sem=recv_sem,
                                            device_id=target, device_id_type=MESH)

    three = jnp.int32(3)
    scope = jax.named_scope
    barrier = pltpu.get_barrier_semaphore()

    def load(i, src, dst):
        return pltpu.make_async_copy(src, dst, one_sem.at[i])

    def mask_loads(sem, part, offset):
        begin = pl.multiple_of(jnp.clip(strip + offset, 0, group - 1) * tile, tile)
        return [load(sem, h.at[pl.ds(begin, tile), :], masks.at[part, m]) for m, h in enumerate((ocean_h, bottom_h))]

    def greet(sem, sec, row):
        pl.semaphore_signal(sem, inc=1, device_id=dev(sec, row), device_id_type=MESH)

    sides = ((0, -1, has_lo), (1, 1, has_hi))
    lo_n = has_lo.astype(jnp.int32)
    hi_n = has_hi.astype(jnp.int32)

    both = has_lo & has_hi
    rows_drive = 3 * tile + 1
    batch = levels // 2 if levels % 2 == 0 else levels

    def for_sides(act):
        pl.when(both)(lambda: act(True))
        pl.when(jnp.logical_not(both))(lambda: act(False))

    def pig_copy(k, sec, part, row):
        from_rows = (pl.ds(0, tile), pl.ds(0, half), pl.ds(half, half))[part]
        to_rows = (pl.ds(0, tile), pl.ds(tile, half), pl.ds(tile + half, half))[part]
        return remote(pig_s.at[k, from_rows], pig.at[sec, k, to_rows], one_sem.at[T_PIG_S],
                      level_sem.at[D_PIG, k], dev(three, row))

    def light_copy(k, sec, begin, row):
        return remote(light_s.at[k], light_out.at[k, :, pl.ds(begin, yt)], one_sem.at[T_LIGHT_S], one_sem.at[D_LIGHT],
                      dev(three, row))

    other = dev(lax.rem(section + 1, jnp.int32(4)), strip)

    def recv(dst, sem):
        remote(dst, dst, sem, sem, other).wait_recv()

    def sent(src, sem):
        remote(src, src, sem, sem, other).wait_send()

    halo_of = ((flow, gflow, D_HALO_S, D_HALO), (mid, gmid, D_MID_S, D_MID))

    def halo_copy(what, k, side, offset):
        own, ghost, send, come = halo_of[what]
        place = pl.ds(half * side, half)
        to = strip + offset
        where = dev(three * jnp.minimum(to, 1) if what == 1 else three, to)
        return remote(own.at[:, k, place, :], ghost.at[:, k, place, :], one_sem.at[send], level_sem.at[come, k], where)

    def relay_copy(k):
        place = pl.ds(0, half)
        return remote(gmid.at[:, k, place, :], gmid.at[:, k, place, :], one_sem.at[T_MID_S], level_sem.at[D_MID, k],
                      dev(three, strip))

    @pl.when(is_dyn)
    def _():
        for copy in (load(D_LOAD, flow_h, flow.at[0:4]), load(D_LOAD, chl_h, flow.at[4])):
            copy.start()
        for _, offset, present in sides:
            @pl.when(present)
            def _():
                greet(barrier, three, strip + offset)
        for part in range(3):
            for copy in mask_loads(D_MASK, part, part - 1):
                copy.start()
        for place, present in ((half, has_lo), (0, has_hi)):
            @pl.when(jnp.logical_not(present))
            def _():
                for f in range(5):
                    gflow[f, :, place:place + half, :] = jnp.zeros((levels, half, cols), jnp.float32)
                for f in range(4):
                    gmid[f, :, place:place + half, :] = jnp.zeros((levels, half, cols), jnp.float32)
                for sec in range(3):
                    pig[sec, :, tile + place:tile + place + half, :] = jnp.zeros((levels, half, yt), jnp.float32)
        total[...] = jnp.zeros_like(total)
        total2[...] = jnp.zeros_like(total2)
        optical[...] = jnp.zeros_like(optical)
        optical2[...] = jnp.zeros_like(optical2)
        light[...] = jnp.ones_like(light)
        light2[...] = jnp.ones_like(light2)
        with scope("d_load"):
            load(D_LOAD, flow, flow).wait()
        with scope("d_bar"):
            pl.semaphore_wait(barrier, 3 + 4 * lo_n + 4 * hi_n)

        def drive_copy(k, sec):
            return remote(drive_send.at[k, sec, pl.ds(0, rows_drive)], drive.at[k, pl.ds(0, rows_drive)],
                          one_sem.at[D_DRIVE_S], level_sem.at[T_DRIVE, k], dev(jnp.int32(sec), strip))

        def edge_copy(k, sec, side, offset):
            span = pl.ds(k + 1 - batch, batch)
            return remote(drive_send.at[span, sec, pl.ds(side * (tile - 1), 1)], drive.at[span, pl.ds(rows_drive + 1 - side, 1)],
                          one_sem.at[D_DRIVE_S], one_sem.at[T_EDGE + lax.div(k, jnp.int32(batch))],
                          dev(jnp.int32(sec), strip + offset))

        ahead = jnp.where(strip == 1, jnp.int32(AHEAD), jnp.int32(0))

        def drive2_copy(k, sec):
            return remote(drive2_send.at[k, sec], forcing_out.at[:, k], one_sem.at[D_DRIVE2_S], one_sem.at[T_DRIVE2],
                          dev(jnp.int32(sec), strip))

        @pl.loop(0, levels)
        def _(k):
            for side, offset, present in sides:
                @pl.when(present)
                def _():
                    halo_copy(0, k, side, offset).start()

        for sec in range(3):
            greet(ready, jnp.int32(sec), strip)
            for _, offset, present in sides:
                @pl.when(present)
                def _():
                    greet(ready, jnp.int32(sec), strip + offset)

        load(D_MASK, masks, masks).wait()

        def deep_of(part):
            return jnp.where(masks[part, 0] == 1, masks[part, 1], 0)

        row_d = lax.broadcasted_iota(jnp.int32, (tile, cols), 0)
        depth[0:tile, :] = deep_of(1)
        depth[tile:wide, :] = jnp.where(row_d < half, deep_of(2) * hi_n, deep_of(0) * lo_n)
        tracers_out[...] = jnp.zeros_like(tracers_out)
        forcing_out[...] = jnp.zeros_like(forcing_out)

        lane_row = lax.broadcasted_iota(jnp.int32, (tile, yt), 1) - lax.broadcasted_iota(jnp.int32, (tile, yt), 0)
        on_diagonal = [lane_row == tile * c for c in range(4)]
        lane_d = lax.broadcasted_iota(jnp.int32, (wide, yt), 1)

        def phase(k, now, pigment, sums, opt_s, light_ref):
            first, last = lane_d == 0, lane_d == yt - 1
            opt = opt_s[...] + (0.05 + 0.3 * pigment)
            lower = jnp.exp(-opt)
            heat = 0.5 * (light_ref[...] - lower)
            opt_s[...] = opt
            light_ref[...] = lower
            sea = k < depth[...]
            wet = jnp.where(sea, 0.05, 0.0)
            heat = jnp.where(sea, heat, 0.0)
            sum_u = None
            for n in range(SUB):
                now, p = substep(now, sums[n], heat, wet, first, last, yt)
                sums[n] = p
                sum_u = now[0] if n == 0 else sum_u + now[0]
                sum_v = now[1] if n == 0 else sum_v + now[1]
            return now, sum_u * (1.0 / SUB), sum_v[0:tile] * (1.0 / SUB)

        @pl.loop(0, levels)
        def _(k):
            with scope("d_halo"):
                for_sides(lambda two: recv(gflow.at[:, k, pl.ds(0, tile if two else half), :], level_sem.at[D_HALO, k]))
            now = tuple(jnp.concatenate([flow[f, k], gflow[f, k]], axis=0) for f in range(4))
            now, mean_u, mean_v = phase(k, now, jnp.concatenate([flow[4, k], gflow[4, k]], axis=0), total, optical, light)
            for f in range(4):
                mid[f, k] = now[f][0:tile]
            for side, offset, present in sides:
                @pl.when(present)
                def _():
                    halo_copy(1, k, side, offset).start()
            mix = 0.1 * now[2][0:tile] - 0.05 * now[3][0:tile]
            spread = jnp.zeros((tile, yt), jnp.float32)
            for c, edge in enumerate((yt - 1, yt, 2 * yt - 1, 2 * yt)):
                spread = jnp.where(on_diagonal[c], mean_v[:, edge:edge + 1], spread)
            turned = jnp.sum(spread, axis=0, keepdims=True)
            for sec in range(3):
                here = slice(sec * yt, (sec + 1) * yt)
                drive_send[k, sec, 0:tile] = mean_u[0:tile, here]
                drive_send[k, sec, tile:2 * tile] = mean_v[:, here]
                drive_send[k, sec, 2 * tile:3 * tile] = mix[:, here]
                drive_send[k, sec, 3 * tile:rows_drive] = turned
            for sec in range(3):
                drive_copy(k, sec).start()
            for side, offset, present in sides:
                @pl.when(present & (lax.rem(k, jnp.int32(batch)) == batch - 1))
                def _():
                    for sec in range(3):
                        edge_copy(k, sec, side, offset).start()

        @pl.loop(0, levels)
        def _(k):
            with scope("d_mid"):
                for_sides(lambda two: recv(gmid.at[:, k, pl.ds(0, tile if two else half), :], level_sem.at[D_MID, k]))
            with scope("d_pig"):
                for_sides(lambda two: recv(pig.at[:, k, pl.ds(0, wide if two else tile + half), :], level_sem.at[D_PIG, k]))
            now = tuple(jnp.concatenate([mid[f, k], gmid[f, k]], axis=0) for f in range(4))
            pigment = jnp.concatenate([pig[sec, k] for sec in range(3)], axis=1)
            now, mean_u, mean_v = phase(k, now, pigment, total2, optical2, light2)
            items = (mean_u[0:tile], mean_v, now[2][0:tile], now[3][0:tile])
            for sec in range(3):
                for f in range(4):
                    drive2_send[k, sec, f] = items[f][:, sec * yt:(sec + 1) * yt]
            drive2_copy(k, 0).start()

            pl.when((k < ahead) | (strip == 0))(lambda: drive2_copy(k, 1).start())
            pl.when(strip == 0)(lambda: drive2_copy(k, 2).start())
            for f in range(4):
                flow_out[f, k] = now[f][0:tile]

        @pl.when(has_lo)
        def _():
            for sec, begin in ((1, ahead), (2, 0)):
                @pl.loop(begin, levels)
                def _(k):
                    drive2_copy(k, sec).start()

        with scope("d_light"):
            recv(light_out, one_sem.at[D_LIGHT])
        with scope("d_sends"):
            for_sides(lambda two: sent(flow.at[:, :, pl.ds(0, tile if two else half), :], one_sem.at[D_HALO_S]))
            for_sides(lambda two: sent(mid.at[:, :, pl.ds(0, tile if two else half), :], one_sem.at[D_MID_S]))
            for_sides(lambda two: sent(drive_send.at[:, :, pl.ds(0, rows_drive + (2 if two else 1)), :], one_sem.at[D_DRIVE_S]))
            sent(drive2_send, one_sem.at[D_DRIVE2_S])

    @pl.when(jnp.logical_not(is_dyn))
    def _():
        for _, offset, present in sides:
            @pl.when(present)
            def _():
                greet(barrier, section, strip + offset)
                greet(barrier, three, strip + offset)
        greet(barrier, three, strip)
        beside = ((0, -1, has_left), (1, 1, has_right))
        for _, offset, present in beside:
            @pl.when(present)
            def _():
                greet(barrier, section + offset, strip)
        loads = [load(T_LOAD, tracers_h, tracers), load(T_FORCE, forcing_h, forcing), load(T_REACT, reaction_h, reaction)]
        loads.extend(mask_loads(T_MASK, 1, 0))
        for copy in loads:
            copy.start()
        for side, present in ((0, has_lo), (1, has_hi)):
            @pl.when(jnp.logical_not(present))
            def _():
                drive[:, rows_drive + side:rows_drive + side + 1] = jnp.zeros((levels, 1, yt), jnp.float32)
        for side, present, bufs in ((0, has_lo, (row_recv, row_recv2)), (1, has_hi, (row_recv, row_recv2)),
                                    (0, has_left, (col_recv, col_recv2)), (1, has_right, (col_recv, col_recv2))):
            @pl.when(jnp.logical_not(present))
            def _():
                for buf in bufs:
                    buf[side] = jnp.zeros(buf.shape[1:], jnp.float32)

        lane = lax.broadcasted_iota(jnp.int32, (tile, yt), 1)
        row = lax.broadcasted_iota(jnp.int32, (tile, yt), 0)
        pair = lax.div(lane, jnp.int32(2))
        odd = lax.rem(lane, jnp.int32(2)) == 1
        relays = (section == 0) & (strip == 0)

        flow_out[...] = jnp.zeros_like(flow_out)
        light_out[...] = jnp.zeros_like(light_out)
        with scope('t_load'):
            for copy in loads[:3]:
                copy.wait()
            load(T_MASK, masks.at[1], masks.at[1]).wait()

        def pack(items):
            packed = jnp.zeros((tile, yt), jnp.float32)
            for i, x in enumerate(items):
                packed = jnp.where(pair == i, pltpu.roll(x, 2 * i + 1, 1), packed)
            return packed

        @pl.loop(0, levels)
        def _(k):
            for i, x in enumerate([forcing[0, k]] + [tracers[i, k] for i in range(nt)]):
                row_send[0, k, i] = x[0:1]
                row_send[1, k, i] = x[tile - 1:tile]

        left = pl.multiple_of(section * yt, yt)
        deep = jnp.where(masks[1, 0, :, pl.ds(left, yt)] == 1, masks[1, 1, :, pl.ds(left, yt)], 0)
        with scope('t_bar'):
            pl.semaphore_wait(barrier, lo_n + hi_n + has_left.astype(jnp.int32) + has_right.astype(jnp.int32))

        def row_copies(rows_s, rows_r, row_ss, row_rs):
            for side, offset, present in sides:
                yield present, remote(rows_s.at[side], rows_r.at[1 - side], one_sem.at[row_ss], row_rs, dev(section, strip + offset))

        def col_copies(cols_s, cols_r, col_ss, col_rs):
            for side, offset, present in beside:
                yield present, remote(cols_s, cols_r.at[1 - side], one_sem.at[col_ss], col_rs, dev(section + offset, strip))

        joint = pair_of(levels)

        def second_sems(k):
            at = lax.div(k, jnp.int32(joint))
            return level_sem.at[T_EDGES2, at], level_sem.at[T_EDGES2, levels // joint + at]

        def exchange_b(k):
            rows_come, cols_come = second_sems(k)
            yield from row_copies(row_send2.at[:, k], row_recv2.at[:, k], T_ROW2_S, rows_come)
            yield from col_copies(col_send2.at[k], col_recv2.at[:, k], T_COL2_S, cols_come)

        def start(exchange):
            for present, copy in exchange:
                pl.when(present)(copy.start)

        def arrive_rows(rows_r, row_rs):
            for_sides(lambda two: recv(rows_r if two else rows_r.at[0], row_rs))

        def arrive_cols(cols_r, col_rs):
            middle = has_left & has_right
            pl.when(middle)(lambda: recv(cols_r, col_rs))
            pl.when(jnp.logical_not(middle))(lambda: recv(cols_r.at[0], col_rs))

        def finish_rows(rows_s, row_ss):
            for_sides(lambda two: sent(rows_s if two else rows_s.at[0], one_sem.at[row_ss]))

        def finish_cols(cols_s, twice, col_ss):
            middle = has_left & has_right
            pl.when(middle)(lambda: sent(twice, one_sem.at[col_ss]))
            pl.when(jnp.logical_not(middle))(lambda: sent(cols_s, one_sem.at[col_ss]))

        with scope("t_ready"):
            for part, send, come in ((pl.ds(0, 3), T_ROW_S, T_LEAD), (pl.ds(3, nt - 2), T_ROW_S, T_ROW)):
                start(row_copies(row_send.at[:, :, part], row_recv.at[:, :, part], send, one_sem.at[come]))

            @pl.loop(0, levels)
            def _(k):
                col_send[k] = pack([tracers[i, k] for i in range(nt)] + [forcing[1, k]])
                start(col_copies(col_send.at[k], col_recv.at[:, k], T_COL_S, one_sem.at[T_COL]))

            pl.semaphore_wait(ready, 1 + lo_n + hi_n)
        with scope("t_xa"):
            arrive_rows(row_recv.at[:, :, pl.ds(0, 3)], one_sem.at[T_LEAD])
            arrive_cols(col_recv, one_sem.at[T_COL])

        def tracer_step(k, which, cs, u, v, growth, u_lo, u_hi, v_edge, rows_of, packed):
            um, up, vm, vp = 1.0 - u, 1.0 + u, 1.0 - v, 1.0 + v
            hi_m, lo_p = 1.0 - u_hi, 1.0 + u_lo
            edge_m, edge_p = 1.0 - v_edge, 1.0 + v_edge
            wet = k < deep
            out = []
            for i in which:
                c = cs[i]
                react = reaction[i, 0] * cs[0]
                for b in range(1, nt):
                    react = react + reaction[i, b] * cs[b]
                nxt = jnp.where(row == tile - 1, rows_of[1, k, i] * hi_m, pltpu.roll(c * um, tile - 1, 0))
                prv = jnp.where(row == 0, rows_of[0, k, i] * lo_p, pltpu.roll(c * up, 1, 0))
                edge = pltpu.roll(packed, yt - (2 * i + 1), 1)
                rgt = pltpu.roll(jnp.where(lane == 0, edge * edge_m, c * vm), yt - 1, 1)
                lft = pltpu.roll(jnp.where(lane == yt - 1, edge * edge_p, c * vp), 1, 1)
                out.append(jnp.where(wet, 0.8 * c + 0.05 * ((nxt + prv) + (rgt + lft)) + growth * react, 0.0))
            return out

        def pig_copies(k):
            return ((None, pig_copy(k, section, 0, strip)), (has_lo, pig_copy(k, section, 1, strip - 1)),
                    (has_hi, pig_copy(k, section, 2, strip + 1)))

        def step_a(k, which):
            cs = [tracers[i, k] for i in range(nt)]
            packed = jnp.where(odd, col_recv[1, k], col_recv[0, k])
            growth = 0.1 * jnp.exp(0.1 * forcing[2, k] - 0.05 * forcing[3, k])
            v_edge = pltpu.roll(packed, yt - (2 * nt + 1), 1)
            return tracer_step(k, which, cs, forcing[0, k], forcing[1, k], growth, row_recv[0, k, 0], row_recv[1, k, 0], v_edge,
                               row_recv.at[:, :, pl.ds(1, nt)], packed)

        @pl.loop(0, levels)
        def _(k):
            new = step_a(k, range(2))
            pig_s[k] = 0.25 * (new[0] * new[0] + new[1] * new[1])
            for present, copy in pig_copies(k):
                if present is None:
                    copy.start()
                else:
                    pl.when(present)(copy.start)
            for i in range(2):
                held[i, k] = new[i]

        with scope("t_rest"):
            arrive_rows(row_recv.at[:, :, pl.ds(3, nt - 2)], one_sem.at[T_ROW])

        @pl.loop(0, levels)
        def _(k):
            new = [held[0, k], held[1, k]] + step_a(k, range(2, nt))
            for i in range(nt):
                held[i, k] = new[i]
                row_send2[0, k, i] = new[i][0:1]
                row_send2[1, k, i] = new[i][tile - 1:tile]
            col_send2[k] = pack(new)
            start(exchange_b(k))

        with scope("t_relay"):
            @pl.when(relays)
            def _():
                @pl.loop(0, levels)
                def _(k):
                    recv(gmid.at[:, k, pl.ds(0, half), :], level_sem.at[D_MID, k])
                    relay_copy(k).start()

        @pl.loop(0, levels)
        def _(k):
            with scope("t_xb"):
                @pl.when(lax.rem(k, jnp.int32(joint)) == 0)
                def _():
                    rows_come, cols_come = second_sems(k)
                    arrive_rows(row_recv2.at[:, pl.ds(k, joint)], rows_come)
                    arrive_cols(col_recv2.at[:, pl.ds(k, joint)], cols_come)
            with scope("t_drive"):
                recv(drive.at[k, pl.ds(0, rows_drive)], level_sem.at[T_DRIVE, k])

                @pl.when(lax.rem(k, jnp.int32(batch)) == 0)
                def _():
                    come = one_sem.at[T_EDGE + lax.div(k, jnp.int32(batch))]
                    for_sides(lambda two: recv(drive.at[pl.ds(k, batch), pl.ds(rows_drive, 2 if two else 1)], come))
            cs = [held[i, k] for i in range(nt)]
            packed = jnp.where(odd, col_recv2[1, k], col_recv2[0, k])
            growth = 0.1 * jnp.exp(drive[k, 2 * tile:3 * tile])
            turned = drive[k, 3 * tile:rows_drive]
            ends = [jnp.sum(jnp.where(lane - row == tile * c, turned, 0.0), axis=1, keepdims=True)
                    for c in (2 * section - 2, 2 * section + 1)]
            v_edge = jnp.where(lane == 0, ends[1], ends[0])
            new = tracer_step(k, range(nt), cs, drive[k, 0:tile], drive[k, tile:2 * tile], growth, drive[k, rows_drive:rows_drive + 1],
                              drive[k, rows_drive + 1:rows_drive + 2], v_edge, row_recv2, packed)
            light_s[k] = 0.25 * (new[0] * new[0] + new[1] * new[1])
            light_copy(k, section, left, strip).start()
            for i in range(nt):
                tracers_out[i, k] = new[i]

        with scope("t_drive2"):
            recv(forcing_out, one_sem.at[T_DRIVE2])
        sent(light_s, one_sem.at[T_LIGHT_S])
        for_sides(lambda two: sent(col_recv.at[:, :, pl.ds(0, tile if two else 3 * tile // 4)], one_sem.at[T_PIG_S]))
        finish_rows(row_send, T_ROW_S)
        finish_rows(row_send2, T_ROW2_S)
        finish_cols(col_send, col_recv, T_COL_S)
        finish_cols(col_send2, col_recv2, T_COL2_S)

        @pl.when(relays)
        def _():
            sent(gmid.at[:, :, pl.ds(0, half), :], one_sem.at[T_MID_S])


def write_out(*refs):
    done = refs[-1]
    copies = [pltpu.make_async_copy(refs[i], refs[4 + i], done.at[i]) for i in range(4)]
    for copy in copies:
        copy.start()
    for copy in copies:
        copy.wait()


def solution(mesh):
    sizes = tuple(mesh.shape[a] for a in AXES)

    def on_device(flow, chl, tracers, forcing, ocean, bottom, reaction):
        levels, tile, cols = chl.shape
        nt, yt = tracers.shape[0], tracers.shape[3]
        f32 = jnp.float32

        def buf(*shape):
            return pltpu.VMEM(shape, f32)

        def sem(*shape):
            return pltpu.SemaphoreType.DMA(shape)

        wide = 2 * tile
        scratch = [
            buf(5, levels, tile, cols), buf(5, levels, tile, cols), buf(*flow.shape), buf(*flow.shape),
            pltpu.VMEM((3, 2, tile, cols), jnp.int32), buf(*tracers.shape), buf(*forcing.shape), pltpu.SMEM(reaction.shape, f32),
            pltpu.VMEM((wide, cols), jnp.int32), buf(SUB, wide, cols), buf(wide, cols), buf(wide, cols),
            buf(SUB, wide, cols), buf(wide, cols), buf(wide, cols), buf(3, levels, wide, yt),
            buf(levels, 3, 4 * tile, yt), buf(levels, 3, 4, tile, yt),
            buf(2, levels, nt + 1, 1, yt), buf(levels, tile, yt), buf(2, levels, nt + 1, 1, yt), buf(2, levels, tile, yt),
            buf(2, levels, nt, 1, yt), buf(levels, tile, yt), buf(2, levels, nt, 1, yt), buf(2, levels, tile, yt),
            buf(nt, levels, tile, yt), buf(levels, tile, yt),
            buf(levels, 4 * tile, yt), buf(levels, tile, yt),
            sem(3, max(levels, 2 * levels // pair_of(levels))), sem(N_ONE), pltpu.SemaphoreType.REGULAR,
        ]
        vmem = pl.BlockSpec(memory_space=pltpu.VMEM)
        shapes = [x.shape for x in (flow, chl, tracers, forcing)]
        room = 67043328 - 4 * sum(math.prod(x) for x in shapes) - 2**16
        results = pl.pallas_call(
            functools.partial(kernel, sizes),
            out_shape=[pltpu.VMEM(x, f32) for x in shapes],
            in_specs=[pl.BlockSpec(memory_space=pltpu.HBM)] * 7,
            out_specs=[vmem] * 4,
            scratch_shapes=scratch,
            compiler_params=pltpu.CompilerParams(collective_id=0, has_side_effects=True, vmem_limit_bytes=room),
        )(flow, chl, tracers, forcing, ocean, bottom, reaction)
        return pl.pallas_call(
            write_out,
            out_shape=[jax.ShapeDtypeStruct(x, f32) for x in shapes],
            in_specs=[vmem] * 4,
            out_specs=[pl.BlockSpec(memory_space=pltpu.HBM)] * 4,
            scratch_shapes=[sem(4)],
            compiler_params=pltpu.CompilerParams(vmem_limit_bytes=4 * 2**20),
        )(*results)

    rows4 = P(None, None, AXES, None)
    rows3 = P(None, AXES, None)
    return jax.shard_map(on_device, mesh=mesh, in_specs=(rows4, rows3, rows4, rows4, P(), P(), P()),
                         out_specs=(rows4, rows3, rows4, rows4), check_vma=False)
```
